32 devices in a mesh: replica: 1, ctx: 32 (over z, y, x, core).
Axes of the slice: x: 2, y: 2, z: 4, core: 2. Of those that a mesh axis runs over, the one named last changes fastest.
Arguments:
- queries: bfloat16 [128, 4096], P(('replica', 'ctx')), may hold values from -4 to 6.2
- own_key: bfloat16 [128, 256], P(('replica', 'ctx')), may hold values from -12 to 12
- own_value: bfloat16 [128, 256], P(('replica', 'ctx')), may hold values from -40 to 40
- cache_keys: bfloat16 [2, 1024, 256], P('replica', 'ctx'), may hold values from -4 to 4.7
- cache_values: bfloat16 [2, 1024, 256], P('replica', 'ctx'), may hold values from -40 to 40
- prefix_of_row: int32 [128], P('replica'), may hold values from 0 to 1, as said below
- context_len: int32 [2], P('replica'), may hold values from 512 to 1024
- hidden_in: bfloat16 [128, 4096], P(('replica', 'ctx')), may hold values from -3 to 3
- w_out: bfloat16 [4096, 4096], P('ctx'), may hold values from -0.09375 to 0.09375
- norm_gain: float32 [4096], replicated, may hold values from 0.5 to 1.5
- expert_ids: int32 [128, 8], P(('replica', 'ctx')), may hold values from 0 to 15, all different within a row; in each aligned block of 4 rows (0 to 3, 4 to 7, ...) at most 4 rows name the same one
- route_weights: float32 [128, 8], P(('replica', 'ctx')), may hold values from 0.05 to 0.4
- gate_up_codes: bfloat16 [32, 4096, 768], P('ctx'), may hold values from -0.09375 to 0.09375
- gate_up_scales: float32 [32, 32, 6], P('ctx'), may hold values from 0.6 to 1.7
- down_codes: bfloat16 [32, 384, 4096], P('ctx'), may hold values from -0.21875 to 0.21875
- down_scales: float32 [32, 3, 32], P('ctx'), may hold values from 0.6 to 1.7
Outputs:
- attention_out: bfloat16 [128, 4096], P(('replica', 'ctx'))
- layer_out: bfloat16 [128, 4096], P(('replica', 'ctx'))
The draws below stay inside these ranges and needn't reach their ends.
Inputs may be any that keep to these rules, and one draw needn't show every extreme that they name: `prefix_of_row`: the rows come in aligned blocks of 64 consecutive rows that all name one prefix. `expert_ids`: each row names 8 different experts; among the 4 rows of one device no expert is named more than 4 times.
All inputs are finite; a program needn't handle non-finite values.
Results may differ from the reference program's by a relative error of at most 0.014.
Values may be sent and summed in bfloat16 or wider, within the bound.
A program may use at most 128 MiB of HBM per device.

```python
import math
import jax
import jax.numpy as jnp
import numpy as np
from jax import lax

D = 4096
QH = 32
KVH = 2
HD = 128
CTX_DEV = 32
CAND = 64
ROW_DEV = 4
TOP = 8
EXP_HID = 768
BLK = 128
DQ = 4096
DKV = 256
CTX = 1024
ROWS = 128
PREFIXES = 2
EXPERTS = 16
CAP = 4
N_CTX = 32


def draw_queries(key, part):
    key_base = jax.random.fold_in(jax.random.fold_in(key, 11), 0)
    drawn = jnp.clip(jax.random.normal(key_base, (ROWS, QH * HD), jnp.float32), -4.0, 4.0)
    return drawn.astype(jnp.bfloat16)


def draw_cache_keys(key, part):
    key_base = jax.random.fold_in(jax.random.fold_in(key, 23), 0)
    drawn = jnp.clip(jax.random.normal(key_base, (PREFIXES, CTX, KVH * HD), jnp.float32), -4.0, 4.0)
    return drawn.astype(jnp.bfloat16)


def draw_prefix_of_row(key, part):
    block_choice = jax.random.randint(jax.random.fold_in(key, 37), (PREFIXES,), 0, PREFIXES).astype(jnp.int32)
    block_of_row = (jnp.arange(ROWS, dtype=jnp.int32) // CAND).astype(jnp.int32)
    return jnp.take(block_choice, block_of_row).astype(jnp.int32)


def levels(stream_key, shape, cuts, smallest, top_value):
    loudness = 1.0
    for dim, blocks in cuts:
        draws = jax.random.uniform(jax.random.fold_in(jax.random.fold_in(stream_key, 6), dim), (blocks,), jnp.float32, smallest / len(cuts), top_value / len(cuts))
        loudness = loudness * jnp.repeat(jnp.exp(draws), shape[dim] // blocks).reshape((-1,) + (1,) * (len(shape) - 1 - dim))
    return loudness


def assign_block(stream_key, own, number, rows, number_of, top, limit, slope):
    order = jax.random.permutation(stream_key, number_of)
    heavy_load, usual = shares(number_of, rows * top, limit, slope, True), shares(number_of, rows * top, limit, slope, False)
    places = jnp.arange(number_of)

    def named(sizes, turn):
        used = int((sizes > 0).sum())
        fixed = max(1, used // 4)
        passed = fixed + (places - fixed + turn * (used - fixed)) % max(1, number_of - fixed)
        return jnp.zeros((number_of,), jnp.int32).at[order[jnp.where(places < fixed, places, passed)]].set(jnp.asarray(sizes, jnp.int32))

    sizes = jnp.where(number % 4 == 0, named(heavy_load, number // 4), named(usual, number - number // 4 - 1))
    mixed = jax.random.permutation(jax.random.fold_in(own, 3), number_of)
    source_of, receiver = mixed[0:number_of // 2 * 2:2], mixed[1:number_of // 2 * 2:2]
    slack = jnp.minimum(sizes[source_of] - 1, limit - sizes[receiver]) // 2
    slack = jnp.where((source_of == order[0]) | (receiver == order[0]) | (sizes[receiver] == 0), 0, jnp.maximum(slack, 0))
    passed = jax.random.randint(jax.random.fold_in(own, 4), (number_of // 2,), 0, 1 << 20) % (slack + 1)
    sizes = sizes.at[source_of].add(-passed).at[receiver].add(passed)
    labels = jnp.searchsorted(jnp.cumsum(sizes), jnp.arange(rows * top), side="right").astype(jnp.int32)
    grid = labels.reshape(top, rows).T
    grid = grid[jax.random.permutation(jax.random.fold_in(own, 1), rows)]
    turn = jax.random.randint(jax.random.fold_in(own, 2), (rows, 1), 0, top)
    return jnp.take_along_axis(grid, (jnp.arange(top)[None, :] + turn) % top, axis=1)


def shares(number_of, total, limit, skew, full):
    loads = [(1 << 20) // math.isqrt(rank ** skew) + 1 for rank in range(1, number_of + 1)]
    largest = limit if full else min(limit, max(-(-total // number_of), total * loads[0] // sum(loads)))
    least = 1 if total - largest >= number_of - 1 else 0
    given, surplus = [largest] + [least] * (number_of - 1), total - largest - least * (number_of - 1)
    while surplus > 0:
        candidates = [i for i in range(1, number_of) if given[i] < largest] or [i for i in range(1, number_of) if given[i] < limit]
        whole, budget = sum([loads[i] for i in candidates]), surplus
        for i in candidates:
            more = min(limit - given[i], max(1, budget * loads[i] // whole), surplus)
            given[i] = given[i] + more
            surplus = surplus - more
    return np.array(given)


def bell_draw(key, dims, width, bound, cuts=(), kind=jnp.bfloat16):
    array = jax.random.normal(key, dims, jnp.float32) * width
    if len(cuts) > 0:
        array = levels(key, dims, cuts, -0.22, 0.18) * array
    return jnp.clip(array, min=-bound, max=bound).astype(kind)


def setup_inputs(seed: int = 0, part: int = 0) -> dict:
    key_of = jax.random.split(jax.random.key(seed), 17)
    part_splits = jax.random.split(jax.random.fold_in(key_of[16], part), 17)
    queries = draw_queries(jax.random.fold_in(jax.random.fold_in(key_of[16], part), 71), part)
    own_key = bell_draw(part_splits[1], (ROWS, DKV), 3.0, 12.0, ((0, 32),))
    own_value = bell_draw(part_splits[2], (ROWS, DKV), 8.0, 40.0, ((0, 32),))
    cache_keys = draw_cache_keys(jax.random.fold_in(jax.random.fold_in(key_of[16], part), 71), part)
    cache_values = bell_draw(part_splits[4], (PREFIXES, CTX, DKV), 8.0, 40.0, ((1, 32),))
    prefix_of_row = draw_prefix_of_row(jax.random.fold_in(jax.random.fold_in(key_of[16], part), 71), part)
    context_len = jax.random.randint(part_splits[6], (PREFIXES,), CTX // 2, CTX + 1).astype(jnp.int32)
    hidden_in = bell_draw(part_splits[7], (ROWS, D), 0.5, 3.0, ((0, 32),))
    w_out = bell_draw(key_of[8], (DQ, D), DQ ** -0.5, 0.09375, ((0, 32),))
    norm_gain = jnp.clip(1.0 + 0.1 * jax.random.normal(key_of[9], (D,), jnp.float32), 0.5, 1.5)
    expert_ids_keys = jax.random.split(jax.random.fold_in(part_splits[10], 1), ROWS // ROW_DEV)
    expert_ids_turns = jax.random.permutation(jax.random.fold_in(part_splits[10], 3), ROWS // ROW_DEV)
    expert_ids = jax.vmap(lambda own, number: assign_block(jax.random.fold_in(part_splits[10], 2), own, number, ROW_DEV, EXPERTS, TOP, CAP, 2))(expert_ids_keys, expert_ids_turns).reshape((ROWS, TOP))
    route_weights = jnp.clip(jnp.exp(math.log(0.4) - 2.0794415 * jax.random.uniform(part_splits[11], (ROWS, TOP), jnp.float32) ** levels(part_splits[11], (ROWS, TOP), ((0, 32),), -0.2, 0.2)), 0.05, 0.4)
    gate_up_codes = bell_draw(key_of[12], (2 * EXPERTS, D, EXP_HID), D ** -0.5, 0.09375, ((0, 32),))
    gate_up_scales = jnp.clip(jnp.exp(math.log(1.7) - 1.04145386 * jax.random.uniform(key_of[13], (2 * EXPERTS, D // BLK, EXP_HID // BLK), jnp.float32) ** levels(key_of[13], (2 * EXPERTS, D // BLK, EXP_HID // BLK), ((0, 32),), -0.2, 0.2)), 0.6, 1.7)
    down_codes = bell_draw(key_of[14], (2 * EXPERTS, EXP_HID // 2, D), EXP_HID ** -0.5, 0.21875, ((0, 32),))
    down_scales = jnp.clip(jnp.exp(math.log(1.7) - 1.04145386 * jax.random.uniform(key_of[15], (2 * EXPERTS, EXP_HID // (2 * BLK), D // BLK), jnp.float32) ** levels(key_of[15], (2 * EXPERTS, EXP_HID // (2 * BLK), D // BLK), ((0, 32),), -0.2, 0.2)), 0.6, 1.7)
    return dict(queries=queries, own_key=own_key, own_value=own_value, cache_keys=cache_keys, cache_values=cache_values, prefix_of_row=prefix_of_row, context_len=context_len, hidden_in=hidden_in, w_out=w_out, norm_gain=norm_gain, expert_ids=expert_ids, route_weights=route_weights, gate_up_codes=gate_up_codes, gate_up_scales=gate_up_scales, down_codes=down_codes, down_scales=down_scales)


NEG = -1e+30
EPSILON = 1e-06

def dequantize(code_values, scales):
    rows_per = code_values.shape[0] // scales.shape[0]
    cols_per = code_values.shape[1] // scales.shape[1]
    spread = jnp.repeat(jnp.repeat(scales, rows_per, axis=0), cols_per, axis=1)
    return (code_values.astype(jnp.float32) * spread).astype(jnp.bfloat16)

def reference(queries, own_key, own_value, cache_keys, cache_values, prefix_of_row, context_len, hidden_in, w_out, norm_gain, expert_ids, route_weights, gate_up_codes, gate_up_scales, down_codes, down_scales):
    row_total = queries.shape[0]
    per_group = QH // KVH
    score_scale = 1.0 / math.sqrt(HD)
    position = jnp.arange(CTX, dtype=jnp.int32).reshape(N_CTX, CTX_DEV)

    def attend_row(row_index):
        prefix = prefix_of_row[row_index]
        length = context_len[prefix]
        key_block = cache_keys[prefix].astype(jnp.float32).reshape(N_CTX, CTX_DEV, KVH, HD)
        values = cache_values[prefix].astype(jnp.float32).reshape(N_CTX, CTX_DEV, KVH, HD)
        query_heads = queries[row_index].astype(jnp.float32).reshape(KVH, per_group, HD)
        scores = jnp.einsum('gqd,ctgd->cgqt', query_heads, key_block) * score_scale
        is_valid = (position < length)[:, None, None, :]
        masked = jnp.where(is_valid, scores, NEG)
        block_max = lax.optimization_barrier(jnp.max(masked, axis=-1))
        weights = jnp.where(is_valid, jnp.exp(masked - block_max[..., None]), 0.0)
        block_total = lax.optimization_barrier(jnp.sum(weights, axis=-1))
        rounded = lax.optimization_barrier(weights.astype(jnp.bfloat16)).astype(jnp.float32)
        numerator = jnp.einsum('cgqt,ctgd->cgqd', rounded, values)
        block_out = numerator / jnp.maximum(block_total, 1.0)[..., None]
        block_out = lax.optimization_barrier(block_out.astype(jnp.bfloat16)).astype(jnp.float32)
        own_keys = own_key[row_index].astype(jnp.float32).reshape(KVH, HD)
        own_score = jnp.einsum('gqd,gd->gq', query_heads, own_keys) * score_scale
        top_score = jnp.maximum(lax.optimization_barrier(jnp.max(block_max, axis=0)), own_score)
        factor = block_total * jnp.exp(block_max - top_score[None])
        own_weight = jnp.exp(own_score - top_score)
        own_values = own_value[row_index].astype(jnp.float32).reshape(KVH, 1, HD)
        numerator_all = lax.optimization_barrier(jnp.sum(factor[..., None] * block_out, axis=0)) + own_weight[..., None] * own_values
        denominator = lax.optimization_barrier(jnp.sum(factor, axis=0)) + own_weight
        return (numerator_all / denominator[..., None]).reshape(QH * HD).astype(jnp.bfloat16)
    attended = lax.map(attend_row, jnp.arange(row_total, dtype=jnp.int32))
    mixed = hidden_in.astype(jnp.float32) + jnp.dot(attended, w_out, preferred_element_type=jnp.float32)
    attention_out = mixed.astype(jnp.bfloat16)
    mean_square = lax.optimization_barrier(jnp.mean(mixed * mixed, axis=-1, keepdims=True))
    normed = (mixed * lax.rsqrt(mean_square + EPSILON) * norm_gain).astype(jnp.bfloat16)
    pick_ids = expert_ids.reshape(-1).astype(jnp.int32)
    pick_count = pick_ids.shape[0]
    pick_row = (jnp.arange(pick_count, dtype=jnp.int32) // TOP).astype(jnp.int32)
    pick_weight = route_weights.reshape(-1)
    sorted_picks = jnp.argsort(pick_ids, stable=True).astype(jnp.int32)
    counts = lax.optimization_barrier(jnp.sum((pick_ids[None, :] == jnp.arange(EXPERTS, dtype=jnp.int32)[:, None]).astype(jnp.int32), axis=1))
    starts = (jnp.cumsum(counts) - counts).astype(jnp.int32)
    window = N_CTX * CAP
    padded_order = jnp.concatenate([sorted_picks, jnp.zeros((window,), jnp.int32)])
    half_width = EXP_HID // 2

    def add_expert(expert, running):
        chosen = lax.dynamic_slice_in_dim(padded_order, starts[expert], window)
        is_live = jnp.arange(window, dtype=jnp.int32) < counts[expert]
        inputs = normed[pick_row[chosen]]
        result = jnp.zeros((window, D), jnp.float32)
        for part_half in range(2):
            entry = 2 * expert + part_half
            gate_up = dequantize(lax.dynamic_index_in_dim(gate_up_codes, entry, 0, False), lax.dynamic_index_in_dim(gate_up_scales, entry, 0, False))
            down_proj = dequantize(lax.dynamic_index_in_dim(down_codes, entry, 0, False), lax.dynamic_index_in_dim(down_scales, entry, 0, False))
            projected_in = jnp.dot(inputs, gate_up, preferred_element_type=jnp.float32)
            activated = (jax.nn.silu(projected_in[:, :half_width]) * projected_in[:, half_width:]).astype(jnp.bfloat16)
            piece_out = jnp.dot(activated, down_proj, preferred_element_type=jnp.float32)
            result = result + lax.optimization_barrier(piece_out.astype(jnp.bfloat16)).astype(jnp.float32)
        scaled = jnp.where(is_live, pick_weight[chosen], 0.0)[:, None] * result
        return running.at[pick_row[chosen]].add(scaled)
    expert_sum = lax.fori_loop(0, EXPERTS, add_expert, jnp.zeros((row_total, D), jnp.float32))
    layer_out = (mixed + expert_sum).astype(jnp.bfloat16)
    return (attention_out, layer_out)
```

```python
import math

import jax
import jax.numpy as jnp
from jax import lax
from jax.experimental import pallas as pl
from jax.experimental.pallas import tpu as pltpu
from jax.sharding import PartitionSpec as P

HD = 128
CAND = 64


NEG = -1e30
EPSILON = 1e-06


def swapped(value, axis, distance):
    return lax.ppermute(value, axis, [(i, i ^ 1 << distance) for i in range(lax.axis_size(axis))])


def dequantize(code_values, scales):
    rows_per = code_values.shape[0] // scales.shape[0]
    cols_per = code_values.shape[1] // scales.shape[1]
    spread = jnp.repeat(jnp.repeat(scales, rows_per, axis=0), cols_per, axis=1)
    return (code_values.astype(jnp.float32) * spread).astype(jnp.bfloat16)


def block_partials(query_heads, key_heads, value_heads, is_valid, score_scale):
    scores = (
        jnp.einsum(
            "brgqd,bstgd->brgqst", query_heads, key_heads, preferred_element_type=jnp.float32
        )
        * score_scale
    )
    valid_full = is_valid[:, None, None, None, :, :]
    masked = jnp.where(valid_full, scores, NEG)
    block_max = jnp.max(masked, axis=-1)
    weights = jnp.where(valid_full, jnp.exp(masked - block_max[..., None]), 0.0)
    block_total = jnp.sum(weights, axis=-1)
    numerator = jnp.einsum(
        "brgqst,bstgd->brgqsd",
        weights.astype(jnp.bfloat16),
        value_heads,
        preferred_element_type=jnp.float32,
    )
    block_out = (numerator / jnp.maximum(block_total, 1.0)[..., None]).astype(jnp.bfloat16)
    return (block_max, block_total, block_out)


def fold_blocks(block_max, block_total, block_out):
    local_top = jnp.max(block_max, axis=-1)
    factor = block_total * jnp.exp(block_max - local_top[..., None])
    numer = jnp.sum(factor[..., None] * block_out.astype(jnp.float32), axis=-2)
    denom = jnp.sum(factor, axis=-1)
    return (local_top, numer, denom)


def merge_pair(first, second):
    top = jnp.maximum(first[0], second[0])
    scale_first = jnp.exp(first[0] - top)
    scale_second = jnp.exp(second[0] - top)
    numer = first[1] * scale_first[..., None] + second[1] * scale_second[..., None]
    denom = first[2] * scale_first + second[2] * scale_second
    return (top, numer, denom)


def flipped(index, pattern, bits):
    total = 0
    for bit in range(bits):
        value = index // (1 << bit) % 2
        if pattern >> bit & 1:
            value = 1 - value
        total = total + value * (1 << bit)
    return total


def greet(me, bits):
    barrier = pltpu.get_barrier_semaphore()
    for bit in range(bits):
        pl.semaphore_signal(
            barrier,
            inc=1,
            device_id={"ctx": flipped(me, 1 << bit, bits)},
            device_id_type=pl.DeviceIdType.MESH,
        )
    pl.semaphore_wait(barrier, bits)


def lane_parts(rows, bits):
    middle = rows // 32 * 16
    first = list(range(bits))
    second = list(range(bits))
    if bits > 2:
        second[1], second[2] = second[2], second[1]
    return ((0, middle, first), (middle, rows - middle, second))


def gather_kernel(bits, block_ref, out_ref, send_sem, recv_sem, own_sem):
    me = lax.axis_index("ctx")
    parts = lane_parts(block_ref.shape[0], bits)
    own = pltpu.make_async_copy(block_ref, out_ref.at[me], own_sem)
    own.start()
    greet(me, bits)
    copies = [{}, {}]
    waited = [set(), set()]
    for step in range(bits):
        for part, (start, size, order) in enumerate(parts):
            bit = order[bits - 1 - step]
            held = [0]
            for earlier in range(step):
                held = held + [p | 1 << order[bits - 1 - earlier] for p in held]
            for pattern in held:
                block = flipped(me, pattern, bits)
                if pattern:
                    if pattern not in waited[part]:
                        copies[part][pattern].wait_recv()
                        waited[part].add(pattern)
                    source = out_ref.at[block, pl.ds(start, size)]
                else:
                    source = block_ref.at[pl.ds(start, size)]
                slot = pattern | 1 << bit
                copy = pltpu.make_async_remote_copy(
                    src_ref=source,
                    dst_ref=out_ref.at[block, pl.ds(start, size)],
                    send_sem=send_sem.at[part, slot],
                    recv_sem=recv_sem.at[part, slot],
                    device_id={"ctx": flipped(me, 1 << bit, bits)},
                    device_id_type=pl.DeviceIdType.MESH,
                )
                copy.start()
                copies[part][slot] = copy
    for part in range(2):
        for slot, copy in copies[part].items():
            if slot not in waited[part]:
                copy.wait_recv()
            copy.wait_send()
    own.wait()


def gather_blocks(block, collective_id):
    shards = lax.axis_size("ctx")
    bits = shards.bit_length() - 1
    return pl.pallas_call(
        lambda *refs: gather_kernel(bits, *refs),
        out_shape=jax.ShapeDtypeStruct((shards,) + block.shape, block.dtype),
        in_specs=[pl.BlockSpec(memory_space=pltpu.VMEM)],
        out_specs=pl.BlockSpec(memory_space=pltpu.VMEM),
        scratch_shapes=[
            pltpu.SemaphoreType.DMA((2, shards)),
            pltpu.SemaphoreType.DMA((2, shards)),
            pltpu.SemaphoreType.DMA,
        ],
        compiler_params=pltpu.CompilerParams(collective_id=collective_id, has_side_effects=True),
        name="gather_blocks",
    )(block)


def scatter_kernel(bits, blocks_ref, out_ref, outbox, inbox, send_sem, recv_sem):
    me = lax.axis_index("ctx")
    shards = 1 << bits
    parts = lane_parts(blocks_ref.shape[1], bits)
    greet(me, bits)
    arrived = [{p: [] for p in range(shards)} for _ in parts]
    pending = [{}, {}]
    finished = [set(), set()]
    sent = []
    next_slot = [0, 0]

    def total(part, pattern):
        start, size, _ = parts[part]
        value = blocks_ref[flipped(me, pattern, bits), pl.ds(start, size), :].astype(jnp.float32)
        for slot in arrived[part][pattern]:
            if slot not in finished[part]:
                pending[part][slot].wait_recv()
                finished[part].add(slot)
            value = value + inbox[slot, pl.ds(start, size), :].astype(jnp.float32)
        return value

    for step in range(bits):
        fresh = []
        for part, (start, size, order) in enumerate(parts):
            bit = order[step]
            done_mask = sum(1 << b for b in order[:step])
            for pattern in range(shards):
                if pattern & done_mask or not pattern >> bit & 1:
                    continue
                slot = next_slot[part]
                next_slot[part] += 1
                if step:
                    outbox[slot, pl.ds(start, size), :] = total(part, pattern).astype(outbox.dtype)
                    source = outbox.at[slot, pl.ds(start, size)]
                else:
                    source = blocks_ref.at[flipped(me, pattern, bits), pl.ds(start, size)]
                copy = pltpu.make_async_remote_copy(
                    src_ref=source,
                    dst_ref=inbox.at[slot, pl.ds(start, size)],
                    send_sem=send_sem.at[part, slot],
                    recv_sem=recv_sem.at[part, slot],
                    device_id={"ctx": flipped(me, 1 << bit, bits)},
                    device_id_type=pl.DeviceIdType.MESH,
                )
                copy.start()
                pending[part][slot] = copy
                sent.append(copy)
                fresh.append((part, pattern ^ 1 << bit, slot))
        for part, pattern, slot in fresh:
            arrived[part][pattern].append(slot)
    for part, (start, size, _) in enumerate(parts):
        out_ref[pl.ds(start, size), :] = total(part, 0)
    for copy in sent:
        copy.wait_send()


def scatter_sum(blocks, collective_id):
    shards = lax.axis_size("ctx")
    bits = shards.bit_length() - 1
    return pl.pallas_call(
        lambda *refs: scatter_kernel(bits, *refs),
        out_shape=jax.ShapeDtypeStruct(blocks.shape[1:], jnp.float32),
        in_specs=[pl.BlockSpec(memory_space=pltpu.VMEM)],
        out_specs=pl.BlockSpec(memory_space=pltpu.VMEM),
        scratch_shapes=[
            pltpu.VMEM(blocks.shape, blocks.dtype),
            pltpu.VMEM(blocks.shape, blocks.dtype),
            pltpu.SemaphoreType.DMA((2, shards)),
            pltpu.SemaphoreType.DMA((2, shards)),
        ],
        compiler_params=pltpu.CompilerParams(collective_id=collective_id, has_side_effects=True),
        name="scatter_sum",
    )(blocks)


def staged_layer(
    queries,
    own_key,
    own_value,
    cache_keys,
    cache_values,
    prefix_of_row,
    context_len,
    hidden_in,
    w_out,
    norm_gain,
    expert_ids,
    route_weights,
    gate_up_codes,
    gate_up_scales,
    down_codes,
    down_scales,
):
    shards = lax.axis_size("ctx")
    device = lax.axis_index("ctx")
    head_size = HD
    local_rows = queries.shape[0]
    key_groups = own_key.shape[1] // head_size
    per_group = queries.shape[1] // own_key.shape[1]
    head_count = key_groups * per_group
    ctx_local = cache_keys.shape[1]
    key_width = cache_keys.shape[2]
    score_scale = 1.0 / math.sqrt(head_size)
    block_prefix = prefix_of_row.reshape(-1, CAND)[:, 0]
    prefix_count = block_prefix.shape[0]
    group_size = CAND // local_rows
    group_bits = group_size.bit_length() - 1
    prefix_bits = (shards // group_size).bit_length() - 1
    group_index = device // group_size
    member = device % group_size
    relay = jnp.concatenate(
        [jnp.take(cache_keys, block_prefix, axis=0), jnp.take(cache_values, block_prefix, axis=0)],
        axis=-1,
    )
    relay_shape = relay.shape
    for bit in range(prefix_bits):
        low = 1 << bit
        view = relay.reshape((relay_shape[0] // (2 * low), 2, low) + relay_shape[1:])
        own_bit = group_index // low % 2
        sent = lax.dynamic_index_in_dim(view, 1 - own_bit, 1, False)
        got = swapped(sent, "ctx", group_bits + bit)
        view = lax.dynamic_update_index_in_dim(view, got, 1 - own_bit, 1)
        relay = view.reshape(relay_shape)
    held = queries
    for bit in range(group_bits):
        other = swapped(held, "ctx", bit)
        upper = device // (1 << bit) % 2
        held = jnp.where(
            upper == 0, jnp.concatenate([held, other], 0), jnp.concatenate([other, held], 0)
        )
    length = jnp.take(context_len, jnp.take(block_prefix, group_index))
    source_block = jnp.arange(prefix_count, dtype=jnp.int32) * group_size + member
    position = source_block[:, None] * ctx_local + jnp.arange(ctx_local, dtype=jnp.int32)[None, :]
    is_valid = (position < length)[None]
    query_heads = held.reshape(1, CAND, key_groups, per_group, head_size)
    key_heads = relay[..., :key_width].reshape(1, prefix_count, ctx_local, key_groups, head_size)
    value_heads = relay[..., key_width:].reshape(1, prefix_count, ctx_local, key_groups, head_size)
    block_max, block_total, block_out = block_partials(
        query_heads, key_heads, value_heads, is_valid, score_scale
    )
    block_max = block_max.reshape(CAND, head_count, prefix_count)
    block_total = block_total.reshape(CAND, head_count, prefix_count)
    block_out = block_out.reshape(CAND, head_count, prefix_count, head_size)
    state = fold_blocks(block_max, block_total, block_out)
    for bit in reversed(range(group_bits)):
        own_bit = device // (1 << bit) % 2
        parts = tuple((item.reshape((2, item.shape[0] // 2) + item.shape[1:]) for item in state))
        sent = tuple((lax.dynamic_index_in_dim(item, 1 - own_bit, 0, False) for item in parts))
        kept = tuple((lax.dynamic_index_in_dim(item, own_bit, 0, False) for item in parts))
        got = swapped(sent, "ctx", bit)
        state = merge_pair(kept, got)
    merged_top, merged_numer, merged_denom = state
    own_heads = queries.reshape(local_rows, key_groups, per_group, head_size)
    own_keys = own_key.reshape(local_rows, key_groups, head_size)
    own_score = (
        jnp.einsum(
            "rgqd,rgd->rgq", own_heads, own_keys, preferred_element_type=jnp.float32
        ).reshape(local_rows, head_count)
        * score_scale
    )
    top_score = jnp.maximum(merged_top, own_score)
    block_scale = jnp.exp(merged_top - top_score)
    own_weight = jnp.exp(own_score - top_score)
    own_term = own_value.reshape(local_rows, key_groups, 1, head_size).astype(
        jnp.float32
    ) * own_weight.reshape(local_rows, key_groups, per_group, 1)
    numerator_all = merged_numer * block_scale[..., None] + own_term.reshape(
        local_rows, head_count, head_size
    )
    denominator = merged_denom * block_scale + own_weight
    attended = (numerator_all / denominator[..., None]).reshape(local_rows, -1).astype(jnp.bfloat16)
    feature_width = hidden_in.shape[1]
    lanes = feature_width // 128
    head_rows = lax.all_to_all(attended, "ctx", split_axis=1, concat_axis=0, tiled=True)
    partial = jnp.dot(head_rows, w_out, preferred_element_type=jnp.float32).astype(jnp.bfloat16)
    projected = scatter_sum(partial.reshape(shards, local_rows * lanes, 128), 1).reshape(
        local_rows, feature_width
    )
    mixed_rows = hidden_in.astype(jnp.float32) + projected
    attention_out = mixed_rows.astype(jnp.bfloat16)
    mean_square = jnp.mean(mixed_rows * mixed_rows, axis=-1, keepdims=True)
    normed = (mixed_rows * lax.rsqrt(mean_square + EPSILON) * norm_gain).astype(jnp.bfloat16)
    experts_all = shards // 2
    chosen = expert_ids[:, :, None] == jnp.arange(experts_all, dtype=jnp.int32)[None, None, :]
    dense = jnp.sum(jnp.where(chosen, route_weights[:, :, None], 0.0), axis=1)
    coarse = lax.reduce_precision(dense, exponent_bits=8, mantissa_bits=7)
    fine = dense - coarse
    weight_cols = jnp.concatenate([coarse, fine], axis=1).astype(jnp.bfloat16)
    weight_lanes = -(-weight_cols.shape[1] // 128)
    weight_cols = jnp.pad(weight_cols, ((0, 0), (0, weight_lanes * 128 - weight_cols.shape[1])))
    weight_block = weight_cols.reshape(local_rows * weight_lanes, 128)
    weight_block = jnp.pad(weight_block, ((0, -weight_block.shape[0] % 16), (0, 0)))
    block = jnp.concatenate([normed.reshape(local_rows * lanes, 128), weight_block], axis=0)
    gate_up = dequantize(gate_up_codes[0], gate_up_scales[0])
    down_proj = dequantize(down_codes[0], down_scales[0])
    half_width = down_proj.shape[0]
    gathered = gather_blocks(block, 2)
    all_rows = shards * local_rows
    flat_rows = gathered[:, : local_rows * lanes].reshape(all_rows, feature_width)
    weight_all = gathered[
        :, local_rows * lanes : local_rows * lanes + local_rows * weight_lanes
    ].reshape(all_rows, weight_lanes * 128)
    column = jnp.arange(weight_lanes * 128, dtype=jnp.int32) % experts_all
    in_use = jnp.arange(weight_lanes * 128, dtype=jnp.int32) < 2 * experts_all
    is_mine = jnp.logical_and(column == device // 2, in_use)
    row_weight = jnp.sum(
        jnp.where(is_mine[None, :], weight_all.astype(jnp.float32), 0.0), axis=1, keepdims=True
    )
    projected_in = jnp.dot(flat_rows, gate_up, preferred_element_type=jnp.float32)
    activated = (jax.nn.silu(projected_in[:, :half_width]) * projected_in[:, half_width:]).astype(
        jnp.bfloat16
    )
    result = jnp.dot(activated, down_proj, preferred_element_type=jnp.float32)
    result = jnp.where(row_weight != 0.0, result * row_weight, 0.0).astype(jnp.bfloat16)
    expert_sum = scatter_sum(result.reshape(shards, local_rows * lanes, 128), 3).reshape(
        local_rows, feature_width
    )
    layer_out = (mixed_rows + expert_sum).astype(jnp.bfloat16)
    return (attention_out, layer_out)


def remote(source, target, send_sem, recv_sem, device):
    copy = pltpu.make_async_remote_copy(
        src_ref=source,
        dst_ref=target,
        send_sem=send_sem,
        recv_sem=recv_sem,
        device_id={"ctx": device},
        device_id_type=pl.DeviceIdType.MESH,
    )
    copy.start()
    return copy


class Place:
    def __init__(self, shards):
        self.shards = shards
        self.bits = shards.bit_length() - 1
        self.column = shards // 8
        self.me = lax.axis_index("ctx")
        self.known = {0: self.me}

    def peer(self, pattern):
        if pattern not in self.known:
            self.known[pattern] = flipped(self.me, pattern, self.bits)
        return self.known[pattern]

    def peers(self):
        return [k * 8 for k in range(1, self.column)] + [2, 4, 6, 1]

    def greet(self):
        barrier = pltpu.get_barrier_semaphore()
        for pattern in self.peers():
            pl.semaphore_signal(
                barrier,
                inc=1,
                device_id={"ctx": self.peer(pattern)},
                device_id_type=pl.DeviceIdType.MESH,
            )

    def met(self):
        pl.semaphore_wait(pltpu.get_barrier_semaphore(), len(self.peers()))


def spread(place, column_source, own, buffer, sems, on_column, on_plane, on_core, filler):
    send_sem, recv_sem = sems
    copies = {}

    def post(source, block, slot, towards):
        copies[slot] = remote(
            source,
            buffer.at[place.peer(block)],
            send_sem.at[slot],
            recv_sem.at[slot],
            place.peer(towards),
        )

    def forward(k):
        source = own if k == 0 else buffer.at[place.peer(k * 8)]
        for plane in (6, 2, 4):
            post(source, k * 8, k * 8 + plane, plane)
        post(source, k * 8, k * 8 + 1, 1)

    for k in reversed(range(1, place.column)):
        post(column_source(k), 0, k * 8, k * 8)
    forward(0)
    on_column(0)
    for k in range(1, place.column):
        copies[k * 8].wait_recv()
        forward(k)
        on_column(k)
    filler()
    for k in range(place.column):
        on_plane(k * 8)
        for plane in (2, 4, 6):
            slot = k * 8 + plane
            copies[slot].wait_recv()
            post(buffer.at[place.peer(slot)], slot, slot + 1, 1)
            on_plane(slot)
    for slot in range(0, place.shards, 2):
        copies[slot + 1].wait_recv()
        on_core(slot + 1)
    return list(copies.values())


def collect(place, values, size, boxes, sems, filler):
    send_sem, recv_sem = sems
    core_out, core_in, plane_out, plane_in, column_out, column_in = boxes
    kind = core_out.dtype
    copies = {}
    chips = place.shards // 2

    def held(pattern):
        start = pl.multiple_of(place.peer(pattern) * size, size)
        return values[pl.ds(start, size), :]

    order = [k * 4 + p for k in reversed(range(place.column)) for p in (3, 1, 2)]
    order = order + [k * 4 for k in reversed(range(place.column))]
    for chip in order:
        core_out[chip] = held(chip * 2 + 1).astype(kind)
        copies[chip] = remote(
            core_out.at[chip], core_in.at[chip], send_sem.at[chip], recv_sem.at[chip], place.peer(1)
        )

    def on_chip(chip):
        copies[chip].wait_recv()
        return held(chip * 2) + core_in[chip].astype(jnp.float32)

    for k in reversed(range(place.column)):
        for p in (3, 1, 2):
            chip = k * 4 + p
            plane_out[chip] = on_chip(chip).astype(kind)
            copies[chips + chip] = remote(
                plane_out.at[chip],
                plane_in.at[chip],
                send_sem.at[chips + chip],
                recv_sem.at[chips + chip],
                place.peer(p * 2),
            )
    filler()

    def on_plane(k):
        total = on_chip(k * 4)
        for p in (1, 2, 3):
            copies[chips + k * 4 + p].wait_recv()
            total = total + plane_in[k * 4 + p].astype(jnp.float32)
        return total

    for k in reversed(range(1, place.column)):
        column_out[k] = on_plane(k).astype(kind)
        copies[chips + k * 4] = remote(
            column_out.at[k],
            column_in.at[k],
            send_sem.at[chips + k * 4],
            recv_sem.at[chips + k * 4],
            place.peer(k * 8),
        )
    total = on_plane(0)
    for k in range(1, place.column):
        copies[chips + k * 4].wait_recv()
        total = total + column_in[k].astype(jnp.float32)
    return total, list(copies.values())


def layer_kernel(
    shards,
    per_block,
    prefix_ref,
    length_ref,
    gate_scale_ref,
    down_scale_ref,
    queries_ref,
    own_key_ref,
    own_value_ref,
    keys_ref,
    values_ref,
    hidden_ref,
    gain_ref,
    ids_ref,
    route_ref,
    w_out_hbm,
    gate_hbm,
    down_hbm,
    attention_ref,
    layer_ref,
    w_out_ref,
    gate_ref,
    down_ref,
    load_sem,
    stage,
    q_send,
    q_column,
    q_plane,
    q_all,
    q_wide,
    kv_send,
    kv_all,
    own_wide,
    attended,
    partial,
    mixed_ref,
    normed_send,
    normed_all,
    rows_wide,
    rows_ref,
    *boxes_and_sems,
):
    first_boxes, second_boxes = boxes_and_sems[0:6], boxes_and_sems[6:12]
    sems = boxes_and_sems[12:]
    q_sems, kv_sems, first_sems, row_sems, second_sems = [sems[2 * i : 2 * i + 2] for i in range(5)]
    place = Place(shards)
    me = place.me
    local_rows, width = queries_ref.shape
    lanes = width // 128
    size = local_rows * lanes
    prefixes, positions, _ = keys_ref.shape
    blocks = shards // per_block
    span = blocks * positions
    key_groups = own_key_ref.shape[1] // HD
    per_group = shards // key_groups
    score_scale = 1.0 / math.sqrt(HD)
    f32 = jnp.float32

    loads = []
    for i, (source, target) in enumerate(
        ((w_out_hbm, w_out_ref), (gate_hbm.at[0], gate_ref), (down_hbm.at[0], down_ref))
    ):
        load = pltpu.make_async_copy(source, target, load_sem.at[i])
        load.start()
        loads.append(load)
    place.greet()

    lengths = []
    for b in range(blocks):
        prefix = prefix_ref[b * per_block * local_rows]
        length = length_ref[0]
        for p in range(1, prefixes):
            length = jnp.where(prefix == p, length_ref[p], length)
        lengths.append(length)
        prefix_of = jnp.full((positions, keys_ref.shape[2]), prefix, jnp.int32)
        for which, ref in enumerate((keys_ref, values_ref)):
            chosen = ref[0].astype(f32)
            for p in range(1, prefixes):
                chosen = jnp.where(prefix_of == p, ref[p].astype(f32), chosen)
            at = which * span + b * positions
            for g in range(key_groups):
                kv_send[g, at : at + positions, :] = chosen[:, g * HD : (g + 1) * HD].astype(
                    jnp.bfloat16
                )
    for g in range(key_groups):
        cut = slice(g * HD, (g + 1) * HD)
        stage[0:16, :] = jnp.zeros((16, HD), f32)
        stage[0:local_rows, :] = own_key_ref[:, cut].astype(f32)
        stage[8 : 8 + local_rows, :] = own_value_ref[:, cut].astype(f32)
        kv_send[g, 2 * span : 2 * span + 16, :] = stage[0:16, :].astype(jnp.bfloat16)
    lane = lax.broadcasted_iota(jnp.int32, (local_rows, 128), 1)
    for expert in range(shards // 2):
        weight = jnp.sum(
            jnp.where(ids_ref[...] == expert, route_ref[...], 0.0), axis=1, keepdims=True
        )
        weight = jnp.broadcast_to(weight, (local_rows, 128))
        coarse = weight.astype(jnp.bfloat16).astype(f32)
        both = jnp.where(lane < 64, coarse, weight - coarse)
        for d in (2 * expert, 2 * expert + 1):
            stage[8 * d : 8 * d + local_rows, :] = queries_ref[:, d * HD : (d + 1) * HD].astype(f32)
            stage[8 * d + local_rows : 8 * d + 2 * local_rows, :] = both
    q_send[...] = stage[...].reshape(shards, 8, 128).astype(jnp.bfloat16)
    place.met()

    q_copies = {}

    def q_post(source, target, slot, towards):
        q_copies[slot] = remote(
            source, target, q_sems[0].at[slot], q_sems[1].at[slot], place.peer(towards)
        )

    def q_blocks(slot, start, count):
        k, plane = slot // 8, slot % 8 // 2
        if plane:
            return q_plane.at[k * 4 + plane, pl.ds(start % 2, count)]
        if k:
            return q_column.at[k, pl.ds(start % 8, count)]
        return q_send.at[pl.ds(start, count)]

    for k in reversed(range(1, place.column)):
        q_post(q_send.at[pl.ds(place.peer(k * 8) // 8 * 8, 8)], q_column.at[k], k * 8, k * 8)

    def q_on_column(k):
        if k:
            q_copies[k * 8].wait_recv()
        for plane in (3, 1, 2):
            start = place.peer(plane * 2) // 2 * 2
            q_post(
                q_blocks(k * 8, start, 2), q_plane.at[k * 4 + plane], k * 8 + plane * 2, plane * 2
            )

    def q_on_plane(slot):
        if slot % 8:
            q_copies[slot].wait_recv()
        origin = place.peer(slot)
        q_post(
            q_blocks(slot, place.peer(1), 1), q_all.at[pl.ds(origin, 1)], slot + 1, 1
        )
        q_all[pl.ds(origin, 1)] = q_blocks(slot, me, 1)[...]

    def q_on_core(slot):
        q_copies[slot].wait_recv()

    my_group = me // per_group

    def dequantize_gate():
        loads[1].wait()

        def block_row(i, carry):
            at = pl.ds(pl.multiple_of(i * 128, 128), 128)
            for j in range(gate_ref.shape[1] // 128):
                cut = slice(j * 128, (j + 1) * 128)
                wide = gate_ref[at, cut].astype(f32) * gate_scale_ref[0, i, j]
                gate_ref[at, cut] = wide.astype(jnp.bfloat16)
            return carry

        lax.fori_loop(0, gate_ref.shape[0] // 128, block_row, 0)

    def dequantize_down():
        loads[2].wait()

        def block_column(j, carry):
            at = pl.ds(pl.multiple_of(j * 128, 128), 128)
            for i in range(down_ref.shape[0] // 128):
                cut = slice(i * 128, (i + 1) * 128)
                wide = down_ref[cut, at].astype(f32) * down_scale_ref[0, i, j]
                down_ref[cut, at] = wide.astype(jnp.bfloat16)
            return carry

        lax.fori_loop(0, down_ref.shape[1] // 128, block_column, 0)

    kv_all[pl.ds(me, 1)] = kv_send[pl.ds(my_group, 1)]
    waits = spread(
        place,
        lambda k: kv_send.at[place.peer(k * 8) // per_group],
        kv_send.at[my_group],
        kv_all,
        kv_sems,
        q_on_column,
        q_on_plane,
        q_on_core,
        dequantize_gate,
    )

    q_wide[...] = q_all[...].astype(f32).reshape(shards * 8, 128)
    own_wide[...] = kv_all[:, 2 * span : 2 * span + 16, :].astype(f32).reshape(shards * 16, 128)
    total_positions = shards * positions
    position = lax.broadcasted_iota(jnp.int32, (1, total_positions), 1)

    def picked(ref, start, count, stride):
        return jnp.concatenate(
            [ref[pl.ds(start + r, count, stride=stride), :] for r in range(local_rows)], axis=0
        )

    for b in range(blocks):
        first = b * per_block
        key_at, value_at = b * positions, span + b * positions
        key = kv_all[:, key_at : key_at + positions, :].reshape(total_positions, HD)
        value = kv_all[:, value_at : value_at + positions, :].reshape(total_positions, HD)
        query = picked(q_wide, first * 8, per_block, 8)
        own_k = picked(own_wide, first * 16, per_block, 16)
        own_v = picked(own_wide, first * 16 + 8, per_block, 16)
        scores = lax.dot_general(
            query.astype(jnp.bfloat16), key, (((1,), (1,)), ((), ())), preferred_element_type=f32
        )
        is_valid = position < lengths[b]
        scores = jnp.where(is_valid, scores * score_scale, NEG)
        own_score = jnp.sum(query * own_k, axis=1, keepdims=True) * score_scale
        top = jnp.maximum(jnp.max(scores, axis=1, keepdims=True), own_score)
        weights = jnp.where(is_valid, jnp.exp(scores - top), 0.0)
        own_weight = jnp.exp(own_score - top)
        denominator = jnp.sum(weights, axis=1, keepdims=True) + own_weight
        numerator = jnp.dot(weights.astype(jnp.bfloat16), value, preferred_element_type=f32)
        result = (numerator + own_weight * own_v) / denominator
        for r in range(local_rows):
            attended[r * shards + first : r * shards + first + per_block, :] = result[
                r * per_block : (r + 1) * per_block, :
            ]

    def scatter_rows(result, first_lane):
        for i in range(result.shape[1] // 128):
            for r in range(local_rows):
                partial[pl.ds(r * lanes + first_lane + i, shards, stride=size), :] = result[
                    r * shards : (r + 1) * shards, i * 128 : (i + 1) * 128
                ]

    loads[0].wait()
    head_rows = attended[...].astype(jnp.bfloat16)
    for i in range(0, width, 512):
        scatter_rows(
            jnp.dot(head_rows, w_out_ref[:, i : i + 512], preferred_element_type=f32), i // 128
        )

    projected, more = collect(place, partial, size, first_boxes, first_sems, dequantize_down)
    waits = waits + more

    for i in range(lanes):
        mixed_ref[pl.ds(i, local_rows, stride=lanes), :] = hidden_ref[
            :, i * 128 : (i + 1) * 128
        ].astype(f32)
    mixed = mixed_ref[...] + projected
    mixed_ref[...] = mixed
    grouped = mixed.reshape(local_rows, lanes, 128)
    mean_square = (
        jnp.sum(jnp.sum(grouped * grouped, axis=1, keepdims=True), axis=2, keepdims=True) / width
    )
    normed = grouped * lax.rsqrt(mean_square + EPSILON) * gain_ref[...][None]
    normed_send[...] = normed.reshape(size, 128).astype(jnp.bfloat16)

    def widen(slot):
        at = pl.ds(pl.multiple_of(place.peer(slot) * size, size), size)
        block = normed_all[place.peer(slot)] if slot else normed_send[...]
        rows_wide[at, :] = block.astype(f32)

    def write_attention():
        for i in range(lanes):
            attention_ref[:, i * 128 : (i + 1) * 128] = mixed_ref[
                pl.ds(i, local_rows, stride=lanes), :
            ].astype(jnp.bfloat16)

    more = spread(
        place,
        lambda k: normed_send,
        normed_send,
        normed_all,
        row_sems,
        lambda k: None,
        widen,
        widen,
        write_attention,
    )
    waits = waits + more
    for i in range(lanes):
        for r in range(local_rows):
            rows_ref[r * shards : (r + 1) * shards, i * 128 : (i + 1) * 128] = rows_wide[
                pl.ds(r * lanes + i, shards, stride=size), :
            ].astype(jnp.bfloat16)
    half = down_ref.shape[0]
    projected_in = jnp.dot(rows_ref[...], gate_ref[...], preferred_element_type=f32)
    split = picked(q_wide, local_rows, shards, 8)
    weight = split[:, 0:1] + split[:, 64:65]
    gate = projected_in[:, :half]
    activated = gate / (1.0 + jnp.exp(-gate)) * projected_in[:, half:]
    activated = jnp.where(weight != 0.0, activated * weight, 0.0).astype(jnp.bfloat16)
    for i in range(0, width, 512):
        scatter_rows(
            jnp.dot(activated, down_ref[:, i : i + 512], preferred_element_type=f32), i // 128
        )
    expert_sum, more = collect(place, partial, size, second_boxes, second_sems, lambda: None)
    waits = waits + more
    mixed_ref[...] = mixed_ref[...] + expert_sum
    for i in range(lanes):
        layer_ref[:, i * 128 : (i + 1) * 128] = mixed_ref[
            pl.ds(i, local_rows, stride=lanes), :
        ].astype(jnp.bfloat16)
    for copy in waits + list(q_copies.values()):
        copy.wait_send()


def fused_layer(
    queries,
    own_key,
    own_value,
    cache_keys,
    cache_values,
    prefix_of_row,
    context_len,
    hidden_in,
    w_out,
    norm_gain,
    expert_ids,
    route_weights,
    gate_up_codes,
    gate_up_scales,
    down_codes,
    down_scales,
):
    shards = lax.axis_size("ctx")
    local_rows, width = queries.shape
    lanes = width // 128
    size = local_rows * lanes
    span = shards * local_rows // CAND * cache_keys.shape[1]
    column = shards // 8
    bf16, f32 = jnp.bfloat16, jnp.float32
    kv_rows = 2 * span + 16
    boxes = [
        pltpu.VMEM((count, size, 128), bf16)
        for count in (shards // 2, shards // 2, shards // 2, shards // 2, column, column)
    ]
    smem = pl.BlockSpec(memory_space=pltpu.SMEM)
    vmem = pl.BlockSpec(memory_space=pltpu.VMEM)
    hbm = pl.BlockSpec(memory_space=pl.ANY)
    out = jax.ShapeDtypeStruct((local_rows, width), bf16)
    return pl.pallas_call(
        lambda *refs: layer_kernel(shards, CAND // local_rows, *refs),
        out_shape=(out, out),
        in_specs=[smem] * 4 + [vmem] * 9 + [hbm] * 3,
        out_specs=(vmem, vmem),
        scratch_shapes=[
            pltpu.VMEM(w_out.shape, bf16),
            pltpu.VMEM(gate_up_codes.shape[1:], bf16),
            pltpu.VMEM(down_codes.shape[1:], bf16),
            pltpu.SemaphoreType.DMA((3,)),
            pltpu.VMEM((shards * 8, 128), f32),
            pltpu.VMEM((shards, 8, 128), bf16),
            pltpu.VMEM((column, 8, 8, 128), bf16),
            pltpu.VMEM((column * 4, 2, 8, 128), bf16),
            pltpu.VMEM((shards, 8, 128), bf16),
            pltpu.VMEM((shards * 8, 128), f32),
            pltpu.VMEM((own_key.shape[1] // HD, kv_rows, 128), bf16),
            pltpu.VMEM((shards, kv_rows, 128), bf16),
            pltpu.VMEM((shards * 16, 128), f32),
            pltpu.VMEM((shards * local_rows, 128), f32),
            pltpu.VMEM((shards * size, 128), f32),
            pltpu.VMEM((size, 128), f32),
            pltpu.VMEM((size, 128), bf16),
            pltpu.VMEM((shards, size, 128), bf16),
            pltpu.VMEM((shards * size, 128), f32),
            pltpu.VMEM((shards * local_rows, width), bf16),
        ]
        + boxes
        + boxes
        + [pltpu.SemaphoreType.DMA((shards,))] * 10,
        compiler_params=pltpu.CompilerParams(collective_id=1, has_side_effects=True),
        name="fused_layer",
    )(
        prefix_of_row,
        context_len,
        gate_up_scales,
        down_scales,
        queries,
        own_key,
        own_value,
        cache_keys,
        cache_values,
        hidden_in,
        norm_gain.reshape(lanes, 128),
        expert_ids,
        route_weights,
        w_out,
        gate_up_codes,
        down_codes,
    )


def fits_fused(queries, own_key, cache_keys, w_out, expert_ids):
    shards = lax.axis_size("ctx")
    local_rows, width = queries.shape
    return (
        shards % 8 == 0
        and shards & (shards - 1) == 0
        and w_out.shape[0] == HD
        and width == shards * HD
        and w_out.shape[1] == width
        and 2 * local_rows == 8
        and shards % (own_key.shape[1] // HD * 8) == 0
        and shards * local_rows % CAND == 0
        and cache_keys.shape[1] % 16 == 0
    )


def local(*arrays):
    queries, own_key, cache_keys = arrays[0], arrays[1], arrays[3]
    if fits_fused(queries, own_key, cache_keys, arrays[8], arrays[10]):
        return fused_layer(*arrays)
    return staged_layer(*arrays)


def solution(mesh):
    return jax.shard_map(
        local,
        mesh=mesh,
        in_specs=(
            P(("replica", "ctx"), None),
            P(("replica", "ctx"), None),
            P(("replica", "ctx"), None),
            P("replica", "ctx", None),
            P("replica", "ctx", None),
            P("replica"),
            P("replica"),
            P(("replica", "ctx"), None),
            P("ctx", None),
            P(),
            P(("replica", "ctx"), None),
            P(("replica", "ctx"), None),
            P("ctx", None, None),
            P("ctx", None, None),
            P("ctx", None, None),
            P("ctx", None, None),
        ),
        out_specs=(P(("replica", "ctx"), None), P(("replica", "ctx"), None)),
        check_vma=False,
    )
```

```python
import math

import jax
import jax.numpy as jnp
from jax import lax
from jax.experimental import pallas as pl
from jax.experimental.pallas import tpu as pltpu
from jax.sharding import PartitionSpec as P

HD = 128
CAND = 64


NEG = -1e30
EPSILON = 1e-06
VMEM_BYTES = None


def swapped(value, axis, distance):
    return lax.ppermute(value, axis, [(i, i ^ 1 << distance) for i in range(lax.axis_size(axis))])


def dequantize(code_values, scales):
    rows_per = code_values.shape[0] // scales.shape[0]
    cols_per = code_values.shape[1] // scales.shape[1]
    spread = jnp.repeat(jnp.repeat(scales, rows_per, axis=0), cols_per, axis=1)
    return (code_values.astype(jnp.float32) * spread).astype(jnp.bfloat16)


def block_partials(query_heads, key_heads, value_heads, is_valid, score_scale):
    scores = (
        jnp.einsum(
            "brgqd,bstgd->brgqst", query_heads, key_heads, preferred_element_type=jnp.float32
        )
        * score_scale
    )
    valid_full = is_valid[:, None, None, None, :, :]
    masked = jnp.where(valid_full, scores, NEG)
    block_max = jnp.max(masked, axis=-1)
    weights = jnp.where(valid_full, jnp.exp(masked - block_max[..., None]), 0.0)
    block_total = jnp.sum(weights, axis=-1)
    numerator = jnp.einsum(
        "brgqst,bstgd->brgqsd",
        weights.astype(jnp.bfloat16),
        value_heads,
        preferred_element_type=jnp.float32,
    )
    block_out = (numerator / jnp.maximum(block_total, 1.0)[..., None]).astype(jnp.bfloat16)
    return (block_max, block_total, block_out)


def fold_blocks(block_max, block_total, block_out):
    local_top = jnp.max(block_max, axis=-1)
    factor = block_total * jnp.exp(block_max - local_top[..., None])
    numer = jnp.sum(factor[..., None] * block_out.astype(jnp.float32), axis=-2)
    denom = jnp.sum(factor, axis=-1)
    return (local_top, numer, denom)


def merge_pair(first, second):
    top = jnp.maximum(first[0], second[0])
    scale_first = jnp.exp(first[0] - top)
    scale_second = jnp.exp(second[0] - top)
    numer = first[1] * scale_first[..., None] + second[1] * scale_second[..., None]
    denom = first[2] * scale_first + second[2] * scale_second
    return (top, numer, denom)


def flipped(index, pattern, bits):
    total = 0
    for bit in range(bits):
        value = index // (1 << bit) % 2
        if pattern >> bit & 1:
            value = 1 - value
        total = total + value * (1 << bit)
    return total


def greet(me, bits):
    barrier = pltpu.get_barrier_semaphore()
    for bit in range(bits):
        pl.semaphore_signal(
            barrier,
            inc=1,
            device_id={"ctx": flipped(me, 1 << bit, bits)},
            device_id_type=pl.DeviceIdType.MESH,
        )
    pl.semaphore_wait(barrier, bits)


def lane_parts(rows, bits):
    middle = rows // 32 * 16
    first = list(range(bits))
    second = list(range(bits))
    if bits > 2:
        second[1], second[2] = second[2], second[1]
    return ((0, middle, first), (middle, rows - middle, second))


def gather_kernel(bits, block_ref, out_ref, send_sem, recv_sem, own_sem):
    me = lax.axis_index("ctx")
    parts = lane_parts(block_ref.shape[0], bits)
    own = pltpu.make_async_copy(block_ref, out_ref.at[me], own_sem)
    own.start()
    greet(me, bits)
    copies = [{}, {}]
    waited = [set(), set()]
    for step in range(bits):
        for part, (start, size, order) in enumerate(parts):
            bit = order[bits - 1 - step]
            held = [0]
            for earlier in range(step):
                held = held + [p | 1 << order[bits - 1 - earlier] for p in held]
            for pattern in held:
                block = flipped(me, pattern, bits)
                if pattern:
                    if pattern not in waited[part]:
                        copies[part][pattern].wait_recv()
                        waited[part].add(pattern)
                    source = out_ref.at[block, pl.ds(start, size)]
                else:
                    source = block_ref.at[pl.ds(start, size)]
                slot = pattern | 1 << bit
                copy = pltpu.make_async_remote_copy(
                    src_ref=source,
                    dst_ref=out_ref.at[block, pl.ds(start, size)],
                    send_sem=send_sem.at[part, slot],
                    recv_sem=recv_sem.at[part, slot],
                    device_id={"ctx": flipped(me, 1 << bit, bits)},
                    device_id_type=pl.DeviceIdType.MESH,
                )
                copy.start()
                copies[part][slot] = copy
    for part in range(2):
        for slot, copy in copies[part].items():
            if slot not in waited[part]:
                copy.wait_recv()
            copy.wait_send()
    own.wait()


def gather_blocks(block, collective_id):
    shards = lax.axis_size("ctx")
    bits = shards.bit_length() - 1
    return pl.pallas_call(
        lambda *refs: gather_kernel(bits, *refs),
        out_shape=jax.ShapeDtypeStruct((shards,) + block.shape, block.dtype),
        in_specs=[pl.BlockSpec(memory_space=pltpu.VMEM)],
        out_specs=pl.BlockSpec(memory_space=pltpu.VMEM),
        scratch_shapes=[
            pltpu.SemaphoreType.DMA((2, shards)),
            pltpu.SemaphoreType.DMA((2, shards)),
            pltpu.SemaphoreType.DMA,
        ],
        compiler_params=pltpu.CompilerParams(collective_id=collective_id, has_side_effects=True),
        name="gather_blocks",
    )(block)


def scatter_kernel(bits, blocks_ref, out_ref, outbox, inbox, send_sem, recv_sem):
    me = lax.axis_index("ctx")
    shards = 1 << bits
    parts = lane_parts(blocks_ref.shape[1], bits)
    greet(me, bits)
    arrived = [{p: [] for p in range(shards)} for _ in parts]
    pending = [{}, {}]
    finished = [set(), set()]
    sent = []
    next_slot = [0, 0]

    def total(part, pattern):
        start, size, _ = parts[part]
        value = blocks_ref[flipped(me, pattern, bits), pl.ds(start, size), :].astype(jnp.float32)
        for slot in arrived[part][pattern]:
            if slot not in finished[part]:
                pending[part][slot].wait_recv()
                finished[part].add(slot)
            value = value + inbox[slot, pl.ds(start, size), :].astype(jnp.float32)
        return value

    for step in range(bits):
        fresh = []
        for part, (start, size, order) in enumerate(parts):
            bit = order[step]
            done_mask = sum(1 << b for b in order[:step])
            for pattern in range(shards):
                if pattern & done_mask or not pattern >> bit & 1:
                    continue
                slot = next_slot[part]
                next_slot[part] += 1
                if step:
                    outbox[slot, pl.ds(start, size), :] = total(part, pattern).astype(outbox.dtype)
                    source = outbox.at[slot, pl.ds(start, size)]
                else:
                    source = blocks_ref.at[flipped(me, pattern, bits), pl.ds(start, size)]
                copy = pltpu.make_async_remote_copy(
                    src_ref=source,
                    dst_ref=inbox.at[slot, pl.ds(start, size)],
                    send_sem=send_sem.at[part, slot],
                    recv_sem=recv_sem.at[part, slot],
                    device_id={"ctx": flipped(me, 1 << bit, bits)},
                    device_id_type=pl.DeviceIdType.MESH,
                )
                copy.start()
                pending[part][slot] = copy
                sent.append(copy)
                fresh.append((part, pattern ^ 1 << bit, slot))
        for part, pattern, slot in fresh:
            arrived[part][pattern].append(slot)
    for part, (start, size, _) in enumerate(parts):
        out_ref[pl.ds(start, size), :] = total(part, 0)
    for copy in sent:
        copy.wait_send()


def scatter_sum(blocks, collective_id):
    shards = lax.axis_size("ctx")
    bits = shards.bit_length() - 1
    return pl.pallas_call(
        lambda *refs: scatter_kernel(bits, *refs),
        out_shape=jax.ShapeDtypeStruct(blocks.shape[1:], jnp.float32),
        in_specs=[pl.BlockSpec(memory_space=pltpu.VMEM)],
        out_specs=pl.BlockSpec(memory_space=pltpu.VMEM),
        scratch_shapes=[
            pltpu.VMEM(blocks.shape, blocks.dtype),
            pltpu.VMEM(blocks.shape, blocks.dtype),
            pltpu.SemaphoreType.DMA((2, shards)),
            pltpu.SemaphoreType.DMA((2, shards)),
        ],
        compiler_params=pltpu.CompilerParams(collective_id=collective_id, has_side_effects=True),
        name="scatter_sum",
    )(blocks)


def staged_layer(
    queries,
    own_key,
    own_value,
    cache_keys,
    cache_values,
    prefix_of_row,
    context_len,
    hidden_in,
    w_out,
    norm_gain,
    expert_ids,
    route_weights,
    gate_up_codes,
    gate_up_scales,
    down_codes,
    down_scales,
):
    shards = lax.axis_size("ctx")
    device = lax.axis_index("ctx")
    head_size = HD
    local_rows = queries.shape[0]
    key_groups = own_key.shape[1] // head_size
    per_group = queries.shape[1] // own_key.shape[1]
    head_count = key_groups * per_group
    ctx_local = cache_keys.shape[1]
    key_width = cache_keys.shape[2]
    score_scale = 1.0 / math.sqrt(head_size)
    block_prefix = prefix_of_row.reshape(-1, CAND)[:, 0]
    prefix_count = block_prefix.shape[0]
    group_size = CAND // local_rows
    group_bits = group_size.bit_length() - 1
    prefix_bits = (shards // group_size).bit_length() - 1
    group_index = device // group_size
    member = device % group_size
    relay = jnp.concatenate(
        [jnp.take(cache_keys, block_prefix, axis=0), jnp.take(cache_values, block_prefix, axis=0)],
        axis=-1,
    )
    relay_shape = relay.shape
    for bit in range(prefix_bits):
        low = 1 << bit
        view = relay.reshape((relay_shape[0] // (2 * low), 2, low) + relay_shape[1:])
        own_bit = group_index // low % 2
        sent = lax.dynamic_index_in_dim(view, 1 - own_bit, 1, False)
        got = swapped(sent, "ctx", group_bits + bit)
        view = lax.dynamic_update_index_in_dim(view, got, 1 - own_bit, 1)
        relay = view.reshape(relay_shape)
    held = queries
    for bit in range(group_bits):
        other = swapped(held, "ctx", bit)
        upper = device // (1 << bit) % 2
        held = jnp.where(
            upper == 0, jnp.concatenate([held, other], 0), jnp.concatenate([other, held], 0)
        )
    length = jnp.take(context_len, jnp.take(block_prefix, group_index))
    source_block = jnp.arange(prefix_count, dtype=jnp.int32) * group_size + member
    position = source_block[:, None] * ctx_local + jnp.arange(ctx_local, dtype=jnp.int32)[None, :]
    is_valid = (position < length)[None]
    query_heads = held.reshape(1, CAND, key_groups, per_group, head_size)
    key_heads = relay[..., :key_width].reshape(1, prefix_count, ctx_local, key_groups, head_size)
    value_heads = relay[..., key_width:].reshape(1, prefix_count, ctx_local, key_groups, head_size)
    block_max, block_total, block_out = block_partials(
        query_heads, key_heads, value_heads, is_valid, score_scale
    )
    block_max = block_max.reshape(CAND, head_count, prefix_count)
    block_total = block_total.reshape(CAND, head_count, prefix_count)
    block_out = block_out.reshape(CAND, head_count, prefix_count, head_size)
    state = fold_blocks(block_max, block_total, block_out)
    for bit in reversed(range(group_bits)):
        own_bit = device // (1 << bit) % 2
        parts = tuple((item.reshape((2, item.shape[0] // 2) + item.shape[1:]) for item in state))
        sent = tuple((lax.dynamic_index_in_dim(item, 1 - own_bit, 0, False) for item in parts))
        kept = tuple((lax.dynamic_index_in_dim(item, own_bit, 0, False) for item in parts))
        got = swapped(sent, "ctx", bit)
        state = merge_pair(kept, got)
    merged_top, merged_numer, merged_denom = state
    own_heads = queries.reshape(local_rows, key_groups, per_group, head_size)
    own_keys = own_key.reshape(local_rows, key_groups, head_size)
    own_score = (
        jnp.einsum(
            "rgqd,rgd->rgq", own_heads, own_keys, preferred_element_type=jnp.float32
        ).reshape(local_rows, head_count)
        * score_scale
    )
    top_score = jnp.maximum(merged_top, own_score)
    block_scale = jnp.exp(merged_top - top_score)
    own_weight = jnp.exp(own_score - top_score)
    own_term = own_value.reshape(local_rows, key_groups, 1, head_size).astype(
        jnp.float32
    ) * own_weight.reshape(local_rows, key_groups, per_group, 1)
    numerator_all = merged_numer * block_scale[..., None] + own_term.reshape(
        local_rows, head_count, head_size
    )
    denominator = merged_denom * block_scale + own_weight
    attended = (numerator_all / denominator[..., None]).reshape(local_rows, -1).astype(jnp.bfloat16)
    feature_width = hidden_in.shape[1]
    lanes = feature_width // 128
    head_rows = lax.all_to_all(attended, "ctx", split_axis=1, concat_axis=0, tiled=True)
    partial = jnp.dot(head_rows, w_out, preferred_element_type=jnp.float32).astype(jnp.bfloat16)
    projected = scatter_sum(partial.reshape(shards, local_rows * lanes, 128), 1).reshape(
        local_rows, feature_width
    )
    mixed_rows = hidden_in.astype(jnp.float32) + projected
    attention_out = mixed_rows.astype(jnp.bfloat16)
    mean_square = jnp.mean(mixed_rows * mixed_rows, axis=-1, keepdims=True)
    normed = (mixed_rows * lax.rsqrt(mean_square + EPSILON) * norm_gain).astype(jnp.bfloat16)
    experts_all = shards // 2
    chosen = expert_ids[:, :, None] == jnp.arange(experts_all, dtype=jnp.int32)[None, None, :]
    dense = jnp.sum(jnp.where(chosen, route_weights[:, :, None], 0.0), axis=1)
    coarse = lax.reduce_precision(dense, exponent_bits=8, mantissa_bits=7)
    fine = dense - coarse
    weight_cols = jnp.concatenate([coarse, fine], axis=1).astype(jnp.bfloat16)
    weight_lanes = -(-weight_cols.shape[1] // 128)
    weight_cols = jnp.pad(weight_cols, ((0, 0), (0, weight_lanes * 128 - weight_cols.shape[1])))
    weight_block = weight_cols.reshape(local_rows * weight_lanes, 128)
    weight_block = jnp.pad(weight_block, ((0, -weight_block.shape[0] % 16), (0, 0)))
    block = jnp.concatenate([normed.reshape(local_rows * lanes, 128), weight_block], axis=0)
    gate_up = dequantize(gate_up_codes[0], gate_up_scales[0])
    down_proj = dequantize(down_codes[0], down_scales[0])
    half_width = down_proj.shape[0]
    gathered = gather_blocks(block, 2)
    all_rows = shards * local_rows
    flat_rows = gathered[:, : local_rows * lanes].reshape(all_rows, feature_width)
    weight_all = gathered[
        :, local_rows * lanes : local_rows * lanes + local_rows * weight_lanes
    ].reshape(all_rows, weight_lanes * 128)
    column = jnp.arange(weight_lanes * 128, dtype=jnp.int32) % experts_all
    in_use = jnp.arange(weight_lanes * 128, dtype=jnp.int32) < 2 * experts_all
    is_mine = jnp.logical_and(column == device // 2, in_use)
    row_weight = jnp.sum(
        jnp.where(is_mine[None, :], weight_all.astype(jnp.float32), 0.0), axis=1, keepdims=True
    )
    projected_in = jnp.dot(flat_rows, gate_up, preferred_element_type=jnp.float32)
    activated = (jax.nn.silu(projected_in[:, :half_width]) * projected_in[:, half_width:]).astype(
        jnp.bfloat16
    )
    result = jnp.dot(activated, down_proj, preferred_element_type=jnp.float32)
    result = jnp.where(row_weight != 0.0, result * row_weight, 0.0).astype(jnp.bfloat16)
    expert_sum = scatter_sum(result.reshape(shards, local_rows * lanes, 128), 3).reshape(
        local_rows, feature_width
    )
    layer_out = (mixed_rows + expert_sum).astype(jnp.bfloat16)
    return (attention_out, layer_out)


def remote(source, target, send_sem, recv_sem, device):
    copy = pltpu.make_async_remote_copy(
        src_ref=source,
        dst_ref=target,
        send_sem=send_sem,
        recv_sem=recv_sem,
        device_id={"ctx": device},
        device_id_type=pl.DeviceIdType.MESH,
    )
    copy.start()
    return copy


class Place:
    def __init__(self, shards):
        self.shards = shards
        self.bits = shards.bit_length() - 1
        self.column = shards // 8
        self.me = lax.axis_index("ctx")
        self.known = {0: self.me}

    def peer(self, pattern):
        if pattern not in self.known:
            self.known[pattern] = flipped(self.me, pattern, self.bits)
        return self.known[pattern]

    def peers(self):
        return [k * 8 for k in range(1, self.column)] + [2, 4, 6, 1]

    def greet(self):
        barrier = pltpu.get_barrier_semaphore()
        for pattern in self.peers():
            pl.semaphore_signal(
                barrier,
                inc=1,
                device_id={"ctx": self.peer(pattern)},
                device_id_type=pl.DeviceIdType.MESH,
            )

    def met(self):
        pl.semaphore_wait(pltpu.get_barrier_semaphore(), len(self.peers()))


def spread(place, column_source, own, buffer, sems, on_column, on_plane, on_core, filler):
    send_sem, recv_sem = sems
    copies = {}

    def post(source, block, slot, towards):
        copies[slot] = remote(
            source,
            buffer.at[place.peer(block)],
            send_sem.at[slot],
            recv_sem.at[slot],
            place.peer(towards),
        )

    def forward(k):
        source = own if k == 0 else buffer.at[place.peer(k * 8)]
        for plane in (6, 2, 4):
            post(source, k * 8, k * 8 + plane, plane)
        post(source, k * 8, k * 8 + 1, 1)

    for k in reversed(range(1, place.column)):
        post(column_source(k), 0, k * 8, k * 8)
    forward(0)
    on_column(0)
    for k in range(1, place.column):
        copies[k * 8].wait_recv()
        forward(k)
        on_column(k)
    filler()
    for k in range(place.column):
        on_plane(k * 8)
        for plane in (2, 4, 6):
            slot = k * 8 + plane
            copies[slot].wait_recv()
            post(buffer.at[place.peer(slot)], slot, slot + 1, 1)
            on_plane(slot)
    for slot in range(0, place.shards, 2):
        copies[slot + 1].wait_recv()
        on_core(slot + 1)
    return list(copies.values())


def collect(place, values, size, boxes, sems, filler):
    send_sem, recv_sem = sems
    core_out, core_in, plane_out, plane_in, column_out, column_in = boxes
    kind = core_out.dtype
    copies = {}
    chips = place.shards // 2

    def held(pattern):
        start = pl.multiple_of(place.peer(pattern) * size, size)
        return values[pl.ds(start, size), :]

    order = [k * 4 + p for k in reversed(range(place.column)) for p in (3, 1, 2)]
    order = order + [k * 4 for k in reversed(range(place.column))]
    for chip in order:
        core_out[chip] = held(chip * 2 + 1).astype(kind)
        copies[chip] = remote(
            core_out.at[chip], core_in.at[chip], send_sem.at[chip], recv_sem.at[chip], place.peer(1)
        )

    def on_chip(chip):
        copies[chip].wait_recv()
        return held(chip * 2) + core_in[chip].astype(jnp.float32)

    for k in reversed(range(place.column)):
        for p in (3, 1, 2):
            chip = k * 4 + p
            plane_out[chip] = on_chip(chip).astype(kind)
            copies[chips + chip] = remote(
                plane_out.at[chip],
                plane_in.at[chip],
                send_sem.at[chips + chip],
                recv_sem.at[chips + chip],
                place.peer(p * 2),
            )
    filler()

    def on_plane(k):
        total = on_chip(k * 4)
        for p in (1, 2, 3):
            copies[chips + k * 4 + p].wait_recv()
            total = total + plane_in[k * 4 + p].astype(jnp.float32)
        return total

    for k in reversed(range(1, place.column)):
        column_out[k] = on_plane(k).astype(kind)
        copies[chips + k * 4] = remote(
            column_out.at[k],
            column_in.at[k],
            send_sem.at[chips + k * 4],
            recv_sem.at[chips + k * 4],
            place.peer(k * 8),
        )
    total = on_plane(0)
    for k in range(1, place.column):
        copies[chips + k * 4].wait_recv()
        total = total + column_in[k].astype(jnp.float32)
    return total, list(copies.values())


def layer_kernel(
    shards,
    per_block,
    *refs,
):
    given, (mixed_out, expert_out), refs = refs[:16], refs[16:18], refs[18:]
    held, load_sem = refs[:16], refs[16]
    (
        prefix_ref,
        length_ref,
        keys_ref,
        values_ref,
        own_key_ref,
        own_value_ref,
        queries_ref,
        ids_ref,
        route_ref,
        w_out_ref,
        gate_ref,
        gate_scale_ref,
        down_ref,
        down_scale_ref,
        hidden_ref,
        gain_ref,
    ) = held
    (
        stage,
        q_send,
        q_column,
        q_plane,
        q_all,
        q_wide,
        kv_send,
        kv_all,
        own_wide,
        attended,
        partial,
        mixed_ref,
        normed_send,
        normed_all,
        rows_wide,
        rows_ref,
    ) = refs[17 : 17 + 16]
    boxes_and_sems = refs[17 + 16 :]
    first_boxes, second_boxes = boxes_and_sems[0:6], boxes_and_sems[6:12]
    sems = boxes_and_sems[12:]
    q_sems, kv_sems, first_sems, row_sems, second_sems = [sems[2 * i : 2 * i + 2] for i in range(5)]
    place = Place(shards)
    me = place.me
    local_rows, width = queries_ref.shape
    lanes = width // 128
    size = local_rows * lanes
    prefixes, positions, _ = keys_ref.shape
    blocks = shards // per_block
    span = blocks * positions
    key_groups = own_key_ref.shape[1] // HD
    per_group = shards // key_groups
    score_scale = 1.0 / math.sqrt(HD)
    f32 = jnp.float32

    place.greet()
    loads = []
    for i, (source, target) in enumerate(zip(given, held)):
        load = pltpu.make_async_copy(source, target, load_sem.at[i])
        load.start()
        loads.append(load)
    for load in loads[:9]:
        load.wait()

    lengths = []
    for b in range(blocks):
        prefix = prefix_ref[b * per_block * local_rows]
        length = length_ref[0]
        for p in range(1, prefixes):
            length = jnp.where(prefix == p, length_ref[p], length)
        lengths.append(length)
        prefix_of = jnp.full((positions, keys_ref.shape[2]), prefix, jnp.int32)
        for which, ref in enumerate((keys_ref, values_ref)):
            chosen = ref[0].astype(f32)
            for p in range(1, prefixes):
                chosen = jnp.where(prefix_of == p, ref[p].astype(f32), chosen)
            at = which * span + b * positions
            for g in range(key_groups):
                kv_send[g, at : at + positions, :] = chosen[:, g * HD : (g + 1) * HD].astype(
                    jnp.bfloat16
                )
    for g in range(key_groups):
        cut = slice(g * HD, (g + 1) * HD)
        stage[0:16, :] = jnp.zeros((16, HD), f32)
        stage[0:local_rows, :] = own_key_ref[:, cut].astype(f32)
        stage[8 : 8 + local_rows, :] = own_value_ref[:, cut].astype(f32)
        kv_send[g, 2 * span : 2 * span + 16, :] = stage[0:16, :].astype(jnp.bfloat16)
    lane = lax.broadcasted_iota(jnp.int32, (local_rows, 128), 1)
    for expert in range(shards // 2):
        weight = jnp.sum(
            jnp.where(ids_ref[...] == expert, route_ref[...], 0.0), axis=1, keepdims=True
        )
        weight = jnp.broadcast_to(weight, (local_rows, 128))
        coarse = weight.astype(jnp.bfloat16).astype(f32)
        both = jnp.where(lane < 64, coarse, weight - coarse)
        for d in (2 * expert, 2 * expert + 1):
            stage[8 * d : 8 * d + local_rows, :] = queries_ref[:, d * HD : (d + 1) * HD].astype(f32)
            stage[8 * d + local_rows : 8 * d + 2 * local_rows, :] = both
    q_send[...] = stage[...].reshape(shards, 8, 128).astype(jnp.bfloat16)
    place.met()

    q_copies = {}

    def q_post(source, target, slot, towards):
        q_copies[slot] = remote(
            source, target, q_sems[0].at[slot], q_sems[1].at[slot], place.peer(towards)
        )

    def q_blocks(slot, start, count):
        k, plane = slot // 8, slot % 8 // 2
        if plane:
            return q_plane.at[k * 4 + plane, pl.ds(start % 2, count)]
        if k:
            return q_column.at[k, pl.ds(start % 8, count)]
        return q_send.at[pl.ds(start, count)]

    for k in reversed(range(1, place.column)):
        q_post(q_send.at[pl.ds(place.peer(k * 8) // 8 * 8, 8)], q_column.at[k], k * 8, k * 8)

    def q_on_column(k):
        if k:
            q_copies[k * 8].wait_recv()
        for plane in (3, 1, 2):
            start = place.peer(plane * 2) // 2 * 2
            q_post(
                q_blocks(k * 8, start, 2), q_plane.at[k * 4 + plane], k * 8 + plane * 2, plane * 2
            )

    def q_on_plane(slot):
        if slot % 8:
            q_copies[slot].wait_recv()
        origin = place.peer(slot)
        q_post(
            q_blocks(slot, place.peer(1), 1), q_all.at[pl.ds(origin, 1)], slot + 1, 1
        )
        q_all[pl.ds(origin, 1)] = q_blocks(slot, me, 1)[...]

    def q_on_core(slot):
        q_copies[slot].wait_recv()

    my_group = me // per_group

    def dequantize_gate():
        loads[10].wait()
        loads[11].wait()

        def block_row(i, carry):
            at = pl.ds(pl.multiple_of(i * 128, 128), 128)
            for j in range(gate_ref.shape[1] // 128):
                cut = slice(j * 128, (j + 1) * 128)
                wide = gate_ref[at, cut].astype(f32) * gate_scale_ref[j, 0, i]
                gate_ref[at, cut] = wide.astype(jnp.bfloat16)
            return carry

        lax.fori_loop(0, gate_ref.shape[0] // 128, block_row, 0)

    def dequantize_down():
        loads[12].wait()
        loads[13].wait()

        def block_column(j, carry):
            at = pl.ds(pl.multiple_of(j * 128, 128), 128)
            for i in range(down_ref.shape[0] // 128):
                cut = slice(i * 128, (i + 1) * 128)
                wide = down_ref[cut, at].astype(f32) * down_scale_ref[i, 0, j]
                down_ref[cut, at] = wide.astype(jnp.bfloat16)
            return carry

        lax.fori_loop(0, down_ref.shape[1] // 128, block_column, 0)

    kv_all[pl.ds(me, 1)] = kv_send[pl.ds(my_group, 1)]
    waits = spread(
        place,
        lambda k: kv_send.at[place.peer(k * 8) // per_group],
        kv_send.at[my_group],
        kv_all,
        kv_sems,
        q_on_column,
        q_on_plane,
        q_on_core,
        dequantize_gate,
    )

    q_wide[...] = q_all[...].astype(f32).reshape(shards * 8, 128)
    own_wide[...] = kv_all[:, 2 * span : 2 * span + 16, :].astype(f32).reshape(shards * 16, 128)
    total_positions = shards * positions
    position = lax.broadcasted_iota(jnp.int32, (1, total_positions), 1)

    def picked(ref, start, count, stride):
        return jnp.concatenate(
            [ref[pl.ds(start + r, count, stride=stride), :] for r in range(local_rows)], axis=0
        )

    for b in range(blocks):
        first = b * per_block
        key_at, value_at = b * positions, span + b * positions
        key = kv_all[:, key_at : key_at + positions, :].reshape(total_positions, HD)
        value = kv_all[:, value_at : value_at + positions, :].reshape(total_positions, HD)
        query = picked(q_wide, first * 8, per_block, 8)
        own_k = picked(own_wide, first * 16, per_block, 16)
        own_v = picked(own_wide, first * 16 + 8, per_block, 16)
        scores = lax.dot_general(
            query.astype(jnp.bfloat16), key, (((1,), (1,)), ((), ())), preferred_element_type=f32
        )
        is_valid = position < lengths[b]
        scores = jnp.where(is_valid, scores * score_scale, NEG)
        own_score = jnp.sum(query * own_k, axis=1, keepdims=True) * score_scale
        top = jnp.maximum(jnp.max(scores, axis=1, keepdims=True), own_score)
        weights = jnp.where(is_valid, jnp.exp(scores - top), 0.0)
        own_weight = jnp.exp(own_score - top)
        denominator = jnp.sum(weights, axis=1, keepdims=True) + own_weight
        numerator = jnp.dot(weights.astype(jnp.bfloat16), value, preferred_element_type=f32)
        result = (numerator + own_weight * own_v) / denominator
        for r in range(local_rows):
            attended[r * shards + first : r * shards + first + per_block, :] = result[
                r * per_block : (r + 1) * per_block, :
            ]

    def scatter_rows(result, first_lane):
        for i in range(result.shape[1] // 128):
            for r in range(local_rows):
                partial[pl.ds(r * lanes + first_lane + i, shards, stride=size), :] = result[
                    r * shards : (r + 1) * shards, i * 128 : (i + 1) * 128
                ]

    loads[9].wait()
    head_rows = attended[...].astype(jnp.bfloat16)
    for i in range(0, width, 512):
        scatter_rows(
            jnp.dot(head_rows, w_out_ref[:, i : i + 512], preferred_element_type=f32), i // 128
        )

    projected, more = collect(place, partial, size, first_boxes, first_sems, dequantize_down)
    waits = waits + more

    loads[14].wait()
    loads[15].wait()
    for i in range(lanes):
        mixed_ref[pl.ds(i, local_rows, stride=lanes), :] = hidden_ref[
            :, i * 128 : (i + 1) * 128
        ].astype(f32)
    mixed = mixed_ref[...] + projected
    mixed_ref[...] = mixed
    grouped = mixed.reshape(local_rows, lanes, 128)
    mean_square = (
        jnp.sum(jnp.sum(grouped * grouped, axis=1, keepdims=True), axis=2, keepdims=True) / width
    )
    normed = grouped * lax.rsqrt(mean_square + EPSILON) * gain_ref[...][None]
    normed_send[...] = normed.reshape(size, 128).astype(jnp.bfloat16)

    def widen(slot):
        at = pl.ds(pl.multiple_of(place.peer(slot) * size, size), size)
        block = normed_all[place.peer(slot)] if slot else normed_send[...]
        rows_wide[at, :] = block.astype(f32)

    def write_attention():
        for i in range(lanes):
            mixed_out[:, i * 128 : (i + 1) * 128] = mixed_ref[
                pl.ds(i, local_rows, stride=lanes), :
            ]

    more = spread(
        place,
        lambda k: normed_send,
        normed_send,
        normed_all,
        row_sems,
        lambda k: None,
        widen,
        widen,
        write_attention,
    )
    waits = waits + more
    for i in range(lanes):
        for r in range(local_rows):
            rows_ref[r * shards : (r + 1) * shards, i * 128 : (i + 1) * 128] = rows_wide[
                pl.ds(r * lanes + i, shards, stride=size), :
            ].astype(jnp.bfloat16)
    half = down_ref.shape[0]
    projected_in = jnp.dot(rows_ref[...], gate_ref[...], preferred_element_type=f32)
    split = picked(q_wide, local_rows, shards, 8)
    weight = split[:, 0:1] + split[:, 64:65]
    gate = projected_in[:, :half]
    activated = gate / (1.0 + jnp.exp(-gate)) * projected_in[:, half:]
    activated = jnp.where(weight != 0.0, activated * weight, 0.0).astype(jnp.bfloat16)
    for i in range(0, width, 512):
        scatter_rows(
            jnp.dot(activated, down_ref[:, i : i + 512], preferred_element_type=f32), i // 128
        )
    expert_sum, more = collect(place, partial, size, second_boxes, second_sems, lambda: None)
    waits = waits + more
    mixed_ref[...] = expert_sum
    for i in range(lanes):
        expert_out[:, i * 128 : (i + 1) * 128] = mixed_ref[pl.ds(i, local_rows, stride=lanes), :]
    for copy in waits + list(q_copies.values()):
        copy.wait_send()


def fused_layer(
    queries,
    own_key,
    own_value,
    cache_keys,
    cache_values,
    prefix_of_row,
    context_len,
    hidden_in,
    w_out,
    norm_gain,
    expert_ids,
    route_weights,
    gate_up_codes,
    gate_up_scales,
    down_codes,
    down_scales,
):
    shards = lax.axis_size("ctx")
    local_rows, width = queries.shape
    lanes = width // 128
    size = local_rows * lanes
    span = shards * local_rows // CAND * cache_keys.shape[1]
    column = shards // 8
    bf16, f32 = jnp.bfloat16, jnp.float32
    kv_rows = 2 * span + 16
    boxes = [
        pltpu.VMEM((count, size, 128), bf16)
        for count in (shards // 2, shards // 2, shards // 2, shards // 2, column, column)
    ]
    operands = (
        prefix_of_row,
        context_len,
        cache_keys,
        cache_values,
        own_key,
        own_value,
        queries,
        expert_ids,
        route_weights,
        w_out,
        gate_up_codes[0],
        gate_up_scales.transpose(2, 0, 1),
        down_codes[0],
        down_scales.transpose(1, 0, 2),
        hidden_in,
        norm_gain.reshape(lanes, 128),
    )
    scalars = (0, 1, 11, 13)
    out = jax.ShapeDtypeStruct((local_rows, width), f32)
    vmem = pl.BlockSpec(memory_space=pltpu.VMEM)
    mixed, expert_sum = pl.pallas_call(
        lambda *refs: layer_kernel(shards, CAND // local_rows, *refs),
        out_shape=(out, out),
        in_specs=[pl.BlockSpec(memory_space=pltpu.HBM)] * len(operands),
        out_specs=(vmem, vmem),
        scratch_shapes=[
            (pltpu.SMEM if i in scalars else pltpu.VMEM)(x.shape, x.dtype)
            for i, x in enumerate(operands)
        ]
        + [
            pltpu.SemaphoreType.DMA((len(operands),)),
            pltpu.VMEM((shards * 8, 128), f32),
            pltpu.VMEM((shards, 8, 128), bf16),
            pltpu.VMEM((column, 8, 8, 128), bf16),
            pltpu.VMEM((column * 4, 2, 8, 128), bf16),
            pltpu.VMEM((shards, 8, 128), bf16),
            pltpu.VMEM((shards * 8, 128), f32),
            pltpu.VMEM((own_key.shape[1] // HD, kv_rows, 128), bf16),
            pltpu.VMEM((shards, kv_rows, 128), bf16),
            pltpu.VMEM((shards * 16, 128), f32),
            pltpu.VMEM((shards * local_rows, 128), f32),
            pltpu.VMEM((shards * size, 128), f32),
            pltpu.VMEM((size, 128), f32),
            pltpu.VMEM((size, 128), bf16),
            pltpu.VMEM((shards, size, 128), bf16),
            pltpu.VMEM((shards * size, 128), f32),
            pltpu.VMEM((shards * local_rows, width), bf16),
        ]
        + boxes
        + boxes
        + [pltpu.SemaphoreType.DMA((shards,))] * 10,
        compiler_params=pltpu.CompilerParams(
            collective_id=1, has_side_effects=True, vmem_limit_bytes=VMEM_BYTES
        ),
        name="fused_layer",
    )(*operands)
    return mixed.astype(bf16), (mixed + expert_sum).astype(bf16)


def fits_fused(queries, own_key, cache_keys, w_out, expert_ids):
    shards = lax.axis_size("ctx")
    local_rows, width = queries.shape
    return (
        shards % 8 == 0
        and shards & (shards - 1) == 0
        and w_out.shape[0] == HD
        and width == shards * HD
        and w_out.shape[1] == width
        and 2 * local_rows == 8
        and shards % (own_key.shape[1] // HD * 8) == 0
        and shards * local_rows % CAND == 0
        and cache_keys.shape[1] % 16 == 0
    )


def local(*arrays):
    queries, own_key, cache_keys = arrays[0], arrays[1], arrays[3]
    if fits_fused(queries, own_key, cache_keys, arrays[8], arrays[10]):
        return fused_layer(*arrays)
    return staged_layer(*arrays)


def solution(mesh):
    return jax.shard_map(
        local,
        mesh=mesh,
        in_specs=(
            P(("replica", "ctx"), None),
            P(("replica", "ctx"), None),
            P(("replica", "ctx"), None),
            P("replica", "ctx", None),
            P("replica", "ctx", None),
            P("replica"),
            P("replica"),
            P(("replica", "ctx"), None),
            P("ctx", None),
            P(),
            P(("replica", "ctx"), None),
            P(("replica", "ctx"), None),
            P("ctx", None, None),
            P("ctx", None, None),
            P("ctx", None, None),
            P("ctx", None, None),
        ),
        out_specs=(P(("replica", "ctx"), None), P(("replica", "ctx"), None)),
        check_vma=False,
    )
```

```python
import math

import jax
import jax.numpy as jnp
from jax import lax
from jax.experimental import pallas as pl
from jax.experimental.pallas import tpu as pltpu
from jax.sharding import PartitionSpec as P

HD = 128
CAND = 64


NEG = -1e30
EPSILON = 1e-06
VMEM_BYTES = None


def swapped(value, axis, distance):
    return lax.ppermute(value, axis, [(i, i ^ 1 << distance) for i in range(lax.axis_size(axis))])


def dequantize(code_values, scales):
    rows_per = code_values.shape[0] // scales.shape[0]
    cols_per = code_values.shape[1] // scales.shape[1]
    spread = jnp.repeat(jnp.repeat(scales, rows_per, axis=0), cols_per, axis=1)
    return (code_values.astype(jnp.float32) * spread).astype(jnp.bfloat16)


def block_partials(query_heads, key_heads, value_heads, is_valid, score_scale):
    scores = (
        jnp.einsum(
            "brgqd,bstgd->brgqst", query_heads, key_heads, preferred_element_type=jnp.float32
        )
        * score_scale
    )
    valid_full = is_valid[:, None, None, None, :, :]
    masked = jnp.where(valid_full, scores, NEG)
    block_max = jnp.max(masked, axis=-1)
    weights = jnp.where(valid_full, jnp.exp(masked - block_max[..., None]), 0.0)
    block_total = jnp.sum(weights, axis=-1)
    numerator = jnp.einsum(
        "brgqst,bstgd->brgqsd",
        weights.astype(jnp.bfloat16),
        value_heads,
        preferred_element_type=jnp.float32,
    )
    block_out = (numerator / jnp.maximum(block_total, 1.0)[..., None]).astype(jnp.bfloat16)
    return (block_max, block_total, block_out)


def fold_blocks(block_max, block_total, block_out):
    local_top = jnp.max(block_max, axis=-1)
    factor = block_total * jnp.exp(block_max - local_top[..., None])
    numer = jnp.sum(factor[..., None] * block_out.astype(jnp.float32), axis=-2)
    denom = jnp.sum(factor, axis=-1)
    return (local_top, numer, denom)


def merge_pair(first, second):
    top = jnp.maximum(first[0], second[0])
    scale_first = jnp.exp(first[0] - top)
    scale_second = jnp.exp(second[0] - top)
    numer = first[1] * scale_first[..., None] + second[1] * scale_second[..., None]
    denom = first[2] * scale_first + second[2] * scale_second
    return (top, numer, denom)


def flipped(index, pattern, bits):
    total = 0
    for bit in range(bits):
        value = index // (1 << bit) % 2
        if pattern >> bit & 1:
            value = 1 - value
        total = total + value * (1 << bit)
    return total


def greet(me, bits):
    barrier = pltpu.get_barrier_semaphore()
    for bit in range(bits):
        pl.semaphore_signal(
            barrier,
            inc=1,
            device_id={"ctx": flipped(me, 1 << bit, bits)},
            device_id_type=pl.DeviceIdType.MESH,
        )
    pl.semaphore_wait(barrier, bits)


def lane_parts(rows, bits):
    middle = rows // 32 * 16
    first = list(range(bits))
    second = list(range(bits))
    if bits > 2:
        second[1], second[2] = second[2], second[1]
    return ((0, middle, first), (middle, rows - middle, second))


def gather_kernel(bits, block_ref, out_ref, send_sem, recv_sem, own_sem):
    me = lax.axis_index("ctx")
    parts = lane_parts(block_ref.shape[0], bits)
    own = pltpu.make_async_copy(block_ref, out_ref.at[me], own_sem)
    own.start()
    greet(me, bits)
    copies = [{}, {}]
    waited = [set(), set()]
    for step in range(bits):
        for part, (start, size, order) in enumerate(parts):
            bit = order[bits - 1 - step]
            held = [0]
            for earlier in range(step):
                held = held + [p | 1 << order[bits - 1 - earlier] for p in held]
            for pattern in held:
                block = flipped(me, pattern, bits)
                if pattern:
                    if pattern not in waited[part]:
                        copies[part][pattern].wait_recv()
                        waited[part].add(pattern)
                    source = out_ref.at[block, pl.ds(start, size)]
                else:
                    source = block_ref.at[pl.ds(start, size)]
                slot = pattern | 1 << bit
                copy = pltpu.make_async_remote_copy(
                    src_ref=source,
                    dst_ref=out_ref.at[block, pl.ds(start, size)],
                    send_sem=send_sem.at[part, slot],
                    recv_sem=recv_sem.at[part, slot],
                    device_id={"ctx": flipped(me, 1 << bit, bits)},
                    device_id_type=pl.DeviceIdType.MESH,
                )
                copy.start()
                copies[part][slot] = copy
    for part in range(2):
        for slot, copy in copies[part].items():
            if slot not in waited[part]:
                copy.wait_recv()
            copy.wait_send()
    own.wait()


def gather_blocks(block, collective_id):
    shards = lax.axis_size("ctx")
    bits = shards.bit_length() - 1
    return pl.pallas_call(
        lambda *refs: gather_kernel(bits, *refs),
        out_shape=jax.ShapeDtypeStruct((shards,) + block.shape, block.dtype),
        in_specs=[pl.BlockSpec(memory_space=pltpu.VMEM)],
        out_specs=pl.BlockSpec(memory_space=pltpu.VMEM),
        scratch_shapes=[
            pltpu.SemaphoreType.DMA((2, shards)),
            pltpu.SemaphoreType.DMA((2, shards)),
            pltpu.SemaphoreType.DMA,
        ],
        compiler_params=pltpu.CompilerParams(collective_id=collective_id, has_side_effects=True),
        name="gather_blocks",
    )(block)


def scatter_kernel(bits, blocks_ref, out_ref, outbox, inbox, send_sem, recv_sem):
    me = lax.axis_index("ctx")
    shards = 1 << bits
    parts = lane_parts(blocks_ref.shape[1], bits)
    greet(me, bits)
    arrived = [{p: [] for p in range(shards)} for _ in parts]
    pending = [{}, {}]
    finished = [set(), set()]
    sent = []
    next_slot = [0, 0]

    def total(part, pattern):
        start, size, _ = parts[part]
        value = blocks_ref[flipped(me, pattern, bits), pl.ds(start, size), :].astype(jnp.float32)
        for slot in arrived[part][pattern]:
            if slot not in finished[part]:
                pending[part][slot].wait_recv()
                finished[part].add(slot)
            value = value + inbox[slot, pl.ds(start, size), :].astype(jnp.float32)
        return value

    for step in range(bits):
        fresh = []
        for part, (start, size, order) in enumerate(parts):
            bit = order[step]
            done_mask = sum(1 << b for b in order[:step])
            for pattern in range(shards):
                if pattern & done_mask or not pattern >> bit & 1:
                    continue
                slot = next_slot[part]
                next_slot[part] += 1
                if step:
                    outbox[slot, pl.ds(start, size), :] = total(part, pattern).astype(outbox.dtype)
                    source = outbox.at[slot, pl.ds(start, size)]
                else:
                    source = blocks_ref.at[flipped(me, pattern, bits), pl.ds(start, size)]
                copy = pltpu.make_async_remote_copy(
                    src_ref=source,
                    dst_ref=inbox.at[slot, pl.ds(start, size)],
                    send_sem=send_sem.at[part, slot],
                    recv_sem=recv_sem.at[part, slot],
                    device_id={"ctx": flipped(me, 1 << bit, bits)},
                    device_id_type=pl.DeviceIdType.MESH,
                )
                copy.start()
                pending[part][slot] = copy
                sent.append(copy)
                fresh.append((part, pattern ^ 1 << bit, slot))
        for part, pattern, slot in fresh:
            arrived[part][pattern].append(slot)
    for part, (start, size, _) in enumerate(parts):
        out_ref[pl.ds(start, size), :] = total(part, 0)
    for copy in sent:
        copy.wait_send()


def scatter_sum(blocks, collective_id):
    shards = lax.axis_size("ctx")
    bits = shards.bit_length() - 1
    return pl.pallas_call(
        lambda *refs: scatter_kernel(bits, *refs),
        out_shape=jax.ShapeDtypeStruct(blocks.shape[1:], jnp.float32),
        in_specs=[pl.BlockSpec(memory_space=pltpu.VMEM)],
        out_specs=pl.BlockSpec(memory_space=pltpu.VMEM),
        scratch_shapes=[
            pltpu.VMEM(blocks.shape, blocks.dtype),
            pltpu.VMEM(blocks.shape, blocks.dtype),
            pltpu.SemaphoreType.DMA((2, shards)),
            pltpu.SemaphoreType.DMA((2, shards)),
        ],
        compiler_params=pltpu.CompilerParams(collective_id=collective_id, has_side_effects=True),
        name="scatter_sum",
    )(blocks)


def staged_layer(
    queries,
    own_key,
    own_value,
    cache_keys,
    cache_values,
    prefix_of_row,
    context_len,
    hidden_in,
    w_out,
    norm_gain,
    expert_ids,
    route_weights,
    gate_up_codes,
    gate_up_scales,
    down_codes,
    down_scales,
):
    shards = lax.axis_size("ctx")
    device = lax.axis_index("ctx")
    head_size = HD
    local_rows = queries.shape[0]
    key_groups = own_key.shape[1] // head_size
    per_group = queries.shape[1] // own_key.shape[1]
    head_count = key_groups * per_group
    ctx_local = cache_keys.shape[1]
    key_width = cache_keys.shape[2]
    score_scale = 1.0 / math.sqrt(head_size)
    block_prefix = prefix_of_row.reshape(-1, CAND)[:, 0]
    prefix_count = block_prefix.shape[0]
    group_size = CAND // local_rows
    group_bits = group_size.bit_length() - 1
    prefix_bits = (shards // group_size).bit_length() - 1
    group_index = device // group_size
    member = device % group_size
    relay = jnp.concatenate(
        [jnp.take(cache_keys, block_prefix, axis=0), jnp.take(cache_values, block_prefix, axis=0)],
        axis=-1,
    )
    relay_shape = relay.shape
    for bit in range(prefix_bits):
        low = 1 << bit
        view = relay.reshape((relay_shape[0] // (2 * low), 2, low) + relay_shape[1:])
        own_bit = group_index // low % 2
        sent = lax.dynamic_index_in_dim(view, 1 - own_bit, 1, False)
        got = swapped(sent, "ctx", group_bits + bit)
        view = lax.dynamic_update_index_in_dim(view, got, 1 - own_bit, 1)
        relay = view.reshape(relay_shape)
    held = queries
    for bit in range(group_bits):
        other = swapped(held, "ctx", bit)
        upper = device // (1 << bit) % 2
        held = jnp.where(
            upper == 0, jnp.concatenate([held, other], 0), jnp.concatenate([other, held], 0)
        )
    length = jnp.take(context_len, jnp.take(block_prefix, group_index))
    source_block = jnp.arange(prefix_count, dtype=jnp.int32) * group_size + member
    position = source_block[:, None] * ctx_local + jnp.arange(ctx_local, dtype=jnp.int32)[None, :]
    is_valid = (position < length)[None]
    query_heads = held.reshape(1, CAND, key_groups, per_group, head_size)
    key_heads = relay[..., :key_width].reshape(1, prefix_count, ctx_local, key_groups, head_size)
    value_heads = relay[..., key_width:].reshape(1, prefix_count, ctx_local, key_groups, head_size)
    block_max, block_total, block_out = block_partials(
        query_heads, key_heads, value_heads, is_valid, score_scale
    )
    block_max = block_max.reshape(CAND, head_count, prefix_count)
    block_total = block_total.reshape(CAND, head_count, prefix_count)
    block_out = block_out.reshape(CAND, head_count, prefix_count, head_size)
    state = fold_blocks(block_max, block_total, block_out)
    for bit in reversed(range(group_bits)):
        own_bit = device // (1 << bit) % 2
        parts = tuple((item.reshape((2, item.shape[0] // 2) + item.shape[1:]) for item in state))
        sent = tuple((lax.dynamic_index_in_dim(item, 1 - own_bit, 0, False) for item in parts))
        kept = tuple((lax.dynamic_index_in_dim(item, own_bit, 0, False) for item in parts))
        got = swapped(sent, "ctx", bit)
        state = merge_pair(kept, got)
    merged_top, merged_numer, merged_denom = state
    own_heads = queries.reshape(local_rows, key_groups, per_group, head_size)
    own_keys = own_key.reshape(local_rows, key_groups, head_size)
    own_score = (
        jnp.einsum(
            "rgqd,rgd->rgq", own_heads, own_keys, preferred_element_type=jnp.float32
        ).reshape(local_rows, head_count)
        * score_scale
    )
    top_score = jnp.maximum(merged_top, own_score)
    block_scale = jnp.exp(merged_top - top_score)
    own_weight = jnp.exp(own_score - top_score)
    own_term = own_value.reshape(local_rows, key_groups, 1, head_size).astype(
        jnp.float32
    ) * own_weight.reshape(local_rows, key_groups, per_group, 1)
    numerator_all = merged_numer * block_scale[..., None] + own_term.reshape(
        local_rows, head_count, head_size
    )
    denominator = merged_denom * block_scale + own_weight
    attended = (numerator_all / denominator[..., None]).reshape(local_rows, -1).astype(jnp.bfloat16)
    feature_width = hidden_in.shape[1]
    lanes = feature_width // 128
    head_rows = lax.all_to_all(attended, "ctx", split_axis=1, concat_axis=0, tiled=True)
    partial = jnp.dot(head_rows, w_out, preferred_element_type=jnp.float32).astype(jnp.bfloat16)
    projected = scatter_sum(partial.reshape(shards, local_rows * lanes, 128), 1).reshape(
        local_rows, feature_width
    )
    mixed_rows = hidden_in.astype(jnp.float32) + projected
    attention_out = mixed_rows.astype(jnp.bfloat16)
    mean_square = jnp.mean(mixed_rows * mixed_rows, axis=-1, keepdims=True)
    normed = (mixed_rows * lax.rsqrt(mean_square + EPSILON) * norm_gain).astype(jnp.bfloat16)
    experts_all = shards // 2
    chosen = expert_ids[:, :, None] == jnp.arange(experts_all, dtype=jnp.int32)[None, None, :]
    dense = jnp.sum(jnp.where(chosen, route_weights[:, :, None], 0.0), axis=1)
    coarse = lax.reduce_precision(dense, exponent_bits=8, mantissa_bits=7)
    fine = dense - coarse
    weight_cols = jnp.concatenate([coarse, fine], axis=1).astype(jnp.bfloat16)
    weight_lanes = -(-weight_cols.shape[1] // 128)
    weight_cols = jnp.pad(weight_cols, ((0, 0), (0, weight_lanes * 128 - weight_cols.shape[1])))
    weight_block = weight_cols.reshape(local_rows * weight_lanes, 128)
    weight_block = jnp.pad(weight_block, ((0, -weight_block.shape[0] % 16), (0, 0)))
    block = jnp.concatenate([normed.reshape(local_rows * lanes, 128), weight_block], axis=0)
    gate_up = dequantize(gate_up_codes[0], gate_up_scales[0])
    down_proj = dequantize(down_codes[0], down_scales[0])
    half_width = down_proj.shape[0]
    gathered = gather_blocks(block, 2)
    all_rows = shards * local_rows
    flat_rows = gathered[:, : local_rows * lanes].reshape(all_rows, feature_width)
    weight_all = gathered[
        :, local_rows * lanes : local_rows * lanes + local_rows * weight_lanes
    ].reshape(all_rows, weight_lanes * 128)
    column = jnp.arange(weight_lanes * 128, dtype=jnp.int32) % experts_all
    in_use = jnp.arange(weight_lanes * 128, dtype=jnp.int32) < 2 * experts_all
    is_mine = jnp.logical_and(column == device // 2, in_use)
    row_weight = jnp.sum(
        jnp.where(is_mine[None, :], weight_all.astype(jnp.float32), 0.0), axis=1, keepdims=True
    )
    projected_in = jnp.dot(flat_rows, gate_up, preferred_element_type=jnp.float32)
    activated = (jax.nn.silu(projected_in[:, :half_width]) * projected_in[:, half_width:]).astype(
        jnp.bfloat16
    )
    result = jnp.dot(activated, down_proj, preferred_element_type=jnp.float32)
    result = jnp.where(row_weight != 0.0, result * row_weight, 0.0).astype(jnp.bfloat16)
    expert_sum = scatter_sum(result.reshape(shards, local_rows * lanes, 128), 3).reshape(
        local_rows, feature_width
    )
    layer_out = (mixed_rows + expert_sum).astype(jnp.bfloat16)
    return (attention_out, layer_out)


def remote(source, target, send_sem, recv_sem, device):
    copy = pltpu.make_async_remote_copy(
        src_ref=source,
        dst_ref=target,
        send_sem=send_sem,
        recv_sem=recv_sem,
        device_id={"ctx": device},
        device_id_type=pl.DeviceIdType.MESH,
    )
    copy.start()
    return copy


class Place:
    def __init__(self, shards):
        self.shards = shards
        self.bits = shards.bit_length() - 1
        self.column = shards // 8
        self.me = lax.axis_index("ctx")
        self.known = {0: self.me}

    def peer(self, pattern):
        if pattern not in self.known:
            self.known[pattern] = flipped(self.me, pattern, self.bits)
        return self.known[pattern]

    def peers(self):
        return [k * 8 for k in range(1, self.column)] + [2, 4, 6, 1]

    def greet(self):
        barrier = pltpu.get_barrier_semaphore()
        for pattern in self.peers():
            pl.semaphore_signal(
                barrier,
                inc=1,
                device_id={"ctx": self.peer(pattern)},
                device_id_type=pl.DeviceIdType.MESH,
            )

    def met(self):
        pl.semaphore_wait(pltpu.get_barrier_semaphore(), len(self.peers()))


def arrived(ref, sem):
    pltpu.make_async_copy(ref, ref, sem).wait()


def spread(place, column_source, buffer, sems, on_start, on_column, on_plane, on_core, filler):
    send_sem, recv_sem = sems
    column = place.column

    def post(kind, source, target, slot, towards):
        return remote(
            source, target, send_sem.at[kind], recv_sem.at[slot], place.peer(towards)
        )

    def forward(k):
        for plane in (3, 1, 2):
            post(1, buffer.at[k, 0, 0], buffer.at[k, plane, 0], column + k, plane * 2)

    for k in reversed(range(1, column)):
        post(0, column_source(k), buffer.at[k, 0, 0], k, k * 8)
    forward(0)
    on_start()
    on_column(0)
    for k in range(1, column):
        arrived(buffer.at[k, 0, 0], recv_sem.at[k])
        forward(k)
        on_column(k)
    filler()
    for k in range(column):
        arrived(buffer.at[k, pl.ds(1, 3), 0], recv_sem.at[column + k])
        post(2, buffer.at[k, :, 0], buffer.at[k, :, 1], 2 * column + k, 1)
        on_plane(k)
    for k in range(column):
        arrived(buffer.at[k, :, 1], recv_sem.at[2 * column + k])
        on_core(k)
    return [
        (buffer.at[pl.ds(1, column - 1), 0, 0], send_sem.at[0]),
        (buffer.at[:, pl.ds(1, 3), 0], send_sem.at[1]),
        (buffer.at[:, :, 0], send_sem.at[2]),
    ]


class Collect:
    def __init__(self, place, values, size, boxes, sems):
        self.place, self.values, self.size = place, values, size
        self.half = size // 2
        self.core_out, self.core_in, self.plane_out, self.plane_in = boxes[0:4]
        self.column_out, self.column_in = boxes[4:6]
        self.kind = self.core_out.dtype
        self.send_sem, self.recv_sem = sems

    def post(self, kind, slot, out_box, in_box, at, towards):
        remote(
            out_box.at[at],
            in_box.at[at],
            self.send_sem.at[kind],
            self.recv_sem.at[slot],
            self.place.peer(towards),
        )

    def slot(self, kind, half, k):
        return (kind * 2 + half) * self.place.column + k

    def held(self, half, pattern):
        start = self.place.peer(pattern) * self.size + half * self.half
        return self.values[pl.ds(pl.multiple_of(start, self.half), self.half), :]

    def core(self, half):
        for k in reversed(range(self.place.column)):
            for plane in range(4):
                self.core_out[half, k, plane] = self.held(half, k * 8 + plane * 2 + 1).astype(
                    self.kind
                )
            self.post(0, self.slot(0, half, k), self.core_out, self.core_in, (half, k), 1)

    def chip(self, half, k, plane):
        return self.held(half, k * 8 + plane * 2) + self.core_in[half, k, plane].astype(jnp.float32)

    def plane(self, half, k):
        arrived(self.core_in.at[half, k], self.recv_sem.at[self.slot(0, half, k)])
        for plane in (3, 1, 2):
            at = (half, k, plane)
            self.plane_out[at] = self.chip(half, k, plane).astype(self.kind)
            self.post(
                1, self.slot(1, half, k), self.plane_out, self.plane_in, at, plane * 2
            )

    def own(self, half, k):
        total = self.chip(half, k, 0)
        arrived(
            self.plane_in.at[half, k, pl.ds(1, 3)], self.recv_sem.at[self.slot(1, half, k)]
        )
        for plane in (1, 2, 3):
            total = total + self.plane_in[half, k, plane].astype(jnp.float32)
        return total

    def column(self, half, k):
        at = (half, k)
        self.column_out[at] = self.own(half, k).astype(self.kind)
        self.post(
            2, 4 * self.place.column + half, self.column_out, self.column_in, at, k * 8
        )

    def run(self, fill, filler):
        steps = [(half, k) for k in reversed(range(1, self.place.column)) for half in range(2)]
        fill(0)
        self.core(0)
        fill(1)
        self.plane(*steps[0])
        self.core(1)
        for step in steps[1:] + [(0, 0), (1, 0)]:
            self.plane(*step)
        filler()
        for step in steps:
            self.column(*step)
        totals = [self.own(half, 0) for half in range(2)]
        others = pl.ds(1, self.place.column - 1)
        for half in range(2):
            arrived(
                self.column_in.at[half, others], self.recv_sem.at[4 * self.place.column + half]
            )
            for k in range(1, self.place.column):
                totals[half] = totals[half] + self.column_in[half, k].astype(jnp.float32)
        return jnp.concatenate(totals, axis=0), [
            (self.core_out, self.send_sem.at[0]),
            (self.plane_out.at[:, :, pl.ds(1, 3)], self.send_sem.at[1]),
            (self.column_out.at[:, others], self.send_sem.at[2]),
        ]


def layer_kernel(
    shards,
    per_block,
    *refs,
):
    given, (mixed_out, expert_out), refs = refs[:16], refs[16:18], refs[18:]
    held, load_sem = refs[:16], refs[16]
    (
        prefix_ref,
        length_ref,
        keys_ref,
        values_ref,
        own_key_ref,
        own_value_ref,
        queries_ref,
        ids_ref,
        route_ref,
        w_out_ref,
        gate_ref,
        gate_scale_ref,
        down_ref,
        down_scale_ref,
        hidden_ref,
        gain_ref,
    ) = held
    (
        stage,
        q_send,
        q_column,
        q_plane,
        q_core,
        q_wide,
        kv_send,
        kv_all,
        own_wide,
        attended,
        partial,
        mixed_ref,
        normed_all,
        rows_wide,
        rows_ref,
    ) = refs[17 : 17 + 15]
    boxes_and_sems = refs[17 + 15 :]
    first_boxes, second_boxes = boxes_and_sems[0:6], boxes_and_sems[6:12]
    sems = boxes_and_sems[12:]
    q_sems, kv_sems, first_sems, row_sems, second_sems = [sems[2 * i : 2 * i + 2] for i in range(5)]
    place = Place(shards)
    me = place.me
    local_rows, width = queries_ref.shape
    lanes = width // 128
    size = local_rows * lanes
    prefixes, positions, _ = keys_ref.shape
    blocks = shards // per_block
    span = blocks * positions
    key_groups = own_key_ref.shape[1] // HD
    per_group = shards // key_groups
    score_scale = 1.0 / math.sqrt(HD)
    f32 = jnp.float32
    half_lanes = lanes // 2

    def lane_at(i):
        return i // half_lanes * (size // 2) + i % half_lanes


    place.greet()
    loads = []
    for i, (source, target) in enumerate(zip(given, held)):
        load = pltpu.make_async_copy(source, target, load_sem.at[i])
        load.start()
        loads.append(load)
    for load in loads[:9]:
        load.wait()

    lengths = []
    for b in range(blocks):
        prefix = prefix_ref[b * per_block * local_rows]
        length = length_ref[0]
        for p in range(1, prefixes):
            length = jnp.where(prefix == p, length_ref[p], length)
        lengths.append(length)
        prefix_of = jnp.full((positions, keys_ref.shape[2]), prefix, jnp.int32)
        for which, ref in enumerate((keys_ref, values_ref)):
            chosen = ref[0].astype(f32)
            for p in range(1, prefixes):
                chosen = jnp.where(prefix_of == p, ref[p].astype(f32), chosen)
            at = which * span + b * positions
            for g in range(key_groups):
                kv_send[g, at : at + positions, :] = chosen[:, g * HD : (g + 1) * HD].astype(
                    jnp.bfloat16
                )
    stage[...] = jnp.zeros((16, HD), f32)
    lane = lax.broadcasted_iota(jnp.int32, (local_rows, 128), 1)
    dense = jnp.zeros((local_rows, 128), f32)
    for choice in range(ids_ref.shape[1]):
        dense = dense + jnp.where(
            lane % 64 == ids_ref[:, choice : choice + 1], route_ref[:, choice : choice + 1], 0.0
        )
    coarse = dense.astype(jnp.bfloat16).astype(f32)
    stage[local_rows : 2 * local_rows, :] = jnp.where(lane < 64, coarse, dense - coarse)
    for g in range(key_groups):
        cut = slice(g * HD, (g + 1) * HD)
        stage[0:local_rows, :] = own_key_ref[:, cut].astype(f32)
        stage[8 : 8 + local_rows, :] = own_value_ref[:, cut].astype(f32)
        kv_send[g, 2 * span : 2 * span + 16, :] = stage[...].astype(jnp.bfloat16)
    for d in range(shards):
        q_send[d] = queries_ref[:, d * HD : (d + 1) * HD]
    place.met()

    column = place.column

    def q_post(kind, source, target, slot, towards):
        remote(source, target, q_sems[0].at[kind], q_sems[1].at[slot], place.peer(towards))

    def q_start():
        for k in reversed(range(1, column)):
            first = place.peer(k * 8) // 8 * 8
            q_post(0, q_send.at[pl.ds(first, 8)], q_column.at[k], k, k * 8)
        q_column[0] = q_send[pl.ds(me // 8 * 8, 8)]

    def q_on_column(k):
        if k:
            arrived(q_column.at[k], q_sems[1].at[k])
        for plane in (3, 1, 2):
            first = place.peer(plane * 2) % 8 // 2 * 2
            source = (q_column.at[k] if k else q_send).at[
                pl.ds(first + (0 if k else me // 8 * 8), 2)
            ]
            q_post(1, source, q_plane.at[k, plane], column + k, plane * 2)
        q_plane[k, 0] = q_column[k, pl.ds(me % 8 // 2 * 2, 2)]

    def q_on_plane(k):
        arrived(q_plane.at[k, pl.ds(1, 3)], q_sems[1].at[column + k])
        q_post(2, q_plane.at[k, :, place.peer(1) % 2], q_core.at[k], 2 * column, 1)

    my_group = me // per_group

    def dequantize_gate():
        loads[10].wait()
        loads[11].wait()

        def block_row(i, carry):
            at = pl.ds(pl.multiple_of(i * 128, 128), 128)
            for j in range(gate_ref.shape[1] // 128):
                cut = slice(j * 128, (j + 1) * 128)
                wide = gate_ref[at, cut].astype(f32) * gate_scale_ref[j, 0, i]
                gate_ref[at, cut] = wide.astype(jnp.bfloat16)
            return carry

        lax.fori_loop(0, gate_ref.shape[0] // 128, block_row, 0)

    def dequantize_down():
        loads[12].wait()
        loads[13].wait()

        def block_column(j, carry):
            at = pl.ds(pl.multiple_of(j * 128, 128), 128)
            for i in range(down_ref.shape[0] // 128):
                cut = slice(i * 128, (i + 1) * 128)
                wide = down_ref[cut, at].astype(f32) * down_scale_ref[i, 0, j]
                down_ref[cut, at] = wide.astype(jnp.bfloat16)
            return carry

        lax.fori_loop(0, down_ref.shape[1] // 128, block_column, 0)

    kv_all[0, 0, 0] = kv_send[my_group]
    waits = spread(
        place,
        lambda k: kv_send.at[place.peer(k * 8) // per_group],
        kv_all,
        kv_sems,
        q_start,
        q_on_column,
        q_on_plane,
        lambda k: None,
        dequantize_gate,
    )

    waits = waits + [
        (q_column.at[pl.ds(1, column - 1)], q_sems[0].at[0]),
        (q_plane.at[:, pl.ds(1, 3)], q_sems[0].at[1]),
        (q_core, q_sems[0].at[2]),
    ]
    arrived(q_core, q_sems[1].at[2 * column])
    for k in range(column):
        for plane in range(4):
            for core, block in ((0, q_plane[k, plane, me % 2]), (1, q_core[k, plane])):
                device = place.peer(k * 8 + plane * 2 + core)
                q_wide[pl.ds(pl.multiple_of(device * 8, 8), local_rows), :] = block.astype(f32)
                own_wide[pl.ds(pl.multiple_of(device * 16, 16), 16), :] = kv_all[
                    k, plane, core, 2 * span : 2 * span + 16
                ].astype(f32)
    total_positions = shards * positions
    counted = lax.broadcasted_iota(jnp.int32, (1, total_positions), 1)
    position = (counted // positions ^ me) * positions + counted % positions

    def picked(ref, start, count, stride):
        return jnp.concatenate(
            [ref[pl.ds(start + r, count, stride=stride), :] for r in range(local_rows)], axis=0
        )

    for b in range(blocks):
        first = b * per_block
        key_at, value_at = b * positions, span + b * positions
        key = kv_all[:, :, :, key_at : key_at + positions, :].reshape(total_positions, HD)
        value = kv_all[:, :, :, value_at : value_at + positions, :].reshape(total_positions, HD)
        query = picked(q_wide, first * 8, per_block, 8)
        own_k = picked(own_wide, first * 16, per_block, 16)
        own_v = picked(own_wide, first * 16 + 8, per_block, 16)
        scores = lax.dot_general(
            query.astype(jnp.bfloat16), key, (((1,), (1,)), ((), ())), preferred_element_type=f32
        )
        is_valid = position < lengths[b]
        scores = jnp.where(is_valid, scores * score_scale, NEG)
        own_score = jnp.sum(query * own_k, axis=1, keepdims=True) * score_scale
        top = jnp.maximum(jnp.max(scores, axis=1, keepdims=True), own_score)
        weights = jnp.where(is_valid, jnp.exp(scores - top), 0.0)
        own_weight = jnp.exp(own_score - top)
        denominator = jnp.sum(weights, axis=1, keepdims=True) + own_weight
        numerator = jnp.dot(weights.astype(jnp.bfloat16), value, preferred_element_type=f32)
        result = (numerator + own_weight * own_v) / denominator
        for r in range(local_rows):
            attended[r * shards + first : r * shards + first + per_block, :] = result[
                r * per_block : (r + 1) * per_block, :
            ]

    def multiply_out(rows, matrix_ref, half):
        for first in range(half * width // 2, (half + 1) * width // 2, 512):
            result = jnp.dot(
                rows, matrix_ref[:, first : first + 512], preferred_element_type=f32
            )
            for i in range(4):
                for r in range(local_rows):
                    start = lane_at(first // 128 + i) + r * half_lanes
                    partial[pl.ds(start, shards, stride=size), :] = result[
                        r * shards : (r + 1) * shards, i * 128 : (i + 1) * 128
                    ]

    loads[9].wait()
    head_rows = attended[...].astype(jnp.bfloat16)
    total = Collect(place, partial, size, first_boxes, first_sems)
    projected, more = total.run(
        lambda half: multiply_out(head_rows, w_out_ref, half), dequantize_down
    )
    waits = waits + more

    loads[14].wait()
    loads[15].wait()
    for i in range(lanes):
        mixed_ref[pl.ds(lane_at(i), local_rows, stride=half_lanes), :] = hidden_ref[
            :, i * 128 : (i + 1) * 128
        ].astype(f32)
    mixed = mixed_ref[...] + projected
    mixed_ref[...] = mixed
    grouped = mixed.reshape(2, local_rows, half_lanes, 128)
    squares = jnp.sum(grouped * grouped, axis=2, keepdims=True)
    squares = jnp.sum(jnp.sum(squares, axis=0, keepdims=True), axis=3, keepdims=True)
    gain = gain_ref[...].reshape(2, 1, half_lanes, 128)
    normed = grouped * lax.rsqrt(squares / width + EPSILON) * gain
    normed_all[0, 0, 0] = normed.reshape(size, 128).astype(jnp.bfloat16)

    def widen(k, core):
        for plane in range(4):
            device = place.peer(k * 8 + plane * 2 + core)
            at = pl.ds(pl.multiple_of(device * size, size), size)
            rows_wide[at, :] = normed_all[k, plane, core].astype(f32)

    def write_attention():
        for i in range(lanes):
            mixed_out[:, i * 128 : (i + 1) * 128] = mixed_ref[
                pl.ds(lane_at(i), local_rows, stride=half_lanes), :
            ]

    more = spread(
        place,
        lambda k: normed_all.at[0, 0, 0],
        normed_all,
        row_sems,
        lambda: None,
        lambda k: None,
        lambda k: widen(k, 0),
        lambda k: widen(k, 1),
        write_attention,
    )
    waits = waits + more
    for i in range(lanes):
        for r in range(local_rows):
            rows_ref[r * shards : (r + 1) * shards, i * 128 : (i + 1) * 128] = rows_wide[
                pl.ds(lane_at(i) + r * half_lanes, shards, stride=size), :
            ].astype(jnp.bfloat16)
    half = down_ref.shape[0]
    projected_in = jnp.dot(rows_ref[...], gate_ref[...], preferred_element_type=f32)
    split = picked(own_wide, local_rows, shards, 16)
    lane = lax.broadcasted_iota(jnp.int32, split.shape, 1)
    weight = jnp.sum(jnp.where(lane % 64 == me // 2, split, 0.0), axis=1, keepdims=True)
    gate = projected_in[:, :half]
    activated = gate / (1.0 + jnp.exp(-gate)) * projected_in[:, half:]
    activated = jnp.where(weight != 0.0, activated * weight, 0.0).astype(jnp.bfloat16)
    total = Collect(place, partial, size, second_boxes, second_sems)
    expert_sum, more = total.run(
        lambda half: multiply_out(activated, down_ref, half), lambda: None
    )
    waits = waits + more
    mixed_ref[...] = expert_sum
    for i in range(lanes):
        expert_out[:, i * 128 : (i + 1) * 128] = mixed_ref[pl.ds(lane_at(i), local_rows, stride=half_lanes), :]
    for ref, sem in waits:
        arrived(ref, sem)


def fused_layer(
    queries,
    own_key,
    own_value,
    cache_keys,
    cache_values,
    prefix_of_row,
    context_len,
    hidden_in,
    w_out,
    norm_gain,
    expert_ids,
    route_weights,
    gate_up_codes,
    gate_up_scales,
    down_codes,
    down_scales,
):
    shards = lax.axis_size("ctx")
    local_rows, width = queries.shape
    lanes = width // 128
    size = local_rows * lanes
    span = shards * local_rows // CAND * cache_keys.shape[1]
    column = shards // 8
    bf16, f32 = jnp.bfloat16, jnp.float32
    kv_rows = 2 * span + 16
    half = size // 2
    boxes = [
        pltpu.VMEM(shape, bf16)
        for shape in (
            (2, column, 4, half, 128),
            (2, column, 4, half, 128),
            (2, column, 4, half, 128),
            (2, column, 4, half, 128),
            (2, column, half, 128),
            (2, column, half, 128),
        )
    ]
    operands = (
        prefix_of_row,
        context_len,
        cache_keys,
        cache_values,
        own_key,
        own_value,
        queries,
        expert_ids,
        route_weights,
        w_out,
        gate_up_codes[0],
        gate_up_scales.transpose(2, 0, 1),
        down_codes[0],
        down_scales.transpose(1, 0, 2),
        hidden_in,
        norm_gain.reshape(lanes, 128),
    )
    scalars = (0, 1, 11, 13)
    out = jax.ShapeDtypeStruct((local_rows, width), f32)
    vmem = pl.BlockSpec(memory_space=pltpu.VMEM)
    mixed, expert_sum = pl.pallas_call(
        lambda *refs: layer_kernel(shards, CAND // local_rows, *refs),
        out_shape=(out, out),
        in_specs=[pl.BlockSpec(memory_space=pltpu.HBM)] * len(operands),
        out_specs=(vmem, vmem),
        scratch_shapes=[
            (pltpu.SMEM if i in scalars else pltpu.VMEM)(x.shape, x.dtype)
            for i, x in enumerate(operands)
        ]
        + [
            pltpu.SemaphoreType.DMA((len(operands),)),
            pltpu.VMEM((16, 128), f32),
            pltpu.VMEM((shards, local_rows, 128), bf16),
            pltpu.VMEM((column, 8, local_rows, 128), bf16),
            pltpu.VMEM((column, 4, 2, local_rows, 128), bf16),
            pltpu.VMEM((column, 4, local_rows, 128), bf16),
            pltpu.VMEM((shards * 8, 128), f32),
            pltpu.VMEM((own_key.shape[1] // HD, kv_rows, 128), bf16),
            pltpu.VMEM((column, 4, 2, kv_rows, 128), bf16),
            pltpu.VMEM((shards * 16, 128), f32),
            pltpu.VMEM((shards * local_rows, 128), f32),
            pltpu.VMEM((shards * size, 128), f32),
            pltpu.VMEM((size, 128), f32),
            pltpu.VMEM((column, 4, 2, size, 128), bf16),
            pltpu.VMEM((shards * size, 128), f32),
            pltpu.VMEM((shards * local_rows, width), bf16),
        ]
        + boxes
        + boxes
        + [pltpu.SemaphoreType.DMA((count,)) for count in (3, 4 * column + 2) * 5],
        compiler_params=pltpu.CompilerParams(
            collective_id=1, has_side_effects=True, vmem_limit_bytes=VMEM_BYTES
        ),
        name="fused_layer",
    )(*operands)
    return mixed.astype(bf16), (mixed + expert_sum).astype(bf16)


def fits_fused(queries, own_key, cache_keys, w_out, expert_ids):
    shards = lax.axis_size("ctx")
    local_rows, width = queries.shape
    return (
        shards % 8 == 0
        and shards & (shards - 1) == 0
        and w_out.shape[0] == HD
        and width == shards * HD
        and w_out.shape[1] == width
        and local_rows == 4
        and width % (256 * 16) == 0
        and shards // 2 <= 64
        and shards % (own_key.shape[1] // HD * 8) == 0
        and shards * local_rows % CAND == 0
        and cache_keys.shape[1] % 16 == 0
    )


def local(*arrays):
    queries, own_key, cache_keys = arrays[0], arrays[1], arrays[3]
    if fits_fused(queries, own_key, cache_keys, arrays[8], arrays[10]):
        return fused_layer(*arrays)
    return staged_layer(*arrays)


def solution(mesh):
    return jax.shard_map(
        local,
        mesh=mesh,
        in_specs=(
            P(("replica", "ctx"), None),
            P(("replica", "ctx"), None),
            P(("replica", "ctx"), None),
            P("replica", "ctx", None),
            P("replica", "ctx", None),
            P("replica"),
            P("replica"),
            P(("replica", "ctx"), None),
            P("ctx", None),
            P(),
            P(("replica", "ctx"), None),
            P(("replica", "ctx"), None),
            P("ctx", None, None),
            P("ctx", None, None),
            P("ctx", None, None),
            P("ctx", None, None),
        ),
        out_specs=(P(("replica", "ctx"), None), P(("replica", "ctx"), None)),
        check_vma=False,
    )
```

```python
import math

import jax
import jax.numpy as jnp
from jax import lax
from jax.experimental import pallas as pl
from jax.experimental.pallas import tpu as pltpu
from jax.sharding import PartitionSpec as P

HD = 128
CAND = 64


NEG = -1e30
EPSILON = 1e-06
VMEM_BYTES = None


def swapped(value, axis, distance):
    return lax.ppermute(value, axis, [(i, i ^ 1 << distance) for i in range(lax.axis_size(axis))])


def dequantize(code_values, scales):
    rows_per = code_values.shape[0] // scales.shape[0]
    cols_per = code_values.shape[1] // scales.shape[1]
    spread = jnp.repeat(jnp.repeat(scales, rows_per, axis=0), cols_per, axis=1)
    return (code_values.astype(jnp.float32) * spread).astype(jnp.bfloat16)


def block_partials(query_heads, key_heads, value_heads, is_valid, score_scale):
    scores = (
        jnp.einsum(
            "brgqd,bstgd->brgqst", query_heads, key_heads, preferred_element_type=jnp.float32
        )
        * score_scale
    )
    valid_full = is_valid[:, None, None, None, :, :]
    masked = jnp.where(valid_full, scores, NEG)
    block_max = jnp.max(masked, axis=-1)
    weights = jnp.where(valid_full, jnp.exp(masked - block_max[..., None]), 0.0)
    block_total = jnp.sum(weights, axis=-1)
    numerator = jnp.einsum(
        "brgqst,bstgd->brgqsd",
        weights.astype(jnp.bfloat16),
        value_heads,
        preferred_element_type=jnp.float32,
    )
    block_out = (numerator / jnp.maximum(block_total, 1.0)[..., None]).astype(jnp.bfloat16)
    return (block_max, block_total, block_out)


def fold_blocks(block_max, block_total, block_out):
    local_top = jnp.max(block_max, axis=-1)
    factor = block_total * jnp.exp(block_max - local_top[..., None])
    numer = jnp.sum(factor[..., None] * block_out.astype(jnp.float32), axis=-2)
    denom = jnp.sum(factor, axis=-1)
    return (local_top, numer, denom)


def merge_pair(first, second):
    top = jnp.maximum(first[0], second[0])
    scale_first = jnp.exp(first[0] - top)
    scale_second = jnp.exp(second[0] - top)
    numer = first[1] * scale_first[..., None] + second[1] * scale_second[..., None]
    denom = first[2] * scale_first + second[2] * scale_second
    return (top, numer, denom)


def flipped(index, pattern, bits):
    total = 0
    for bit in range(bits):
        value = index // (1 << bit) % 2
        if pattern >> bit & 1:
            value = 1 - value
        total = total + value * (1 << bit)
    return total


def greet(me, bits):
    barrier = pltpu.get_barrier_semaphore()
    for bit in range(bits):
        pl.semaphore_signal(
            barrier,
            inc=1,
            device_id={"ctx": flipped(me, 1 << bit, bits)},
            device_id_type=pl.DeviceIdType.MESH,
        )
    pl.semaphore_wait(barrier, bits)


def lane_parts(rows, bits):
    middle = rows // 32 * 16
    first = list(range(bits))
    second = list(range(bits))
    if bits > 2:
        second[1], second[2] = second[2], second[1]
    return ((0, middle, first), (middle, rows - middle, second))


def gather_kernel(bits, block_ref, out_ref, send_sem, recv_sem, own_sem):
    me = lax.axis_index("ctx")
    parts = lane_parts(block_ref.shape[0], bits)
    own = pltpu.make_async_copy(block_ref, out_ref.at[me], own_sem)
    own.start()
    greet(me, bits)
    copies = [{}, {}]
    waited = [set(), set()]
    for step in range(bits):
        for part, (start, size, order) in enumerate(parts):
            bit = order[bits - 1 - step]
            held = [0]
            for earlier in range(step):
                held = held + [p | 1 << order[bits - 1 - earlier] for p in held]
            for pattern in held:
                block = flipped(me, pattern, bits)
                if pattern:
                    if pattern not in waited[part]:
                        copies[part][pattern].wait_recv()
                        waited[part].add(pattern)
                    source = out_ref.at[block, pl.ds(start, size)]
                else:
                    source = block_ref.at[pl.ds(start, size)]
                slot = pattern | 1 << bit
                copy = pltpu.make_async_remote_copy(
                    src_ref=source,
                    dst_ref=out_ref.at[block, pl.ds(start, size)],
                    send_sem=send_sem.at[part, slot],
                    recv_sem=recv_sem.at[part, slot],
                    device_id={"ctx": flipped(me, 1 << bit, bits)},
                    device_id_type=pl.DeviceIdType.MESH,
                )
                copy.start()
                copies[part][slot] = copy
    for part in range(2):
        for slot, copy in copies[part].items():
            if slot not in waited[part]:
                copy.wait_recv()
            copy.wait_send()
    own.wait()


def gather_blocks(block, collective_id):
    shards = lax.axis_size("ctx")
    bits = shards.bit_length() - 1
    return pl.pallas_call(
        lambda *refs: gather_kernel(bits, *refs),
        out_shape=jax.ShapeDtypeStruct((shards,) + block.shape, block.dtype),
        in_specs=[pl.BlockSpec(memory_space=pltpu.VMEM)],
        out_specs=pl.BlockSpec(memory_space=pltpu.VMEM),
        scratch_shapes=[
            pltpu.SemaphoreType.DMA((2, shards)),
            pltpu.SemaphoreType.DMA((2, shards)),
            pltpu.SemaphoreType.DMA,
        ],
        compiler_params=pltpu.CompilerParams(collective_id=collective_id, has_side_effects=True),
        name="gather_blocks",
    )(block)


def scatter_kernel(bits, blocks_ref, out_ref, outbox, inbox, send_sem, recv_sem):
    me = lax.axis_index("ctx")
    shards = 1 << bits
    parts = lane_parts(blocks_ref.shape[1], bits)
    greet(me, bits)
    arrived = [{p: [] for p in range(shards)} for _ in parts]
    pending = [{}, {}]
    finished = [set(), set()]
    sent = []
    next_slot = [0, 0]

    def total(part, pattern):
        start, size, _ = parts[part]
        value = blocks_ref[flipped(me, pattern, bits), pl.ds(start, size), :].astype(jnp.float32)
        for slot in arrived[part][pattern]:
            if slot not in finished[part]:
                pending[part][slot].wait_recv()
                finished[part].add(slot)
            value = value + inbox[slot, pl.ds(start, size), :].astype(jnp.float32)
        return value

    for step in range(bits):
        fresh = []
        for part, (start, size, order) in enumerate(parts):
            bit = order[step]
            done_mask = sum(1 << b for b in order[:step])
            for pattern in range(shards):
                if pattern & done_mask or not pattern >> bit & 1:
                    continue
                slot = next_slot[part]
                next_slot[part] += 1
                if step:
                    outbox[slot, pl.ds(start, size), :] = total(part, pattern).astype(outbox.dtype)
                    source = outbox.at[slot, pl.ds(start, size)]
                else:
                    source = blocks_ref.at[flipped(me, pattern, bits), pl.ds(start, size)]
                copy = pltpu.make_async_remote_copy(
                    src_ref=source,
                    dst_ref=inbox.at[slot, pl.ds(start, size)],
                    send_sem=send_sem.at[part, slot],
                    recv_sem=recv_sem.at[part, slot],
                    device_id={"ctx": flipped(me, 1 << bit, bits)},
                    device_id_type=pl.DeviceIdType.MESH,
                )
                copy.start()
                pending[part][slot] = copy
                sent.append(copy)
                fresh.append((part, pattern ^ 1 << bit, slot))
        for part, pattern, slot in fresh:
            arrived[part][pattern].append(slot)
    for part, (start, size, _) in enumerate(parts):
        out_ref[pl.ds(start, size), :] = total(part, 0)
    for copy in sent:
        copy.wait_send()


def scatter_sum(blocks, collective_id):
    shards = lax.axis_size("ctx")
    bits = shards.bit_length() - 1
    return pl.pallas_call(
        lambda *refs: scatter_kernel(bits, *refs),
        out_shape=jax.ShapeDtypeStruct(blocks.shape[1:], jnp.float32),
        in_specs=[pl.BlockSpec(memory_space=pltpu.VMEM)],
        out_specs=pl.BlockSpec(memory_space=pltpu.VMEM),
        scratch_shapes=[
            pltpu.VMEM(blocks.shape, blocks.dtype),
            pltpu.VMEM(blocks.shape, blocks.dtype),
            pltpu.SemaphoreType.DMA((2, shards)),
            pltpu.SemaphoreType.DMA((2, shards)),
        ],
        compiler_params=pltpu.CompilerParams(collective_id=collective_id, has_side_effects=True),
        name="scatter_sum",
    )(blocks)


def staged_layer(
    queries,
    own_key,
    own_value,
    cache_keys,
    cache_values,
    prefix_of_row,
    context_len,
    hidden_in,
    w_out,
    norm_gain,
    expert_ids,
    route_weights,
    gate_up_codes,
    gate_up_scales,
    down_codes,
    down_scales,
):
    shards = lax.axis_size("ctx")
    device = lax.axis_index("ctx")
    head_size = HD
    local_rows = queries.shape[0]
    key_groups = own_key.shape[1] // head_size
    per_group = queries.shape[1] // own_key.shape[1]
    head_count = key_groups * per_group
    ctx_local = cache_keys.shape[1]
    key_width = cache_keys.shape[2]
    score_scale = 1.0 / math.sqrt(head_size)
    block_prefix = prefix_of_row.reshape(-1, CAND)[:, 0]
    prefix_count = block_prefix.shape[0]
    group_size = CAND // local_rows
    group_bits = group_size.bit_length() - 1
    prefix_bits = (shards // group_size).bit_length() - 1
    group_index = device // group_size
    member = device % group_size
    relay = jnp.concatenate(
        [jnp.take(cache_keys, block_prefix, axis=0), jnp.take(cache_values, block_prefix, axis=0)],
        axis=-1,
    )
    relay_shape = relay.shape
    for bit in range(prefix_bits):
        low = 1 << bit
        view = relay.reshape((relay_shape[0] // (2 * low), 2, low) + relay_shape[1:])
        own_bit = group_index // low % 2
        sent = lax.dynamic_index_in_dim(view, 1 - own_bit, 1, False)
        got = swapped(sent, "ctx", group_bits + bit)
        view = lax.dynamic_update_index_in_dim(view, got, 1 - own_bit, 1)
        relay = view.reshape(relay_shape)
    held = queries
    for bit in range(group_bits):
        other = swapped(held, "ctx", bit)
        upper = device // (1 << bit) % 2
        held = jnp.where(
            upper == 0, jnp.concatenate([held, other], 0), jnp.concatenate([other, held], 0)
        )
    length = jnp.take(context_len, jnp.take(block_prefix, group_index))
    source_block = jnp.arange(prefix_count, dtype=jnp.int32) * group_size + member
    position = source_block[:, None] * ctx_local + jnp.arange(ctx_local, dtype=jnp.int32)[None, :]
    is_valid = (position < length)[None]
    query_heads = held.reshape(1, CAND, key_groups, per_group, head_size)
    key_heads = relay[..., :key_width].reshape(1, prefix_count, ctx_local, key_groups, head_size)
    value_heads = relay[..., key_width:].reshape(1, prefix_count, ctx_local, key_groups, head_size)
    block_max, block_total, block_out = block_partials(
        query_heads, key_heads, value_heads, is_valid, score_scale
    )
    block_max = block_max.reshape(CAND, head_count, prefix_count)
    block_total = block_total.reshape(CAND, head_count, prefix_count)
    block_out = block_out.reshape(CAND, head_count, prefix_count, head_size)
    state = fold_blocks(block_max, block_total, block_out)
    for bit in reversed(range(group_bits)):
        own_bit = device // (1 << bit) % 2
        parts = tuple((item.reshape((2, item.shape[0] // 2) + item.shape[1:]) for item in state))
        sent = tuple((lax.dynamic_index_in_dim(item, 1 - own_bit, 0, False) for item in parts))
        kept = tuple((lax.dynamic_index_in_dim(item, own_bit, 0, False) for item in parts))
        got = swapped(sent, "ctx", bit)
        state = merge_pair(kept, got)
    merged_top, merged_numer, merged_denom = state
    own_heads = queries.reshape(local_rows, key_groups, per_group, head_size)
    own_keys = own_key.reshape(local_rows, key_groups, head_size)
    own_score = (
        jnp.einsum(
            "rgqd,rgd->rgq", own_heads, own_keys, preferred_element_type=jnp.float32
        ).reshape(local_rows, head_count)
        * score_scale
    )
    top_score = jnp.maximum(merged_top, own_score)
    block_scale = jnp.exp(merged_top - top_score)
    own_weight = jnp.exp(own_score - top_score)
    own_term = own_value.reshape(local_rows, key_groups, 1, head_size).astype(
        jnp.float32
    ) * own_weight.reshape(local_rows, key_groups, per_group, 1)
    numerator_all = merged_numer * block_scale[..., None] + own_term.reshape(
        local_rows, head_count, head_size
    )
    denominator = merged_denom * block_scale + own_weight
    attended = (numerator_all / denominator[..., None]).reshape(local_rows, -1).astype(jnp.bfloat16)
    feature_width = hidden_in.shape[1]
    lanes = feature_width // 128
    head_rows = lax.all_to_all(attended, "ctx", split_axis=1, concat_axis=0, tiled=True)
    partial = jnp.dot(head_rows, w_out, preferred_element_type=jnp.float32).astype(jnp.bfloat16)
    projected = scatter_sum(partial.reshape(shards, local_rows * lanes, 128), 1).reshape(
        local_rows, feature_width
    )
    mixed_rows = hidden_in.astype(jnp.float32) + projected
    attention_out = mixed_rows.astype(jnp.bfloat16)
    mean_square = jnp.mean(mixed_rows * mixed_rows, axis=-1, keepdims=True)
    normed = (mixed_rows * lax.rsqrt(mean_square + EPSILON) * norm_gain).astype(jnp.bfloat16)
    experts_all = shards // 2
    chosen = expert_ids[:, :, None] == jnp.arange(experts_all, dtype=jnp.int32)[None, None, :]
    dense = jnp.sum(jnp.where(chosen, route_weights[:, :, None], 0.0), axis=1)
    coarse = lax.reduce_precision(dense, exponent_bits=8, mantissa_bits=7)
    fine = dense - coarse
    weight_cols = jnp.concatenate([coarse, fine], axis=1).astype(jnp.bfloat16)
    weight_lanes = -(-weight_cols.shape[1] // 128)
    weight_cols = jnp.pad(weight_cols, ((0, 0), (0, weight_lanes * 128 - weight_cols.shape[1])))
    weight_block = weight_cols.reshape(local_rows * weight_lanes, 128)
    weight_block = jnp.pad(weight_block, ((0, -weight_block.shape[0] % 16), (0, 0)))
    block = jnp.concatenate([normed.reshape(local_rows * lanes, 128), weight_block], axis=0)
    gate_up = dequantize(gate_up_codes[0], gate_up_scales[0])
    down_proj = dequantize(down_codes[0], down_scales[0])
    half_width = down_proj.shape[0]
    gathered = gather_blocks(block, 2)
    all_rows = shards * local_rows
    flat_rows = gathered[:, : local_rows * lanes].reshape(all_rows, feature_width)
    weight_all = gathered[
        :, local_rows * lanes : local_rows * lanes + local_rows * weight_lanes
    ].reshape(all_rows, weight_lanes * 128)
    column = jnp.arange(weight_lanes * 128, dtype=jnp.int32) % experts_all
    in_use = jnp.arange(weight_lanes * 128, dtype=jnp.int32) < 2 * experts_all
    is_mine = jnp.logical_and(column == device // 2, in_use)
    row_weight = jnp.sum(
        jnp.where(is_mine[None, :], weight_all.astype(jnp.float32), 0.0), axis=1, keepdims=True
    )
    projected_in = jnp.dot(flat_rows, gate_up, preferred_element_type=jnp.float32)
    activated = (jax.nn.silu(projected_in[:, :half_width]) * projected_in[:, half_width:]).astype(
        jnp.bfloat16
    )
    result = jnp.dot(activated, down_proj, preferred_element_type=jnp.float32)
    result = jnp.where(row_weight != 0.0, result * row_weight, 0.0).astype(jnp.bfloat16)
    expert_sum = scatter_sum(result.reshape(shards, local_rows * lanes, 128), 3).reshape(
        local_rows, feature_width
    )
    layer_out = (mixed_rows + expert_sum).astype(jnp.bfloat16)
    return (attention_out, layer_out)


def remote(source, target, send_sem, recv_sem, device):
    copy = pltpu.make_async_remote_copy(
        src_ref=source,
        dst_ref=target,
        send_sem=send_sem,
        recv_sem=recv_sem,
        device_id={"ctx": device},
        device_id_type=pl.DeviceIdType.MESH,
    )
    copy.start()
    return copy


class Place:
    def __init__(self, shards):
        self.shards = shards
        self.bits = shards.bit_length() - 1
        self.column = shards // 8
        self.me = lax.axis_index("ctx")
        self.known = {0: self.me}

    def peer(self, pattern):
        if pattern not in self.known:
            self.known[pattern] = flipped(self.me, pattern, self.bits)
        return self.known[pattern]

    def peers(self):
        return [k * 8 for k in range(1, self.column)] + [2, 4, 6, 1]

    def greet(self):
        barrier = pltpu.get_barrier_semaphore()
        for pattern in self.peers():
            pl.semaphore_signal(
                barrier,
                inc=1,
                device_id={"ctx": self.peer(pattern)},
                device_id_type=pl.DeviceIdType.MESH,
            )

    def met(self):
        pl.semaphore_wait(pltpu.get_barrier_semaphore(), len(self.peers()))


def arrived(ref, sem):
    pltpu.make_async_copy(ref, ref, sem).wait()


def spread(place, column_source, buffer, sems, on_start, on_column, on_plane, on_core, filler):
    send_sem, recv_sem = sems
    column = place.column

    def post(kind, source, target, slot, towards):
        return remote(
            source, target, send_sem.at[kind], recv_sem.at[slot], place.peer(towards)
        )

    def forward(k):
        for plane in (3, 1, 2):
            post(1, buffer.at[k, 0, 0], buffer.at[k, plane, 0], column + k, plane * 2)

    for k in reversed(range(1, column)):
        post(0, column_source(k), buffer.at[k, 0, 0], k, k * 8)
        on_start(k)
    forward(0)
    on_column(0)
    for k in range(1, column):
        arrived(buffer.at[k, 0, 0], recv_sem.at[k])
        forward(k)
        on_column(k)
    filler()
    for k in range(column):
        arrived(buffer.at[k, pl.ds(1, 3), 0], recv_sem.at[column + k])
        post(2, buffer.at[k, :, 0], buffer.at[k, :, 1], 2 * column + k, 1)
        on_plane(k)
    for k in range(column):
        arrived(buffer.at[k, :, 1], recv_sem.at[2 * column + k])
        on_core(k)
    return [
        (buffer.at[pl.ds(1, column - 1), 0, 0], send_sem.at[0]),
        (buffer.at[:, pl.ds(1, 3), 0], send_sem.at[1]),
        (buffer.at[:, :, 0], send_sem.at[2]),
    ]


def pieces_of(lanes):
    part = lanes // 4
    return ((0, part, True), (part, 2 * part, False), (3 * part, part, False))


class Piece:
    def __init__(self, place, values, size, local_rows, piece, boxes, sems):
        self.place, self.values, self.size = place, values, size
        self.first, self.rows = piece[0] * local_rows, piece[1] * local_rows
        self.core_out, self.core_in, self.plane_out, self.plane_in = boxes[0:4]
        self.column_out, self.column_in = boxes[4:6]
        self.kind = self.core_out.dtype
        self.send_sem, self.recv_sem = sems
        self.others = pl.ds(1, place.column - 1)

    def post(self, kind, slot, source, target, towards):
        remote(
            source,
            target,
            self.send_sem.at[kind],
            self.recv_sem.at[slot],
            self.place.peer(towards),
        )

    def held(self, pattern):
        start = self.place.peer(pattern) * self.size + self.first
        return self.values[pl.ds(pl.multiple_of(start, 8), self.rows), :]

    def core(self):
        for k in reversed(range(self.place.column)):
            for plane in range(4):
                self.core_out[k, plane] = self.held(k * 8 + plane * 2 + 1).astype(self.kind)
            self.post(0, k, self.core_out.at[k], self.core_in.at[k], 1)

    def met(self, k):
        arrived(self.core_in.at[k], self.recv_sem.at[k])

    def chip(self, k, plane):
        return self.held(k * 8 + plane * 2) + self.core_in[k, plane].astype(jnp.float32)


class PlaneFirst(Piece):
    def plane(self, k):
        self.met(k)
        for plane in (3, 1, 2):
            self.plane_out[k, plane] = self.chip(k, plane).astype(self.kind)
            self.post(
                1,
                self.place.column + k,
                self.plane_out.at[k, plane],
                self.plane_in.at[k, plane],
                plane * 2,
            )

    def own(self, k):
        total = self.chip(k, 0)
        arrived(self.plane_in.at[k, pl.ds(1, 3)], self.recv_sem.at[self.place.column + k])
        for plane in (1, 2, 3):
            total = total + self.plane_in[k, plane].astype(jnp.float32)
        return total

    def column(self, k):
        self.column_out[k] = self.own(k).astype(self.kind)
        self.post(
            2, 2 * self.place.column, self.column_out.at[k], self.column_in.at[k], k * 8
        )

    def total(self):
        value = self.own(0)
        arrived(self.column_in.at[self.others], self.recv_sem.at[2 * self.place.column])
        for k in range(1, self.place.column):
            value = value + self.column_in[k].astype(jnp.float32)
        return value

    def sent(self):
        return [
            (self.core_out, self.send_sem.at[0]),
            (self.plane_out.at[:, pl.ds(1, 3)], self.send_sem.at[1]),
            (self.column_out.at[self.others], self.send_sem.at[2]),
        ]


class ColumnFirst(Piece):
    def columns(self):
        for k in reversed(range(1, self.place.column)):
            self.met(k)
            for plane in range(4):
                self.column_out[k, plane] = self.chip(k, plane).astype(self.kind)
            self.post(
                2, self.place.column + 1, self.column_out.at[k], self.column_in.at[k], k * 8
            )

    def line(self, plane):
        value = self.chip(0, plane)
        for k in range(1, self.place.column):
            value = value + self.column_in[k, plane].astype(jnp.float32)
        return value

    def planes(self):
        self.met(0)
        arrived(self.column_in.at[self.others], self.recv_sem.at[self.place.column + 1])
        for plane in (3, 1, 2):
            self.plane_out[plane] = self.line(plane).astype(self.kind)
            self.post(
                1,
                self.place.column,
                self.plane_out.at[plane],
                self.plane_in.at[plane],
                plane * 2,
            )

    def total(self):
        value = self.line(0)
        arrived(self.plane_in.at[pl.ds(1, 3)], self.recv_sem.at[self.place.column])
        for plane in (1, 2, 3):
            value = value + self.plane_in[plane].astype(jnp.float32)
        return value

    def sent(self):
        return [
            (self.core_out, self.send_sem.at[0]),
            (self.plane_out.at[pl.ds(1, 3)], self.send_sem.at[1]),
            (self.column_out.at[self.others], self.send_sem.at[2]),
        ]


def collect(place, values, size, local_rows, boxes, sems, fill, filler):
    pieces = pieces_of(size // local_rows)
    made = [
        (ColumnFirst if piece[2] else PlaneFirst)(
            place,
            values,
            size,
            local_rows,
            piece,
            boxes[6 * i : 6 * i + 6],
            sems[2 * i : 2 * i + 2],
        )
        for i, piece in enumerate(pieces)
    ]
    across, wide, rest = made
    far = list(reversed(range(1, place.column)))
    fill(0)
    across.core()
    fill(1)
    across.columns()
    wide.core()
    fill(2)
    wide.plane(far[0])
    rest.core()
    for k in far[1:]:
        wide.plane(k)
    for k in far:
        rest.plane(k)
    wide.plane(0)
    rest.plane(0)
    filler()
    wide.column(far[0])
    across.planes()
    for k in far[1:]:
        wide.column(k)
    for k in far:
        rest.column(k)
    total = jnp.concatenate([piece.total() for piece in made], axis=0)
    return total, [copy for piece in made for copy in piece.sent()]


def layer_kernel(
    shards,
    per_block,
    *refs,
):
    given, (mixed_out, expert_out), refs = refs[:16], refs[16:18], refs[18:]
    held, load_sem = refs[:16], refs[16]
    (
        prefix_ref,
        length_ref,
        keys_ref,
        values_ref,
        own_key_ref,
        own_value_ref,
        queries_ref,
        ids_ref,
        route_ref,
        w_out_ref,
        gate_ref,
        gate_scale_ref,
        down_ref,
        down_scale_ref,
        hidden_ref,
        gain_ref,
    ) = held
    (
        stage,
        q_send,
        q_column,
        q_plane,
        q_core,
        q_wide,
        kv_send,
        kv_all,
        own_wide,
        attended,
        partial,
        mixed_ref,
        normed_all,
        rows_wide,
        rows_ref,
    ) = refs[17 : 17 + 15]
    boxes_and_sems = refs[17 + 15 :]
    first_boxes, second_boxes = boxes_and_sems[0:18], boxes_and_sems[18:36]
    sems = boxes_and_sems[36:]
    q_sems, kv_sems, row_sems = [sems[2 * i : 2 * i + 2] for i in range(3)]
    first_sems, second_sems = sems[6:12], sems[12:18]
    place = Place(shards)
    me = place.me
    local_rows, width = queries_ref.shape
    lanes = width // 128
    size = local_rows * lanes
    prefixes, positions, _ = keys_ref.shape
    blocks = shards // per_block
    span = blocks * positions
    key_groups = own_key_ref.shape[1] // HD
    per_group = shards // key_groups
    score_scale = 1.0 / math.sqrt(HD)
    f32 = jnp.float32
    pieces = pieces_of(lanes)

    def rows_of(i):
        for first, count, _ in pieces:
            if first <= i < first + count:
                return first * local_rows + i - first, count

    place.greet()
    loads = []
    for i, (source, target) in enumerate(zip(given, held)):
        load = pltpu.make_async_copy(source, target, load_sem.at[i])
        load.start()
        loads.append(load)
    for load in loads[:9]:
        load.wait()

    lengths = []
    for b in range(blocks):
        prefix = prefix_ref[b * per_block * local_rows]
        length = length_ref[0]
        for p in range(1, prefixes):
            length = jnp.where(prefix == p, length_ref[p], length)
        lengths.append(length)
        prefix_of = jnp.full((positions, keys_ref.shape[2]), prefix, jnp.int32)
        for which, ref in enumerate((keys_ref, values_ref)):
            chosen = ref[0].astype(f32)
            for p in range(1, prefixes):
                chosen = jnp.where(prefix_of == p, ref[p].astype(f32), chosen)
            at = which * span + b * positions
            for g in range(key_groups):
                kv_send[g, at : at + positions, :] = chosen[:, g * HD : (g + 1) * HD].astype(
                    jnp.bfloat16
                )
    stage[...] = jnp.zeros((16, HD), f32)
    lane = lax.broadcasted_iota(jnp.int32, (local_rows, 128), 1)
    dense = jnp.zeros((local_rows, 128), f32)
    for choice in range(ids_ref.shape[1]):
        dense = dense + jnp.where(
            lane % 64 == ids_ref[:, choice : choice + 1], route_ref[:, choice : choice + 1], 0.0
        )
    coarse = dense.astype(jnp.bfloat16).astype(f32)
    stage[local_rows : 2 * local_rows, :] = jnp.where(lane < 64, coarse, dense - coarse)
    for g in range(key_groups):
        cut = slice(g * HD, (g + 1) * HD)
        stage[0:local_rows, :] = own_key_ref[:, cut].astype(f32)
        stage[8 : 8 + local_rows, :] = own_value_ref[:, cut].astype(f32)
        kv_send[g, 2 * span : 2 * span + 16, :] = stage[...].astype(jnp.bfloat16)
    for d in range(shards):
        q_send[d] = queries_ref[:, d * HD : (d + 1) * HD]
    place.met()

    column = place.column

    def q_post(kind, source, target, slot, towards):
        remote(source, target, q_sems[0].at[kind], q_sems[1].at[slot], place.peer(towards))

    def q_start(k):
        first = place.peer(k * 8) // 8 * 8
        q_post(0, q_send.at[pl.ds(first, 8)], q_column.at[k], k, k * 8)

    def q_on_column(k):
        if k:
            arrived(q_column.at[k], q_sems[1].at[k])
        for plane in (3, 1, 2):
            first = place.peer(plane * 2) % 8 // 2 * 2
            source = (q_column.at[k] if k else q_send).at[
                pl.ds(first + (0 if k else me // 8 * 8), 2)
            ]
            q_post(1, source, q_plane.at[k, plane], column + k, plane * 2)
        mine = me // 2 * 2
        q_plane[k, 0] = q_column[k, pl.ds(mine % 8, 2)] if k else q_send[pl.ds(mine, 2)]

    def q_on_plane(k):
        arrived(q_plane.at[k, pl.ds(1, 3)], q_sems[1].at[column + k])
        q_post(2, q_plane.at[k, :, place.peer(1) % 2], q_core.at[k], 2 * column, 1)

    my_group = me // per_group

    def dequantize_gate():
        loads[10].wait()
        loads[11].wait()

        def block_row(i, carry):
            at = pl.ds(pl.multiple_of(i * 128, 128), 128)
            for j in range(gate_ref.shape[1] // 128):
                cut = slice(j * 128, (j + 1) * 128)
                wide = gate_ref[at, cut].astype(f32) * gate_scale_ref[j, 0, i]
                gate_ref[at, cut] = wide.astype(jnp.bfloat16)
            return carry

        lax.fori_loop(0, gate_ref.shape[0] // 128, block_row, 0)

    def dequantize_down():
        loads[12].wait()
        loads[13].wait()

        def block_column(j, carry):
            at = pl.ds(pl.multiple_of(j * 128, 128), 128)
            for i in range(down_ref.shape[0] // 128):
                cut = slice(i * 128, (i + 1) * 128)
                wide = down_ref[cut, at].astype(f32) * down_scale_ref[i, 0, j]
                down_ref[cut, at] = wide.astype(jnp.bfloat16)
            return carry

        lax.fori_loop(0, down_ref.shape[1] // 128, block_column, 0)

    kv_all[0, 0, 0] = kv_send[my_group]
    waits = spread(
        place,
        lambda k: kv_send.at[place.peer(k * 8) // per_group],
        kv_all,
        kv_sems,
        q_start,
        q_on_column,
        q_on_plane,
        lambda k: None,
        dequantize_gate,
    )

    waits = waits + [
        (q_column.at[pl.ds(1, column - 1)], q_sems[0].at[0]),
        (q_plane.at[:, pl.ds(1, 3)], q_sems[0].at[1]),
        (q_core, q_sems[0].at[2]),
    ]
    arrived(q_core, q_sems[1].at[2 * column])
    for k in range(column):
        for plane in range(4):
            for core, block in ((0, q_plane[k, plane, me % 2]), (1, q_core[k, plane])):
                device = place.peer(k * 8 + plane * 2 + core)
                q_wide[pl.ds(pl.multiple_of(device * 8, 8), local_rows), :] = block.astype(f32)
                own_wide[pl.ds(pl.multiple_of(device * 16, 16), 16), :] = kv_all[
                    k, plane, core, 2 * span : 2 * span + 16
                ].astype(f32)
    total_positions = shards * positions
    counted = lax.broadcasted_iota(jnp.int32, (1, total_positions), 1)
    position = (counted // positions ^ me) * positions + counted % positions

    def picked(ref, start, count, stride):
        return jnp.concatenate(
            [ref[pl.ds(start + r, count, stride=stride), :] for r in range(local_rows)], axis=0
        )

    for b in range(blocks):
        first = b * per_block
        key_at, value_at = b * positions, span + b * positions
        key = kv_all[:, :, :, key_at : key_at + positions, :].reshape(total_positions, HD)
        value = kv_all[:, :, :, value_at : value_at + positions, :].reshape(total_positions, HD)
        query = picked(q_wide, first * 8, per_block, 8)
        own_k = picked(own_wide, first * 16, per_block, 16)
        own_v = picked(own_wide, first * 16 + 8, per_block, 16)
        scores = lax.dot_general(
            query.astype(jnp.bfloat16), key, (((1,), (1,)), ((), ())), preferred_element_type=f32
        )
        is_valid = position < lengths[b]
        scores = jnp.where(is_valid, scores * score_scale, NEG)
        own_score = jnp.sum(query * own_k, axis=1, keepdims=True) * score_scale
        top = jnp.maximum(jnp.max(scores, axis=1, keepdims=True), own_score)
        weights = jnp.where(is_valid, jnp.exp(scores - top), 0.0)
        own_weight = jnp.exp(own_score - top)
        denominator = jnp.sum(weights, axis=1, keepdims=True) + own_weight
        numerator = jnp.dot(weights.astype(jnp.bfloat16), value, preferred_element_type=f32)
        result = (numerator + own_weight * own_v) / denominator
        for r in range(local_rows):
            attended[r * shards + first : r * shards + first + per_block, :] = result[
                r * per_block : (r + 1) * per_block, :
            ]

    def multiply_out(rows, matrix_ref, piece):
        first, count, _ = pieces[piece]
        for at in range(first, first + count, 4):
            result = jnp.dot(
                rows, matrix_ref[:, at * 128 : (at + 4) * 128], preferred_element_type=f32
            )
            for i in range(4):
                start, apart = rows_of(at + i)
                for r in range(local_rows):
                    partial[pl.ds(start + r * apart, shards, stride=size), :] = result[
                        r * shards : (r + 1) * shards, i * 128 : (i + 1) * 128
                    ]

    loads[9].wait()
    head_rows = attended[...].astype(jnp.bfloat16)
    projected, more = collect(
        place,
        partial,
        size,
        local_rows,
        first_boxes,
        first_sems,
        lambda piece: multiply_out(head_rows, w_out_ref, piece),
        dequantize_down,
    )
    waits = waits + more

    loads[14].wait()
    loads[15].wait()
    for i in range(lanes):
        mixed_ref[pl.ds(rows_of(i)[0], local_rows, stride=rows_of(i)[1]), :] = hidden_ref[
            :, i * 128 : (i + 1) * 128
        ].astype(f32)
    mixed = mixed_ref[...] + projected
    mixed_ref[...] = mixed
    grouped = [
        mixed[first * local_rows : (first + count) * local_rows].reshape(local_rows, count, 128)
        for first, count, _ in pieces
    ]
    squares = sum(jnp.sum(part * part, axis=1, keepdims=True) for part in grouped)
    squares = jnp.sum(squares, axis=2, keepdims=True)
    scale = lax.rsqrt(squares / width + EPSILON)
    normed = jnp.concatenate(
        [
            (part * scale * gain_ref[first : first + count, :][None]).reshape(-1, 128)
            for part, (first, count, _) in zip(grouped, pieces)
        ],
        axis=0,
    )
    normed_all[0, 0, 0] = normed.astype(jnp.bfloat16)

    def widen(k, core):
        for plane in range(4):
            device = place.peer(k * 8 + plane * 2 + core)
            at = pl.ds(pl.multiple_of(device * size, size), size)
            rows_wide[at, :] = normed_all[k, plane, core].astype(f32)

    def write_attention():
        for i in range(lanes):
            mixed_out[:, i * 128 : (i + 1) * 128] = mixed_ref[
                pl.ds(rows_of(i)[0], local_rows, stride=rows_of(i)[1]), :
            ]

    more = spread(
        place,
        lambda k: normed_all.at[0, 0, 0],
        normed_all,
        row_sems,
        lambda k: None,
        lambda k: None,
        lambda k: widen(k, 0),
        lambda k: widen(k, 1),
        write_attention,
    )
    waits = waits + more
    for i in range(lanes):
        start, apart = rows_of(i)
        for r in range(local_rows):
            rows_ref[r * shards : (r + 1) * shards, i * 128 : (i + 1) * 128] = rows_wide[
                pl.ds(start + r * apart, shards, stride=size), :
            ].astype(jnp.bfloat16)
    half = down_ref.shape[0]
    projected_in = jnp.dot(rows_ref[...], gate_ref[...], preferred_element_type=f32)
    split = picked(own_wide, local_rows, shards, 16)
    lane = lax.broadcasted_iota(jnp.int32, split.shape, 1)
    weight = jnp.sum(jnp.where(lane % 64 == me // 2, split, 0.0), axis=1, keepdims=True)
    gate = projected_in[:, :half]
    activated = gate / (1.0 + jnp.exp(-gate)) * projected_in[:, half:]
    activated = jnp.where(weight != 0.0, activated * weight, 0.0).astype(jnp.bfloat16)
    expert_sum, more = collect(
        place,
        partial,
        size,
        local_rows,
        second_boxes,
        second_sems,
        lambda piece: multiply_out(activated, down_ref, piece),
        lambda: None,
    )
    waits = waits + more
    mixed_ref[...] = expert_sum
    for i in range(lanes):
        expert_out[:, i * 128 : (i + 1) * 128] = mixed_ref[pl.ds(rows_of(i)[0], local_rows, stride=rows_of(i)[1]), :]
    for ref, sem in waits:
        arrived(ref, sem)


def fused_layer(
    queries,
    own_key,
    own_value,
    cache_keys,
    cache_values,
    prefix_of_row,
    context_len,
    hidden_in,
    w_out,
    norm_gain,
    expert_ids,
    route_weights,
    gate_up_codes,
    gate_up_scales,
    down_codes,
    down_scales,
):
    shards = lax.axis_size("ctx")
    local_rows, width = queries.shape
    lanes = width // 128
    size = local_rows * lanes
    span = shards * local_rows // CAND * cache_keys.shape[1]
    column = shards // 8
    bf16, f32 = jnp.bfloat16, jnp.float32
    kv_rows = 2 * span + 16
    boxes = []
    for _, count, column_first in pieces_of(lanes):
        rows = count * local_rows
        chips, line, plane = (column, 4, rows, 128), (column, rows, 128), (4, rows, 128)
        last = (plane, plane, chips, chips) if column_first else (chips, chips, line, line)
        boxes = boxes + [pltpu.VMEM(shape, bf16) for shape in (chips, chips) + last]
    operands = (
        prefix_of_row,
        context_len,
        cache_keys,
        cache_values,
        own_key,
        own_value,
        queries,
        expert_ids,
        route_weights,
        w_out,
        gate_up_codes[0],
        gate_up_scales.transpose(2, 0, 1),
        down_codes[0],
        down_scales.transpose(1, 0, 2),
        hidden_in,
        norm_gain.reshape(lanes, 128),
    )
    scalars = (0, 1, 11, 13)
    out = jax.ShapeDtypeStruct((local_rows, width), f32)
    vmem = pl.BlockSpec(memory_space=pltpu.VMEM)
    mixed, expert_sum = pl.pallas_call(
        lambda *refs: layer_kernel(shards, CAND // local_rows, *refs),
        out_shape=(out, out),
        in_specs=[pl.BlockSpec(memory_space=pltpu.HBM)] * len(operands),
        out_specs=(vmem, vmem),
        scratch_shapes=[
            (pltpu.SMEM if i in scalars else pltpu.VMEM)(x.shape, x.dtype)
            for i, x in enumerate(operands)
        ]
        + [
            pltpu.SemaphoreType.DMA((len(operands),)),
            pltpu.VMEM((16, 128), f32),
            pltpu.VMEM((shards, local_rows, 128), bf16),
            pltpu.VMEM((column, 8, local_rows, 128), bf16),
            pltpu.VMEM((column, 4, 2, local_rows, 128), bf16),
            pltpu.VMEM((column, 4, local_rows, 128), bf16),
            pltpu.VMEM((shards * 8, 128), f32),
            pltpu.VMEM((own_key.shape[1] // HD, kv_rows, 128), bf16),
            pltpu.VMEM((column, 4, 2, kv_rows, 128), bf16),
            pltpu.VMEM((shards * 16, 128), f32),
            pltpu.VMEM((shards * local_rows, 128), f32),
            pltpu.VMEM((shards * size, 128), f32),
            pltpu.VMEM((size, 128), f32),
            pltpu.VMEM((column, 4, 2, size, 128), bf16),
            pltpu.VMEM((shards * size, 128), f32),
            pltpu.VMEM((shards * local_rows, width), bf16),
        ]
        + boxes
        + boxes
        + [
            pltpu.SemaphoreType.DMA((count,))
            for count in (3, 2 * column + 1, 3, 3 * column, 3, 3 * column)
            + (3, column + 2, 3, 2 * column + 1, 3, 2 * column + 1) * 2
        ],
        compiler_params=pltpu.CompilerParams(
            collective_id=1, has_side_effects=True, vmem_limit_bytes=VMEM_BYTES
        ),
        name="fused_layer",
    )(*operands)
    return mixed.astype(bf16), (mixed + expert_sum).astype(bf16)


def fits_fused(queries, own_key, cache_keys, w_out, expert_ids):
    shards = lax.axis_size("ctx")
    local_rows, width = queries.shape
    return (
        shards % 8 == 0
        and shards & (shards - 1) == 0
        and w_out.shape[0] == HD
        and width == shards * HD
        and w_out.shape[1] == width
        and local_rows == 4
        and width % (128 * 32) == 0
        and shards // 2 <= 64
        and shards % (own_key.shape[1] // HD * 8) == 0
        and shards * local_rows % CAND == 0
        and cache_keys.shape[1] % 16 == 0
    )


def local(*arrays):
    queries, own_key, cache_keys = arrays[0], arrays[1], arrays[3]
    if fits_fused(queries, own_key, cache_keys, arrays[8], arrays[10]):
        return fused_layer(*arrays)
    return staged_layer(*arrays)


def solution(mesh):
    return jax.shard_map(
        local,
        mesh=mesh,
        in_specs=(
            P(("replica", "ctx"), None),
            P(("replica", "ctx"), None),
            P(("replica", "ctx"), None),
            P("replica", "ctx", None),
            P("replica", "ctx", None),
            P("replica"),
            P("replica"),
            P(("replica", "ctx"), None),
            P("ctx", None),
            P(),
            P(("replica", "ctx"), None),
            P(("replica", "ctx"), None),
            P("ctx", None, None),
            P("ctx", None, None),
            P("ctx", None, None),
            P("ctx", None, None),
        ),
        out_specs=(P(("replica", "ctx"), None), P(("replica", "ctx"), None)),
        check_vma=False,
    )
```

```python
import math

import jax
import jax.numpy as jnp
from jax import lax
from jax.experimental import pallas as pl
from jax.experimental.pallas import tpu as pltpu
from jax.sharding import PartitionSpec as P

HD = 128
CAND = 64


NEG = -1e30
EPSILON = 1e-06
VMEM_BYTES = None
ACROSS = 2
REST = 3


def swapped(value, axis, distance):
    return lax.ppermute(value, axis, [(i, i ^ 1 << distance) for i in range(lax.axis_size(axis))])


def dequantize(code_values, scales):
    rows_per = code_values.shape[0] // scales.shape[0]
    cols_per = code_values.shape[1] // scales.shape[1]
    spread = jnp.repeat(jnp.repeat(scales, rows_per, axis=0), cols_per, axis=1)
    return (code_values.astype(jnp.float32) * spread).astype(jnp.bfloat16)


def block_partials(query_heads, key_heads, value_heads, is_valid, score_scale):
    scores = (
        jnp.einsum(
            "brgqd,bstgd->brgqst", query_heads, key_heads, preferred_element_type=jnp.float32
        )
        * score_scale
    )
    valid_full = is_valid[:, None, None, None, :, :]
    masked = jnp.where(valid_full, scores, NEG)
    block_max = jnp.max(masked, axis=-1)
    weights = jnp.where(valid_full, jnp.exp(masked - block_max[..., None]), 0.0)
    block_total = jnp.sum(weights, axis=-1)
    numerator = jnp.einsum(
        "brgqst,bstgd->brgqsd",
        weights.astype(jnp.bfloat16),
        value_heads,
        preferred_element_type=jnp.float32,
    )
    block_out = (numerator / jnp.maximum(block_total, 1.0)[..., None]).astype(jnp.bfloat16)
    return (block_max, block_total, block_out)


def fold_blocks(block_max, block_total, block_out):
    local_top = jnp.max(block_max, axis=-1)
    factor = block_total * jnp.exp(block_max - local_top[..., None])
    numer = jnp.sum(factor[..., None] * block_out.astype(jnp.float32), axis=-2)
    denom = jnp.sum(factor, axis=-1)
    return (local_top, numer, denom)


def merge_pair(first, second):
    top = jnp.maximum(first[0], second[0])
    scale_first = jnp.exp(first[0] - top)
    scale_second = jnp.exp(second[0] - top)
    numer = first[1] * scale_first[..., None] + second[1] * scale_second[..., None]
    denom = first[2] * scale_first + second[2] * scale_second
    return (top, numer, denom)


def flipped(index, pattern, bits):
    total = 0
    for bit in range(bits):
        value = index // (1 << bit) % 2
        if pattern >> bit & 1:
            value = 1 - value
        total = total + value * (1 << bit)
    return total


def greet(me, bits):
    barrier = pltpu.get_barrier_semaphore()
    for bit in range(bits):
        pl.semaphore_signal(
            barrier,
            inc=1,
            device_id={"ctx": flipped(me, 1 << bit, bits)},
            device_id_type=pl.DeviceIdType.MESH,
        )
    pl.semaphore_wait(barrier, bits)


def lane_parts(rows, bits):
    middle = rows // 32 * 16
    first = list(range(bits))
    second = list(range(bits))
    if bits > 2:
        second[1], second[2] = second[2], second[1]
    return ((0, middle, first), (middle, rows - middle, second))


def gather_kernel(bits, block_ref, out_ref, send_sem, recv_sem, own_sem):
    me = lax.axis_index("ctx")
    parts = lane_parts(block_ref.shape[0], bits)
    own = pltpu.make_async_copy(block_ref, out_ref.at[me], own_sem)
    own.start()
    greet(me, bits)
    copies = [{}, {}]
    waited = [set(), set()]
    for step in range(bits):
        for part, (start, size, order) in enumerate(parts):
            bit = order[bits - 1 - step]
            held = [0]
            for earlier in range(step):
                held = held + [p | 1 << order[bits - 1 - earlier] for p in held]
            for pattern in held:
                block = flipped(me, pattern, bits)
                if pattern:
                    if pattern not in waited[part]:
                        copies[part][pattern].wait_recv()
                        waited[part].add(pattern)
                    source = out_ref.at[block, pl.ds(start, size)]
                else:
                    source = block_ref.at[pl.ds(start, size)]
                slot = pattern | 1 << bit
                copy = pltpu.make_async_remote_copy(
                    src_ref=source,
                    dst_ref=out_ref.at[block, pl.ds(start, size)],
                    send_sem=send_sem.at[part, slot],
                    recv_sem=recv_sem.at[part, slot],
                    device_id={"ctx": flipped(me, 1 << bit, bits)},
                    device_id_type=pl.DeviceIdType.MESH,
                )
                copy.start()
                copies[part][slot] = copy
    for part in range(2):
        for slot, copy in copies[part].items():
            if slot not in waited[part]:
                copy.wait_recv()
            copy.wait_send()
    own.wait()


def gather_blocks(block, collective_id):
    shards = lax.axis_size("ctx")
    bits = shards.bit_length() - 1
    return pl.pallas_call(
        lambda *refs: gather_kernel(bits, *refs),
        out_shape=jax.ShapeDtypeStruct((shards,) + block.shape, block.dtype),
        in_specs=[pl.BlockSpec(memory_space=pltpu.VMEM)],
        out_specs=pl.BlockSpec(memory_space=pltpu.VMEM),
        scratch_shapes=[
            pltpu.SemaphoreType.DMA((2, shards)),
            pltpu.SemaphoreType.DMA((2, shards)),
            pltpu.SemaphoreType.DMA,
        ],
        compiler_params=pltpu.CompilerParams(collective_id=collective_id, has_side_effects=True),
        name="gather_blocks",
    )(block)


def scatter_kernel(bits, blocks_ref, out_ref, outbox, inbox, send_sem, recv_sem):
    me = lax.axis_index("ctx")
    shards = 1 << bits
    parts = lane_parts(blocks_ref.shape[1], bits)
    greet(me, bits)
    arrived = [{p: [] for p in range(shards)} for _ in parts]
    pending = [{}, {}]
    finished = [set(), set()]
    sent = []
    next_slot = [0, 0]

    def total(part, pattern):
        start, size, _ = parts[part]
        value = blocks_ref[flipped(me, pattern, bits), pl.ds(start, size), :].astype(jnp.float32)
        for slot in arrived[part][pattern]:
            if slot not in finished[part]:
                pending[part][slot].wait_recv()
                finished[part].add(slot)
            value = value + inbox[slot, pl.ds(start, size), :].astype(jnp.float32)
        return value

    for step in range(bits):
        fresh = []
        for part, (start, size, order) in enumerate(parts):
            bit = order[step]
            done_mask = sum(1 << b for b in order[:step])
            for pattern in range(shards):
                if pattern & done_mask or not pattern >> bit & 1:
                    continue
                slot = next_slot[part]
                next_slot[part] += 1
                if step:
                    outbox[slot, pl.ds(start, size), :] = total(part, pattern).astype(outbox.dtype)
                    source = outbox.at[slot, pl.ds(start, size)]
                else:
                    source = blocks_ref.at[flipped(me, pattern, bits), pl.ds(start, size)]
                copy = pltpu.make_async_remote_copy(
                    src_ref=source,
                    dst_ref=inbox.at[slot, pl.ds(start, size)],
                    send_sem=send_sem.at[part, slot],
                    recv_sem=recv_sem.at[part, slot],
                    device_id={"ctx": flipped(me, 1 << bit, bits)},
                    device_id_type=pl.DeviceIdType.MESH,
                )
                copy.start()
                pending[part][slot] = copy
                sent.append(copy)
                fresh.append((part, pattern ^ 1 << bit, slot))
        for part, pattern, slot in fresh:
            arrived[part][pattern].append(slot)
    for part, (start, size, _) in enumerate(parts):
        out_ref[pl.ds(start, size), :] = total(part, 0)
    for copy in sent:
        copy.wait_send()


def scatter_sum(blocks, collective_id):
    shards = lax.axis_size("ctx")
    bits = shards.bit_length() - 1
    return pl.pallas_call(
        lambda *refs: scatter_kernel(bits, *refs),
        out_shape=jax.ShapeDtypeStruct(blocks.shape[1:], jnp.float32),
        in_specs=[pl.BlockSpec(memory_space=pltpu.VMEM)],
        out_specs=pl.BlockSpec(memory_space=pltpu.VMEM),
        scratch_shapes=[
            pltpu.VMEM(blocks.shape, blocks.dtype),
            pltpu.VMEM(blocks.shape, blocks.dtype),
            pltpu.SemaphoreType.DMA((2, shards)),
            pltpu.SemaphoreType.DMA((2, shards)),
        ],
        compiler_params=pltpu.CompilerParams(collective_id=collective_id, has_side_effects=True),
        name="scatter_sum",
    )(blocks)


def staged_layer(
    queries,
    own_key,
    own_value,
    cache_keys,
    cache_values,
    prefix_of_row,
    context_len,
    hidden_in,
    w_out,
    norm_gain,
    expert_ids,
    route_weights,
    gate_up_codes,
    gate_up_scales,
    down_codes,
    down_scales,
):
    shards = lax.axis_size("ctx")
    device = lax.axis_index("ctx")
    head_size = HD
    local_rows = queries.shape[0]
    key_groups = own_key.shape[1] // head_size
    per_group = queries.shape[1] // own_key.shape[1]
    head_count = key_groups * per_group
    ctx_local = cache_keys.shape[1]
    key_width = cache_keys.shape[2]
    score_scale = 1.0 / math.sqrt(head_size)
    block_prefix = prefix_of_row.reshape(-1, CAND)[:, 0]
    prefix_count = block_prefix.shape[0]
    group_size = CAND // local_rows
    group_bits = group_size.bit_length() - 1
    prefix_bits = (shards // group_size).bit_length() - 1
    group_index = device // group_size
    member = device % group_size
    relay = jnp.concatenate(
        [jnp.take(cache_keys, block_prefix, axis=0), jnp.take(cache_values, block_prefix, axis=0)],
        axis=-1,
    )
    relay_shape = relay.shape
    for bit in range(prefix_bits):
        low = 1 << bit
        view = relay.reshape((relay_shape[0] // (2 * low), 2, low) + relay_shape[1:])
        own_bit = group_index // low % 2
        sent = lax.dynamic_index_in_dim(view, 1 - own_bit, 1, False)
        got = swapped(sent, "ctx", group_bits + bit)
        view = lax.dynamic_update_index_in_dim(view, got, 1 - own_bit, 1)
        relay = view.reshape(relay_shape)
    held = queries
    for bit in range(group_bits):
        other = swapped(held, "ctx", bit)
        upper = device // (1 << bit) % 2
        held = jnp.where(
            upper == 0, jnp.concatenate([held, other], 0), jnp.concatenate([other, held], 0)
        )
    length = jnp.take(context_len, jnp.take(block_prefix, group_index))
    source_block = jnp.arange(prefix_count, dtype=jnp.int32) * group_size + member
    position = source_block[:, None] * ctx_local + jnp.arange(ctx_local, dtype=jnp.int32)[None, :]
    is_valid = (position < length)[None]
    query_heads = held.reshape(1, CAND, key_groups, per_group, head_size)
    key_heads = relay[..., :key_width].reshape(1, prefix_count, ctx_local, key_groups, head_size)
    value_heads = relay[..., key_width:].reshape(1, prefix_count, ctx_local, key_groups, head_size)
    block_max, block_total, block_out = block_partials(
        query_heads, key_heads, value_heads, is_valid, score_scale
    )
    block_max = block_max.reshape(CAND, head_count, prefix_count)
    block_total = block_total.reshape(CAND, head_count, prefix_count)
    block_out = block_out.reshape(CAND, head_count, prefix_count, head_size)
    state = fold_blocks(block_max, block_total, block_out)
    for bit in reversed(range(group_bits)):
        own_bit = device // (1 << bit) % 2
        parts = tuple((item.reshape((2, item.shape[0] // 2) + item.shape[1:]) for item in state))
        sent = tuple((lax.dynamic_index_in_dim(item, 1 - own_bit, 0, False) for item in parts))
        kept = tuple((lax.dynamic_index_in_dim(item, own_bit, 0, False) for item in parts))
        got = swapped(sent, "ctx", bit)
        state = merge_pair(kept, got)
    merged_top, merged_numer, merged_denom = state
    own_heads = queries.reshape(local_rows, key_groups, per_group, head_size)
    own_keys = own_key.reshape(local_rows, key_groups, head_size)
    own_score = (
        jnp.einsum(
            "rgqd,rgd->rgq", own_heads, own_keys, preferred_element_type=jnp.float32
        ).reshape(local_rows, head_count)
        * score_scale
    )
    top_score = jnp.maximum(merged_top, own_score)
    block_scale = jnp.exp(merged_top - top_score)
    own_weight = jnp.exp(own_score - top_score)
    own_term = own_value.reshape(local_rows, key_groups, 1, head_size).astype(
        jnp.float32
    ) * own_weight.reshape(local_rows, key_groups, per_group, 1)
    numerator_all = merged_numer * block_scale[..., None] + own_term.reshape(
        local_rows, head_count, head_size
    )
    denominator = merged_denom * block_scale + own_weight
    attended = (numerator_all / denominator[..., None]).reshape(local_rows, -1).astype(jnp.bfloat16)
    feature_width = hidden_in.shape[1]
    lanes = feature_width // 128
    head_rows = lax.all_to_all(attended, "ctx", split_axis=1, concat_axis=0, tiled=True)
    partial = jnp.dot(head_rows, w_out, preferred_element_type=jnp.float32).astype(jnp.bfloat16)
    projected = scatter_sum(partial.reshape(shards, local_rows * lanes, 128), 1).reshape(
        local_rows, feature_width
    )
    mixed_rows = hidden_in.astype(jnp.float32) + projected
    attention_out = mixed_rows.astype(jnp.bfloat16)
    mean_square = jnp.mean(mixed_rows * mixed_rows, axis=-1, keepdims=True)
    normed = (mixed_rows * lax.rsqrt(mean_square + EPSILON) * norm_gain).astype(jnp.bfloat16)
    experts_all = shards // 2
    chosen = expert_ids[:, :, None] == jnp.arange(experts_all, dtype=jnp.int32)[None, None, :]
    dense = jnp.sum(jnp.where(chosen, route_weights[:, :, None], 0.0), axis=1)
    coarse = lax.reduce_precision(dense, exponent_bits=8, mantissa_bits=7)
    fine = dense - coarse
    weight_cols = jnp.concatenate([coarse, fine], axis=1).astype(jnp.bfloat16)
    weight_lanes = -(-weight_cols.shape[1] // 128)
    weight_cols = jnp.pad(weight_cols, ((0, 0), (0, weight_lanes * 128 - weight_cols.shape[1])))
    weight_block = weight_cols.reshape(local_rows * weight_lanes, 128)
    weight_block = jnp.pad(weight_block, ((0, -weight_block.shape[0] % 16), (0, 0)))
    block = jnp.concatenate([normed.reshape(local_rows * lanes, 128), weight_block], axis=0)
    gate_up = dequantize(gate_up_codes[0], gate_up_scales[0])
    down_proj = dequantize(down_codes[0], down_scales[0])
    half_width = down_proj.shape[0]
    gathered = gather_blocks(block, 2)
    all_rows = shards * local_rows
    flat_rows = gathered[:, : local_rows * lanes].reshape(all_rows, feature_width)
    weight_all = gathered[
        :, local_rows * lanes : local_rows * lanes + local_rows * weight_lanes
    ].reshape(all_rows, weight_lanes * 128)
    column = jnp.arange(weight_lanes * 128, dtype=jnp.int32) % experts_all
    in_use = jnp.arange(weight_lanes * 128, dtype=jnp.int32) < 2 * experts_all
    is_mine = jnp.logical_and(column == device // 2, in_use)
    row_weight = jnp.sum(
        jnp.where(is_mine[None, :], weight_all.astype(jnp.float32), 0.0), axis=1, keepdims=True
    )
    projected_in = jnp.dot(flat_rows, gate_up, preferred_element_type=jnp.float32)
    activated = (jax.nn.silu(projected_in[:, :half_width]) * projected_in[:, half_width:]).astype(
        jnp.bfloat16
    )
    result = jnp.dot(activated, down_proj, preferred_element_type=jnp.float32)
    result = jnp.where(row_weight != 0.0, result * row_weight, 0.0).astype(jnp.bfloat16)
    expert_sum = scatter_sum(result.reshape(shards, local_rows * lanes, 128), 3).reshape(
        local_rows, feature_width
    )
    layer_out = (mixed_rows + expert_sum).astype(jnp.bfloat16)
    return (attention_out, layer_out)


def remote(source, target, send_sem, recv_sem, device):
    copy = pltpu.make_async_remote_copy(
        src_ref=source,
        dst_ref=target,
        send_sem=send_sem,
        recv_sem=recv_sem,
        device_id={"ctx": device},
        device_id_type=pl.DeviceIdType.MESH,
    )
    copy.start()
    return copy


class Place:
    def __init__(self, shards):
        self.shards = shards
        self.bits = shards.bit_length() - 1
        self.column = shards // 8
        self.me = lax.axis_index("ctx")
        self.known = {0: self.me}

    def peer(self, pattern):
        if pattern not in self.known:
            self.known[pattern] = flipped(self.me, pattern, self.bits)
        return self.known[pattern]

    def peers(self):
        return [k * 8 for k in range(1, self.column)] + [2, 4, 6, 1]

    def greet(self):
        barrier = pltpu.get_barrier_semaphore()
        for pattern in self.peers():
            pl.semaphore_signal(
                barrier,
                inc=1,
                device_id={"ctx": self.peer(pattern)},
                device_id_type=pl.DeviceIdType.MESH,
            )

    def met(self):
        pl.semaphore_wait(pltpu.get_barrier_semaphore(), len(self.peers()))


def arrived(ref, sem):
    pltpu.make_async_copy(ref, ref, sem).wait()


def spread(place, column_source, buffer, sems, on_start, on_column, on_plane, on_core, filler):
    send_sem, recv_sem = sems
    column = place.column

    def post(kind, source, target, slot, towards):
        return remote(
            source, target, send_sem.at[kind], recv_sem.at[slot], place.peer(towards)
        )

    def forward(k):
        for plane in (3, 1, 2):
            post(1, buffer.at[k, 0, 0], buffer.at[k, plane, 0], column + k, plane * 2)

    for k in reversed(range(1, column)):
        post(0, column_source(k), buffer.at[k, 0, 0], k, k * 8)
        on_start(k)
    forward(0)
    on_column(0)
    for k in range(1, column):
        arrived(buffer.at[k, 0, 0], recv_sem.at[k])
        forward(k)
        on_column(k)
    filler()
    for k in range(column):
        arrived(buffer.at[k, pl.ds(1, 3), 0], recv_sem.at[column + k])
        post(2, buffer.at[k, :, 0], buffer.at[k, :, 1], 2 * column + k, 1)
        on_plane(k)
    for k in range(column):
        arrived(buffer.at[k, :, 1], recv_sem.at[2 * column + k])
        on_core(k)
    return [
        (buffer.at[pl.ds(1, column - 1), 0, 0], send_sem.at[0]),
        (buffer.at[:, pl.ds(1, 3), 0], send_sem.at[1]),
        (buffer.at[:, :, 0], send_sem.at[2]),
    ]


def pieces_of(lanes):
    part = lanes // 8
    across, rest = ACROSS * part, REST * part
    wide = lanes - across - rest
    return ((0, across, True), (across, wide, False), (across + wide, rest, False))


class Piece:
    def __init__(self, place, values, size, local_rows, piece, boxes, sems):
        self.place, self.values, self.size = place, values, size
        self.first, self.rows = piece[0] * local_rows, piece[1] * local_rows
        self.core_out, self.core_in, self.plane_out, self.plane_in = boxes[0:4]
        self.column_out, self.column_in = boxes[4:6]
        self.kind = self.core_out.dtype
        self.send_sem, self.recv_sem = sems
        self.others = pl.ds(1, place.column - 1)

    def post(self, kind, slot, source, target, towards):
        remote(
            source,
            target,
            self.send_sem.at[kind],
            self.recv_sem.at[slot],
            self.place.peer(towards),
        )

    def held(self, pattern):
        start = self.place.peer(pattern) * self.size + self.first
        return self.values[pl.ds(pl.multiple_of(start, 8), self.rows), :]

    def core(self):
        for k in reversed(range(self.place.column)):
            for plane in range(4):
                self.core_out[k, plane] = self.held(k * 8 + plane * 2 + 1).astype(self.kind)
            self.post(0, k, self.core_out.at[k], self.core_in.at[k], 1)

    def met(self, k):
        arrived(self.core_in.at[k], self.recv_sem.at[k])

    def chip(self, k, plane):
        return self.held(k * 8 + plane * 2) + self.core_in[k, plane].astype(jnp.float32)


class PlaneFirst(Piece):
    def plane(self, k):
        self.met(k)
        for plane in (3, 1, 2):
            self.plane_out[k, plane] = self.chip(k, plane).astype(self.kind)
            self.post(
                1,
                self.place.column + k,
                self.plane_out.at[k, plane],
                self.plane_in.at[k, plane],
                plane * 2,
            )

    def own(self, k):
        total = self.chip(k, 0)
        arrived(self.plane_in.at[k, pl.ds(1, 3)], self.recv_sem.at[self.place.column + k])
        for plane in (1, 2, 3):
            total = total + self.plane_in[k, plane].astype(jnp.float32)
        return total

    def column(self, k):
        self.column_out[k] = self.own(k).astype(self.kind)
        self.post(
            2, 2 * self.place.column, self.column_out.at[k], self.column_in.at[k], k * 8
        )

    def total(self):
        value = self.own(0)
        arrived(self.column_in.at[self.others], self.recv_sem.at[2 * self.place.column])
        for k in range(1, self.place.column):
            value = value + self.column_in[k].astype(jnp.float32)
        return value

    def sent(self):
        return [
            (self.core_out, self.send_sem.at[0]),
            (self.plane_out.at[:, pl.ds(1, 3)], self.send_sem.at[1]),
            (self.column_out.at[self.others], self.send_sem.at[2]),
        ]


class ColumnFirst(Piece):
    def columns(self):
        for k in reversed(range(1, self.place.column)):
            self.met(k)
            for plane in range(4):
                self.column_out[k, plane] = self.chip(k, plane).astype(self.kind)
            self.post(
                2, self.place.column + 1, self.column_out.at[k], self.column_in.at[k], k * 8
            )

    def line(self, plane):
        value = self.chip(0, plane)
        for k in range(1, self.place.column):
            value = value + self.column_in[k, plane].astype(jnp.float32)
        return value

    def planes(self):
        self.met(0)
        arrived(self.column_in.at[self.others], self.recv_sem.at[self.place.column + 1])
        for plane in (3, 1, 2):
            self.plane_out[plane] = self.line(plane).astype(self.kind)
            self.post(
                1,
                self.place.column,
                self.plane_out.at[plane],
                self.plane_in.at[plane],
                plane * 2,
            )

    def total(self):
        value = self.line(0)
        arrived(self.plane_in.at[pl.ds(1, 3)], self.recv_sem.at[self.place.column])
        for plane in (1, 2, 3):
            value = value + self.plane_in[plane].astype(jnp.float32)
        return value

    def sent(self):
        return [
            (self.core_out, self.send_sem.at[0]),
            (self.plane_out.at[pl.ds(1, 3)], self.send_sem.at[1]),
            (self.column_out.at[self.others], self.send_sem.at[2]),
        ]


def collect(place, values, size, local_rows, boxes, sems, fill, filler):
    pieces = pieces_of(size // local_rows)
    made = [
        (ColumnFirst if piece[2] else PlaneFirst)(
            place,
            values,
            size,
            local_rows,
            piece,
            boxes[6 * i : 6 * i + 6],
            sems[2 * i : 2 * i + 2],
        )
        for i, piece in enumerate(pieces)
    ]
    across, wide, rest = made
    far = list(reversed(range(1, place.column)))
    fill(0)
    across.core()
    fill(2)
    rest.core()
    across.columns()
    fill(1)
    for k in far[:2]:
        rest.plane(k)
    wide.core()
    for k in far[2:]:
        rest.plane(k)
    for k in far:
        wide.plane(k)
    rest.plane(0)
    wide.plane(0)
    filler()
    rest.column(far[0])
    rest.column(far[1])
    across.planes()
    for k in far[2:]:
        rest.column(k)
    for k in far:
        wide.column(k)
    total = jnp.concatenate([piece.total() for piece in made], axis=0)
    return total, [copy for piece in made for copy in piece.sent()]


def layer_kernel(
    shards,
    per_block,
    *refs,
):
    given, (mixed_out, expert_out), refs = refs[:16], refs[16:18], refs[18:]
    held, load_sem = refs[:16], refs[16]
    (
        prefix_ref,
        length_ref,
        keys_ref,
        values_ref,
        own_key_ref,
        own_value_ref,
        queries_ref,
        ids_ref,
        route_ref,
        w_out_ref,
        gate_ref,
        gate_scale_ref,
        down_ref,
        down_scale_ref,
        hidden_ref,
        gain_ref,
    ) = held
    (
        stage,
        q_send,
        q_column,
        q_plane,
        q_core,
        q_wide,
        kv_send,
        kv_all,
        own_wide,
        attended,
        partial,
        mixed_ref,
        normed_ref,
        normed_all,
        rows_wide,
        rows_ref,
    ) = refs[17 : 17 + 16]
    boxes_and_sems = refs[17 + 16 :]
    first_boxes, second_boxes = boxes_and_sems[0:18], boxes_and_sems[18:36]
    sems = boxes_and_sems[36:]
    q_sems, kv_sems, row_sems = [sems[2 * i : 2 * i + 2] for i in range(3)]
    first_sems, second_sems = sems[6:12], sems[12:18]
    place = Place(shards)
    me = place.me
    local_rows, width = queries_ref.shape
    lanes = width // 128
    size = local_rows * lanes
    prefixes, positions, _ = keys_ref.shape
    blocks = shards // per_block
    span = blocks * positions
    key_groups = own_key_ref.shape[1] // HD
    per_group = shards // key_groups
    score_scale = 1.0 / math.sqrt(HD)
    f32 = jnp.float32
    pieces = pieces_of(lanes)

    place.greet()
    loads = []
    for i, (source, target) in enumerate(zip(given, held)):
        load = pltpu.make_async_copy(source, target, load_sem.at[i])
        load.start()
        loads.append(load)
    for load in loads[:9]:
        load.wait()

    lengths = []
    for b in range(blocks):
        prefix = prefix_ref[b * per_block * local_rows]
        length = length_ref[0]
        for p in range(1, prefixes):
            length = jnp.where(prefix == p, length_ref[p], length)
        lengths.append(length)
        prefix_of = jnp.full((positions, keys_ref.shape[2]), prefix, jnp.int32)
        for which, ref in enumerate((keys_ref, values_ref)):
            chosen = ref[0].astype(f32)
            for p in range(1, prefixes):
                chosen = jnp.where(prefix_of == p, ref[p].astype(f32), chosen)
            at = which * span + b * positions
            for g in range(key_groups):
                kv_send[g, at : at + positions, :] = chosen[:, g * HD : (g + 1) * HD].astype(
                    jnp.bfloat16
                )
    stage[...] = jnp.zeros((16, HD), f32)
    lane = lax.broadcasted_iota(jnp.int32, (local_rows, 128), 1)
    dense = jnp.zeros((local_rows, 128), f32)
    for choice in range(ids_ref.shape[1]):
        dense = dense + jnp.where(
            lane % 64 == ids_ref[:, choice : choice + 1], route_ref[:, choice : choice + 1], 0.0
        )
    coarse = dense.astype(jnp.bfloat16).astype(f32)
    stage[local_rows : 2 * local_rows, :] = jnp.where(lane < 64, coarse, dense - coarse)
    for g in range(key_groups):
        cut = slice(g * HD, (g + 1) * HD)
        stage[0:local_rows, :] = own_key_ref[:, cut].astype(f32)
        stage[8 : 8 + local_rows, :] = own_value_ref[:, cut].astype(f32)
        kv_send[g, 2 * span : 2 * span + 16, :] = stage[...].astype(jnp.bfloat16)
    for d in range(shards):
        q_send[d] = queries_ref[:, d * HD : (d + 1) * HD]
    place.met()

    column = place.column

    def q_post(kind, source, target, slot, towards):
        remote(source, target, q_sems[0].at[kind], q_sems[1].at[slot], place.peer(towards))

    def q_start(k):
        first = place.peer(k * 8) // 8 * 8
        q_post(0, q_send.at[pl.ds(first, 8)], q_column.at[k], k, k * 8)

    def q_on_column(k):
        if k:
            arrived(q_column.at[k], q_sems[1].at[k])
        for plane in (3, 1, 2):
            first = place.peer(plane * 2) % 8 // 2 * 2
            source = (q_column.at[k] if k else q_send).at[
                pl.ds(first + (0 if k else me // 8 * 8), 2)
            ]
            q_post(1, source, q_plane.at[k, plane], column + k, plane * 2)
        mine = me // 2 * 2
        q_plane[k, 0] = q_column[k, pl.ds(mine % 8, 2)] if k else q_send[pl.ds(mine, 2)]

    def q_on_plane(k):
        arrived(q_plane.at[k, pl.ds(1, 3)], q_sems[1].at[column + k])
        q_post(2, q_plane.at[k, :, place.peer(1) % 2], q_core.at[k], 2 * column, 1)

    my_group = me // per_group

    def dequantize_gate():
        loads[10].wait()
        loads[11].wait()

        def block_row(i, carry):
            at = pl.ds(pl.multiple_of(i * 128, 128), 128)
            for j in range(gate_ref.shape[1] // 128):
                cut = slice(j * 128, (j + 1) * 128)
                wide = gate_ref[at, cut].astype(f32) * gate_scale_ref[j, 0, i]
                gate_ref[at, cut] = wide.astype(jnp.bfloat16)
            return carry

        lax.fori_loop(0, gate_ref.shape[0] // 128, block_row, 0)

    def dequantize_down():
        loads[12].wait()
        loads[13].wait()

        def block_column(j, carry):
            at = pl.ds(pl.multiple_of(j * 128, 128), 128)
            for i in range(down_ref.shape[0] // 128):
                cut = slice(i * 128, (i + 1) * 128)
                wide = down_ref[cut, at].astype(f32) * down_scale_ref[i, 0, j]
                down_ref[cut, at] = wide.astype(jnp.bfloat16)
            return carry

        lax.fori_loop(0, down_ref.shape[1] // 128, block_column, 0)

    kv_all[0, 0, 0] = kv_send[my_group]
    waits = spread(
        place,
        lambda k: kv_send.at[place.peer(k * 8) // per_group],
        kv_all,
        kv_sems,
        q_start,
        q_on_column,
        q_on_plane,
        lambda k: None,
        dequantize_gate,
    )

    waits = waits + [
        (q_column.at[pl.ds(1, column - 1)], q_sems[0].at[0]),
        (q_plane.at[:, pl.ds(1, 3)], q_sems[0].at[1]),
        (q_core, q_sems[0].at[2]),
    ]
    arrived(q_core, q_sems[1].at[2 * column])
    for k in range(column):
        for plane in range(4):
            for core, block in ((0, q_plane[k, plane, me % 2]), (1, q_core[k, plane])):
                device = place.peer(k * 8 + plane * 2 + core)
                q_wide[pl.ds(pl.multiple_of(device * 8, 8), local_rows), :] = block.astype(f32)
                own_wide[pl.ds(pl.multiple_of(device * 16, 16), 16), :] = kv_all[
                    k, plane, core, 2 * span : 2 * span + 16
                ].astype(f32)
    total_positions = shards * positions
    counted = lax.broadcasted_iota(jnp.int32, (1, total_positions), 1)
    position = (counted // positions ^ me) * positions + counted % positions

    def picked(ref, start, count, stride):
        return jnp.concatenate(
            [ref[pl.ds(start + r, count, stride=stride), :] for r in range(local_rows)], axis=0
        )

    for b in range(blocks):
        first = b * per_block
        key_at, value_at = b * positions, span + b * positions
        key = kv_all[:, :, :, key_at : key_at + positions, :].reshape(total_positions, HD)
        value = kv_all[:, :, :, value_at : value_at + positions, :].reshape(total_positions, HD)
        query = picked(q_wide, first * 8, per_block, 8)
        own_k = picked(own_wide, first * 16, per_block, 16)
        own_v = picked(own_wide, first * 16 + 8, per_block, 16)
        scores = lax.dot_general(
            query.astype(jnp.bfloat16), key, (((1,), (1,)), ((), ())), preferred_element_type=f32
        )
        is_valid = position < lengths[b]
        scores = jnp.where(is_valid, scores * score_scale, NEG)
        own_score = jnp.sum(query * own_k, axis=1, keepdims=True) * score_scale
        top = jnp.maximum(jnp.max(scores, axis=1, keepdims=True), own_score)
        weights = jnp.where(is_valid, jnp.exp(scores - top), 0.0)
        own_weight = jnp.exp(own_score - top)
        denominator = jnp.sum(weights, axis=1, keepdims=True) + own_weight
        numerator = jnp.dot(weights.astype(jnp.bfloat16), value, preferred_element_type=f32)
        result = (numerator + own_weight * own_v) / denominator
        for r in range(local_rows):
            attended[r * shards + first : r * shards + first + per_block, :] = result[
                r * per_block : (r + 1) * per_block, :
            ]

    def multiply_out(rows, matrix_ref, piece):
        first, count, _ = pieces[piece]
        for at in range(first, first + count, 4):
            result = jnp.dot(
                rows, matrix_ref[:, at * 128 : (at + 4) * 128], preferred_element_type=f32
            )
            for i in range(4):
                for r in range(local_rows):
                    partial[pl.ds((at + i) * local_rows + r, shards, stride=size), :] = result[
                        r * shards : (r + 1) * shards, i * 128 : (i + 1) * 128
                    ]

    loads[9].wait()
    head_rows = attended[...].astype(jnp.bfloat16)
    projected, more = collect(
        place,
        partial,
        size,
        local_rows,
        first_boxes,
        first_sems,
        lambda piece: multiply_out(head_rows, w_out_ref, piece),
        dequantize_down,
    )
    waits = waits + more

    loads[14].wait()
    loads[15].wait()
    for i in range(lanes):
        mixed_ref[i * local_rows : (i + 1) * local_rows, :] = hidden_ref[
            :, i * 128 : (i + 1) * 128
        ].astype(f32)
    mixed = mixed_ref[...] + projected
    mixed_ref[...] = mixed
    for r in range(local_rows):
        row = mixed_ref[pl.ds(r, lanes, stride=local_rows), :]
        squares = jnp.sum(jnp.sum(row * row, axis=0, keepdims=True), axis=1, keepdims=True)
        normed_ref[pl.ds(r, lanes, stride=local_rows), :] = (
            row * lax.rsqrt(squares / width + EPSILON) * gain_ref[...]
        )
    normed_all[0, 0, 0] = normed_ref[...].astype(jnp.bfloat16)

    def widen(k, core):
        for plane in range(4):
            device = place.peer(k * 8 + plane * 2 + core)
            at = pl.ds(pl.multiple_of(device * size, size), size)
            rows_wide[at, :] = normed_all[k, plane, core].astype(f32)

    def write_attention():
        for i in range(lanes):
            mixed_out[:, i * 128 : (i + 1) * 128] = mixed_ref[
                i * local_rows : (i + 1) * local_rows, :
            ]

    more = spread(
        place,
        lambda k: normed_all.at[0, 0, 0],
        normed_all,
        row_sems,
        lambda k: None,
        lambda k: None,
        lambda k: widen(k, 0),
        lambda k: widen(k, 1),
        write_attention,
    )
    waits = waits + more
    for i in range(lanes):
        for r in range(local_rows):
            rows_ref[r * shards : (r + 1) * shards, i * 128 : (i + 1) * 128] = rows_wide[
                pl.ds(i * local_rows + r, shards, stride=size), :
            ].astype(jnp.bfloat16)
    half = down_ref.shape[0]
    projected_in = jnp.dot(rows_ref[...], gate_ref[...], preferred_element_type=f32)
    split = picked(own_wide, local_rows, shards, 16)
    lane = lax.broadcasted_iota(jnp.int32, split.shape, 1)
    weight = jnp.sum(jnp.where(lane % 64 == me // 2, split, 0.0), axis=1, keepdims=True)
    gate = projected_in[:, :half]
    activated = gate / (1.0 + jnp.exp(-gate)) * projected_in[:, half:]
    activated = jnp.where(weight != 0.0, activated * weight, 0.0).astype(jnp.bfloat16)
    expert_sum, more = collect(
        place,
        partial,
        size,
        local_rows,
        second_boxes,
        second_sems,
        lambda piece: multiply_out(activated, down_ref, piece),
        lambda: None,
    )
    waits = waits + more
    mixed_ref[...] = expert_sum
    for i in range(lanes):
        expert_out[:, i * 128 : (i + 1) * 128] = mixed_ref[i * local_rows : (i + 1) * local_rows, :]
    for ref, sem in waits:
        arrived(ref, sem)


def fused_layer(
    queries,
    own_key,
    own_value,
    cache_keys,
    cache_values,
    prefix_of_row,
    context_len,
    hidden_in,
    w_out,
    norm_gain,
    expert_ids,
    route_weights,
    gate_up_codes,
    gate_up_scales,
    down_codes,
    down_scales,
):
    shards = lax.axis_size("ctx")
    local_rows, width = queries.shape
    lanes = width // 128
    size = local_rows * lanes
    span = shards * local_rows // CAND * cache_keys.shape[1]
    column = shards // 8
    bf16, f32 = jnp.bfloat16, jnp.float32
    kv_rows = 2 * span + 16
    boxes = []
    for _, count, column_first in pieces_of(lanes):
        rows = count * local_rows
        chips, line, plane = (column, 4, rows, 128), (column, rows, 128), (4, rows, 128)
        last = (plane, plane, chips, chips) if column_first else (chips, chips, line, line)
        boxes = boxes + [pltpu.VMEM(shape, bf16) for shape in (chips, chips) + last]
    operands = (
        prefix_of_row,
        context_len,
        cache_keys,
        cache_values,
        own_key,
        own_value,
        queries,
        expert_ids,
        route_weights,
        w_out,
        gate_up_codes[0],
        gate_up_scales.transpose(2, 0, 1),
        down_codes[0],
        down_scales.transpose(1, 0, 2),
        hidden_in,
        norm_gain.reshape(lanes, 128),
    )
    scalars = (0, 1, 11, 13)
    out = jax.ShapeDtypeStruct((local_rows, width), f32)
    vmem = pl.BlockSpec(memory_space=pltpu.VMEM)
    mixed, expert_sum = pl.pallas_call(
        lambda *refs: layer_kernel(shards, CAND // local_rows, *refs),
        out_shape=(out, out),
        in_specs=[pl.BlockSpec(memory_space=pltpu.HBM)] * len(operands),
        out_specs=(vmem, vmem),
        scratch_shapes=[
            (pltpu.SMEM if i in scalars else pltpu.VMEM)(x.shape, x.dtype)
            for i, x in enumerate(operands)
        ]
        + [
            pltpu.SemaphoreType.DMA((len(operands),)),
            pltpu.VMEM((16, 128), f32),
            pltpu.VMEM((shards, local_rows, 128), bf16),
            pltpu.VMEM((column, 8, local_rows, 128), bf16),
            pltpu.VMEM((column, 4, 2, local_rows, 128), bf16),
            pltpu.VMEM((column, 4, local_rows, 128), bf16),
            pltpu.VMEM((shards * 8, 128), f32),
            pltpu.VMEM((own_key.shape[1] // HD, kv_rows, 128), bf16),
            pltpu.VMEM((column, 4, 2, kv_rows, 128), bf16),
            pltpu.VMEM((shards * 16, 128), f32),
            pltpu.VMEM((shards * local_rows, 128), f32),
            pltpu.VMEM((shards * size, 128), f32),
            pltpu.VMEM((size, 128), f32),
            pltpu.VMEM((size, 128), f32),
            pltpu.VMEM((column, 4, 2, size, 128), bf16),
            pltpu.VMEM((shards * size, 128), f32),
            pltpu.VMEM((shards * local_rows, width), bf16),
        ]
        + boxes
        + boxes
        + [
            pltpu.SemaphoreType.DMA((count,))
            for count in (3, 2 * column + 1, 3, 3 * column, 3, 3 * column)
            + (3, column + 2, 3, 2 * column + 1, 3, 2 * column + 1) * 2
        ],
        compiler_params=pltpu.CompilerParams(
            collective_id=1, has_side_effects=True, vmem_limit_bytes=VMEM_BYTES
        ),
        name="fused_layer",
    )(*operands)
    return mixed.astype(bf16), (mixed + expert_sum).astype(bf16)


def fits_fused(queries, own_key, cache_keys, w_out, expert_ids):
    shards = lax.axis_size("ctx")
    local_rows, width = queries.shape
    return (
        shards % 8 == 0
        and shards & (shards - 1) == 0
        and w_out.shape[0] == HD
        and width == shards * HD
        and w_out.shape[1] == width
        and local_rows == 4
        and width % (128 * 32) == 0
        and shards // 2 <= 64
        and shards % (own_key.shape[1] // HD * 8) == 0
        and shards * local_rows % CAND == 0
        and cache_keys.shape[1] % 16 == 0
    )


def local(*arrays):
    queries, own_key, cache_keys = arrays[0], arrays[1], arrays[3]
    if fits_fused(queries, own_key, cache_keys, arrays[8], arrays[10]):
        return fused_layer(*arrays)
    return staged_layer(*arrays)


def solution(mesh):
    return jax.shard_map(
        local,
        mesh=mesh,
        in_specs=(
            P(("replica", "ctx"), None),
            P(("replica", "ctx"), None),
            P(("replica", "ctx"), None),
            P("replica", "ctx", None),
            P("replica", "ctx", None),
            P("replica"),
            P("replica"),
            P(("replica", "ctx"), None),
            P("ctx", None),
            P(),
            P(("replica", "ctx"), None),
            P(("replica", "ctx"), None),
            P("ctx", None, None),
            P("ctx", None, None),
            P("ctx", None, None),
            P("ctx", None, None),
        ),
        out_specs=(P(("replica", "ctx"), None), P(("replica", "ctx"), None)),
        check_vma=False,
    )
```

```python
import math

import jax
import jax.numpy as jnp
from jax import lax
from jax.experimental import pallas as pl
from jax.experimental.pallas import tpu as pltpu
from jax.sharding import PartitionSpec as P

HD = 128
CAND = 64


NEG = -1e30
EPSILON = 1e-06
VMEM_BYTES = None
ACROSS = 2
REST = 3


def swapped(value, axis, distance):
    return lax.ppermute(value, axis, [(i, i ^ 1 << distance) for i in range(lax.axis_size(axis))])


def dequantize(code_values, scales):
    rows_per = code_values.shape[0] // scales.shape[0]
    cols_per = code_values.shape[1] // scales.shape[1]
    spread = jnp.repeat(jnp.repeat(scales, rows_per, axis=0), cols_per, axis=1)
    return (code_values.astype(jnp.float32) * spread).astype(jnp.bfloat16)


def block_partials(query_heads, key_heads, value_heads, is_valid, score_scale):
    scores = (
        jnp.einsum(
            "brgqd,bstgd->brgqst", query_heads, key_heads, preferred_element_type=jnp.float32
        )
        * score_scale
    )
    valid_full = is_valid[:, None, None, None, :, :]
    masked = jnp.where(valid_full, scores, NEG)
    block_max = jnp.max(masked, axis=-1)
    weights = jnp.where(valid_full, jnp.exp(masked - block_max[..., None]), 0.0)
    block_total = jnp.sum(weights, axis=-1)
    numerator = jnp.einsum(
        "brgqst,bstgd->brgqsd",
        weights.astype(jnp.bfloat16),
        value_heads,
        preferred_element_type=jnp.float32,
    )
    block_out = (numerator / jnp.maximum(block_total, 1.0)[..., None]).astype(jnp.bfloat16)
    return (block_max, block_total, block_out)


def fold_blocks(block_max, block_total, block_out):
    local_top = jnp.max(block_max, axis=-1)
    factor = block_total * jnp.exp(block_max - local_top[..., None])
    numer = jnp.sum(factor[..., None] * block_out.astype(jnp.float32), axis=-2)
    denom = jnp.sum(factor, axis=-1)
    return (local_top, numer, denom)


def merge_pair(first, second):
    top = jnp.maximum(first[0], second[0])
    scale_first = jnp.exp(first[0] - top)
    scale_second = jnp.exp(second[0] - top)
    numer = first[1] * scale_first[..., None] + second[1] * scale_second[..., None]
    denom = first[2] * scale_first + second[2] * scale_second
    return (top, numer, denom)


def flipped(index, pattern, bits):
    total = 0
    for bit in range(bits):
        value = index // (1 << bit) % 2
        if pattern >> bit & 1:
            value = 1 - value
        total = total + value * (1 << bit)
    return total


def greet(me, bits):
    barrier = pltpu.get_barrier_semaphore()
    for bit in range(bits):
        pl.semaphore_signal(
            barrier,
            inc=1,
            device_id={"ctx": flipped(me, 1 << bit, bits)},
            device_id_type=pl.DeviceIdType.MESH,
        )
    pl.semaphore_wait(barrier, bits)


def lane_parts(rows, bits):
    middle = rows // 32 * 16
    first = list(range(bits))
    second = list(range(bits))
    if bits > 2:
        second[1], second[2] = second[2], second[1]
    return ((0, middle, first), (middle, rows - middle, second))


def gather_kernel(bits, block_ref, out_ref, send_sem, recv_sem, own_sem):
    me = lax.axis_index("ctx")
    parts = lane_parts(block_ref.shape[0], bits)
    own = pltpu.make_async_copy(block_ref, out_ref.at[me], own_sem)
    own.start()
    greet(me, bits)
    copies = [{}, {}]
    waited = [set(), set()]
    for step in range(bits):
        for part, (start, size, order) in enumerate(parts):
            bit = order[bits - 1 - step]
            held = [0]
            for earlier in range(step):
                held = held + [p | 1 << order[bits - 1 - earlier] for p in held]
            for pattern in held:
                block = flipped(me, pattern, bits)
                if pattern:
                    if pattern not in waited[part]:
                        copies[part][pattern].wait_recv()
                        waited[part].add(pattern)
                    source = out_ref.at[block, pl.ds(start, size)]
                else:
                    source = block_ref.at[pl.ds(start, size)]
                slot = pattern | 1 << bit
                copy = pltpu.make_async_remote_copy(
                    src_ref=source,
                    dst_ref=out_ref.at[block, pl.ds(start, size)],
                    send_sem=send_sem.at[part, slot],
                    recv_sem=recv_sem.at[part, slot],
                    device_id={"ctx": flipped(me, 1 << bit, bits)},
                    device_id_type=pl.DeviceIdType.MESH,
                )
                copy.start()
                copies[part][slot] = copy
    for part in range(2):
        for slot, copy in copies[part].items():
            if slot not in waited[part]:
                copy.wait_recv()
            copy.wait_send()
    own.wait()


def gather_blocks(block, collective_id):
    shards = lax.axis_size("ctx")
    bits = shards.bit_length() - 1
    return pl.pallas_call(
        lambda *refs: gather_kernel(bits, *refs),
        out_shape=jax.ShapeDtypeStruct((shards,) + block.shape, block.dtype),
        in_specs=[pl.BlockSpec(memory_space=pltpu.VMEM)],
        out_specs=pl.BlockSpec(memory_space=pltpu.VMEM),
        scratch_shapes=[
            pltpu.SemaphoreType.DMA((2, shards)),
            pltpu.SemaphoreType.DMA((2, shards)),
            pltpu.SemaphoreType.DMA,
        ],
        compiler_params=pltpu.CompilerParams(collective_id=collective_id, has_side_effects=True),
        name="gather_blocks",
    )(block)


def scatter_kernel(bits, blocks_ref, out_ref, outbox, inbox, send_sem, recv_sem):
    me = lax.axis_index("ctx")
    shards = 1 << bits
    parts = lane_parts(blocks_ref.shape[1], bits)
    greet(me, bits)
    arrived = [{p: [] for p in range(shards)} for _ in parts]
    pending = [{}, {}]
    finished = [set(), set()]
    sent = []
    next_slot = [0, 0]

    def total(part, pattern):
        start, size, _ = parts[part]
        value = blocks_ref[flipped(me, pattern, bits), pl.ds(start, size), :].astype(jnp.float32)
        for slot in arrived[part][pattern]:
            if slot not in finished[part]:
                pending[part][slot].wait_recv()
                finished[part].add(slot)
            value = value + inbox[slot, pl.ds(start, size), :].astype(jnp.float32)
        return value

    for step in range(bits):
        fresh = []
        for part, (start, size, order) in enumerate(parts):
            bit = order[step]
            done_mask = sum(1 << b for b in order[:step])
            for pattern in range(shards):
                if pattern & done_mask or not pattern >> bit & 1:
                    continue
                slot = next_slot[part]
                next_slot[part] += 1
                if step:
                    outbox[slot, pl.ds(start, size), :] = total(part, pattern).astype(outbox.dtype)
                    source = outbox.at[slot, pl.ds(start, size)]
                else:
                    source = blocks_ref.at[flipped(me, pattern, bits), pl.ds(start, size)]
                copy = pltpu.make_async_remote_copy(
                    src_ref=source,
                    dst_ref=inbox.at[slot, pl.ds(start, size)],
                    send_sem=send_sem.at[part, slot],
                    recv_sem=recv_sem.at[part, slot],
                    device_id={"ctx": flipped(me, 1 << bit, bits)},
                    device_id_type=pl.DeviceIdType.MESH,
                )
                copy.start()
                pending[part][slot] = copy
                sent.append(copy)
                fresh.append((part, pattern ^ 1 << bit, slot))
        for part, pattern, slot in fresh:
            arrived[part][pattern].append(slot)
    for part, (start, size, _) in enumerate(parts):
        out_ref[pl.ds(start, size), :] = total(part, 0)
    for copy in sent:
        copy.wait_send()


def scatter_sum(blocks, collective_id):
    shards = lax.axis_size("ctx")
    bits = shards.bit_length() - 1
    return pl.pallas_call(
        lambda *refs: scatter_kernel(bits, *refs),
        out_shape=jax.ShapeDtypeStruct(blocks.shape[1:], jnp.float32),
        in_specs=[pl.BlockSpec(memory_space=pltpu.VMEM)],
        out_specs=pl.BlockSpec(memory_space=pltpu.VMEM),
        scratch_shapes=[
            pltpu.VMEM(blocks.shape, blocks.dtype),
            pltpu.VMEM(blocks.shape, blocks.dtype),
            pltpu.SemaphoreType.DMA((2, shards)),
            pltpu.SemaphoreType.DMA((2, shards)),
        ],
        compiler_params=pltpu.CompilerParams(collective_id=collective_id, has_side_effects=True),
        name="scatter_sum",
    )(blocks)


def staged_layer(
    queries,
    own_key,
    own_value,
    cache_keys,
    cache_values,
    prefix_of_row,
    context_len,
    hidden_in,
    w_out,
    norm_gain,
    expert_ids,
    route_weights,
    gate_up_codes,
    gate_up_scales,
    down_codes,
    down_scales,
):
    shards = lax.axis_size("ctx")
    device = lax.axis_index("ctx")
    head_size = HD
    local_rows = queries.shape[0]
    key_groups = own_key.shape[1] // head_size
    per_group = queries.shape[1] // own_key.shape[1]
    head_count = key_groups * per_group
    ctx_local = cache_keys.shape[1]
    key_width = cache_keys.shape[2]
    score_scale = 1.0 / math.sqrt(head_size)
    block_prefix = prefix_of_row.reshape(-1, CAND)[:, 0]
    prefix_count = block_prefix.shape[0]
    group_size = CAND // local_rows
    group_bits = group_size.bit_length() - 1
    prefix_bits = (shards // group_size).bit_length() - 1
    group_index = device // group_size
    member = device % group_size
    relay = jnp.concatenate(
        [jnp.take(cache_keys, block_prefix, axis=0), jnp.take(cache_values, block_prefix, axis=0)],
        axis=-1,
    )
    relay_shape = relay.shape
    for bit in range(prefix_bits):
        low = 1 << bit
        view = relay.reshape((relay_shape[0] // (2 * low), 2, low) + relay_shape[1:])
        own_bit = group_index // low % 2
        sent = lax.dynamic_index_in_dim(view, 1 - own_bit, 1, False)
        got = swapped(sent, "ctx", group_bits + bit)
        view = lax.dynamic_update_index_in_dim(view, got, 1 - own_bit, 1)
        relay = view.reshape(relay_shape)
    held = queries
    for bit in range(group_bits):
        other = swapped(held, "ctx", bit)
        upper = device // (1 << bit) % 2
        held = jnp.where(
            upper == 0, jnp.concatenate([held, other], 0), jnp.concatenate([other, held], 0)
        )
    length = jnp.take(context_len, jnp.take(block_prefix, group_index))
    source_block = jnp.arange(prefix_count, dtype=jnp.int32) * group_size + member
    position = source_block[:, None] * ctx_local + jnp.arange(ctx_local, dtype=jnp.int32)[None, :]
    is_valid = (position < length)[None]
    query_heads = held.reshape(1, CAND, key_groups, per_group, head_size)
    key_heads = relay[..., :key_width].reshape(1, prefix_count, ctx_local, key_groups, head_size)
    value_heads = relay[..., key_width:].reshape(1, prefix_count, ctx_local, key_groups, head_size)
    block_max, block_total, block_out = block_partials(
        query_heads, key_heads, value_heads, is_valid, score_scale
    )
    block_max = block_max.reshape(CAND, head_count, prefix_count)
    block_total = block_total.reshape(CAND, head_count, prefix_count)
    block_out = block_out.reshape(CAND, head_count, prefix_count, head_size)
    state = fold_blocks(block_max, block_total, block_out)
    for bit in reversed(range(group_bits)):
        own_bit = device // (1 << bit) % 2
        parts = tuple((item.reshape((2, item.shape[0] // 2) + item.shape[1:]) for item in state))
        sent = tuple((lax.dynamic_index_in_dim(item, 1 - own_bit, 0, False) for item in parts))
        kept = tuple((lax.dynamic_index_in_dim(item, own_bit, 0, False) for item in parts))
        got = swapped(sent, "ctx", bit)
        state = merge_pair(kept, got)
    merged_top, merged_numer, merged_denom = state
    own_heads = queries.reshape(local_rows, key_groups, per_group, head_size)
    own_keys = own_key.reshape(local_rows, key_groups, head_size)
    own_score = (
        jnp.einsum(
            "rgqd,rgd->rgq", own_heads, own_keys, preferred_element_type=jnp.float32
        ).reshape(local_rows, head_count)
        * score_scale
    )
    top_score = jnp.maximum(merged_top, own_score)
    block_scale = jnp.exp(merged_top - top_score)
    own_weight = jnp.exp(own_score - top_score)
    own_term = own_value.reshape(local_rows, key_groups, 1, head_size).astype(
        jnp.float32
    ) * own_weight.reshape(local_rows, key_groups, per_group, 1)
    numerator_all = merged_numer * block_scale[..., None] + own_term.reshape(
        local_rows, head_count, head_size
    )
    denominator = merged_denom * block_scale + own_weight
    attended = (numerator_all / denominator[..., None]).reshape(local_rows, -1).astype(jnp.bfloat16)
    feature_width = hidden_in.shape[1]
    lanes = feature_width // 128
    head_rows = lax.all_to_all(attended, "ctx", split_axis=1, concat_axis=0, tiled=True)
    partial = jnp.dot(head_rows, w_out, preferred_element_type=jnp.float32).astype(jnp.bfloat16)
    projected = scatter_sum(partial.reshape(shards, local_rows * lanes, 128), 1).reshape(
        local_rows, feature_width
    )
    mixed_rows = hidden_in.astype(jnp.float32) + projected
    attention_out = mixed_rows.astype(jnp.bfloat16)
    mean_square = jnp.mean(mixed_rows * mixed_rows, axis=-1, keepdims=True)
    normed = (mixed_rows * lax.rsqrt(mean_square + EPSILON) * norm_gain).astype(jnp.bfloat16)
    experts_all = shards // 2
    chosen = expert_ids[:, :, None] == jnp.arange(experts_all, dtype=jnp.int32)[None, None, :]
    dense = jnp.sum(jnp.where(chosen, route_weights[:, :, None], 0.0), axis=1)
    coarse = lax.reduce_precision(dense, exponent_bits=8, mantissa_bits=7)
    fine = dense - coarse
    weight_cols = jnp.concatenate([coarse, fine], axis=1).astype(jnp.bfloat16)
    weight_lanes = -(-weight_cols.shape[1] // 128)
    weight_cols = jnp.pad(weight_cols, ((0, 0), (0, weight_lanes * 128 - weight_cols.shape[1])))
    weight_block = weight_cols.reshape(local_rows * weight_lanes, 128)
    weight_block = jnp.pad(weight_block, ((0, -weight_block.shape[0] % 16), (0, 0)))
    block = jnp.concatenate([normed.reshape(local_rows * lanes, 128), weight_block], axis=0)
    gate_up = dequantize(gate_up_codes[0], gate_up_scales[0])
    down_proj = dequantize(down_codes[0], down_scales[0])
    half_width = down_proj.shape[0]
    gathered = gather_blocks(block, 2)
    all_rows = shards * local_rows
    flat_rows = gathered[:, : local_rows * lanes].reshape(all_rows, feature_width)
    weight_all = gathered[
        :, local_rows * lanes : local_rows * lanes + local_rows * weight_lanes
    ].reshape(all_rows, weight_lanes * 128)
    column = jnp.arange(weight_lanes * 128, dtype=jnp.int32) % experts_all
    in_use = jnp.arange(weight_lanes * 128, dtype=jnp.int32) < 2 * experts_all
    is_mine = jnp.logical_and(column == device // 2, in_use)
    row_weight = jnp.sum(
        jnp.where(is_mine[None, :], weight_all.astype(jnp.float32), 0.0), axis=1, keepdims=True
    )
    projected_in = jnp.dot(flat_rows, gate_up, preferred_element_type=jnp.float32)
    activated = (jax.nn.silu(projected_in[:, :half_width]) * projected_in[:, half_width:]).astype(
        jnp.bfloat16
    )
    result = jnp.dot(activated, down_proj, preferred_element_type=jnp.float32)
    result = jnp.where(row_weight != 0.0, result * row_weight, 0.0).astype(jnp.bfloat16)
    expert_sum = scatter_sum(result.reshape(shards, local_rows * lanes, 128), 3).reshape(
        local_rows, feature_width
    )
    layer_out = (mixed_rows + expert_sum).astype(jnp.bfloat16)
    return (attention_out, layer_out)


def remote(source, target, send_sem, recv_sem, device):
    copy = pltpu.make_async_remote_copy(
        src_ref=source,
        dst_ref=target,
        send_sem=send_sem,
        recv_sem=recv_sem,
        device_id={"ctx": device},
        device_id_type=pl.DeviceIdType.MESH,
    )
    copy.start()
    return copy


class Place:
    def __init__(self, shards):
        self.shards = shards
        self.bits = shards.bit_length() - 1
        self.column = shards // 8
        self.me = lax.axis_index("ctx")
        self.known = {0: self.me}

    def peer(self, pattern):
        if pattern not in self.known:
            self.known[pattern] = flipped(self.me, pattern, self.bits)
        return self.known[pattern]

    def peers(self):
        return [k * 8 for k in range(1, self.column)] + [2, 4, 6, 1]

    def greet(self):
        barrier = pltpu.get_barrier_semaphore()
        for pattern in self.peers():
            pl.semaphore_signal(
                barrier,
                inc=1,
                device_id={"ctx": self.peer(pattern)},
                device_id_type=pl.DeviceIdType.MESH,
            )

    def met(self):
        pl.semaphore_wait(pltpu.get_barrier_semaphore(), len(self.peers()))


def arrived(ref, sem):
    pltpu.make_async_copy(ref, ref, sem).wait()


def spread(place, column_source, buffer, sems, on_start, on_column, on_plane, on_core, filler):
    send_sem, recv_sem = sems
    column = place.column

    def post(kind, source, target, slot, towards):
        return remote(
            source, target, send_sem.at[kind], recv_sem.at[slot], place.peer(towards)
        )

    def forward(k):
        for plane in (3, 1, 2):
            post(1, buffer.at[k, 0, 0], buffer.at[k, plane, 0], column + k, plane * 2)

    for k in reversed(range(1, column)):
        on_start(k)
        post(0, column_source(k), buffer.at[k, 0, 0], k, k * 8)
    on_column(0)
    forward(0)
    for k in range(1, column):
        on_column(k)
        arrived(buffer.at[k, 0, 0], recv_sem.at[k])
        forward(k)
    filler()
    for k in range(column):
        arrived(buffer.at[k, pl.ds(1, 3), 0], recv_sem.at[column + k])
        post(2, buffer.at[k, :, 0], buffer.at[k, :, 1], 2 * column + k, 1)
        on_plane(k)
    for k in range(column):
        arrived(buffer.at[k, :, 1], recv_sem.at[2 * column + k])
        on_core(k)
    return [
        (buffer.at[pl.ds(1, column - 1), 0, 0], send_sem.at[0]),
        (buffer.at[:, pl.ds(1, 3), 0], send_sem.at[1]),
        (buffer.at[:, :, 0], send_sem.at[2]),
    ]


def pieces_of(lanes):
    part = lanes // 8
    across, rest = ACROSS * part, REST * part
    wide = lanes - across - rest
    return ((0, across, True), (across, wide, False), (across + wide, rest, False))


class Piece:
    def __init__(self, place, values, size, local_rows, piece, boxes, sems):
        self.place, self.values, self.size = place, values, size
        self.first, self.rows = piece[0] * local_rows, piece[1] * local_rows
        self.core_out, self.core_in, self.plane_out, self.plane_in = boxes[0:4]
        self.column_out, self.column_in = boxes[4:6]
        self.kind = self.core_out.dtype
        self.send_sem, self.recv_sem = sems
        self.others = pl.ds(1, place.column - 1)

    def post(self, kind, slot, source, target, towards):
        remote(
            source,
            target,
            self.send_sem.at[kind],
            self.recv_sem.at[slot],
            self.place.peer(towards),
        )

    def held(self, pattern):
        start = self.place.peer(pattern) * self.size + self.first
        return self.values[pl.ds(pl.multiple_of(start, 8), self.rows), :]

    def core(self):
        for k in reversed(range(self.place.column)):
            for plane in range(4):
                self.core_out[k, plane] = self.held(k * 8 + plane * 2 + 1).astype(self.kind)
            self.post(0, k, self.core_out.at[k], self.core_in.at[k], 1)

    def met(self, k):
        arrived(self.core_in.at[k], self.recv_sem.at[k])

    def chip(self, k, plane):
        return self.held(k * 8 + plane * 2) + self.core_in[k, plane].astype(jnp.float32)


class PlaneFirst(Piece):
    def plane(self, k):
        self.met(k)
        for plane in (3, 1, 2):
            self.plane_out[k, plane] = self.chip(k, plane).astype(self.kind)
            self.post(
                1,
                self.place.column + k,
                self.plane_out.at[k, plane],
                self.plane_in.at[k, plane],
                plane * 2,
            )

    def own(self, k):
        total = self.chip(k, 0)
        arrived(self.plane_in.at[k, pl.ds(1, 3)], self.recv_sem.at[self.place.column + k])
        for plane in (1, 2, 3):
            total = total + self.plane_in[k, plane].astype(jnp.float32)
        return total

    def column(self, k):
        self.column_out[k] = self.own(k).astype(self.kind)
        self.post(
            2, 2 * self.place.column, self.column_out.at[k], self.column_in.at[k], k * 8
        )

    def total(self):
        value = self.own(0)
        arrived(self.column_in.at[self.others], self.recv_sem.at[2 * self.place.column])
        for k in range(1, self.place.column):
            value = value + self.column_in[k].astype(jnp.float32)
        return value

    def sent(self):
        return [
            (self.core_out, self.send_sem.at[0]),
            (self.plane_out.at[:, pl.ds(1, 3)], self.send_sem.at[1]),
            (self.column_out.at[self.others], self.send_sem.at[2]),
        ]


class ColumnFirst(Piece):
    def columns(self):
        for k in reversed(range(1, self.place.column)):
            self.met(k)
            for plane in range(4):
                self.column_out[k, plane] = self.chip(k, plane).astype(self.kind)
            self.post(
                2, self.place.column + 1, self.column_out.at[k], self.column_in.at[k], k * 8
            )

    def line(self, plane):
        value = self.chip(0, plane)
        for k in range(1, self.place.column):
            value = value + self.column_in[k, plane].astype(jnp.float32)
        return value

    def planes(self):
        self.met(0)
        arrived(self.column_in.at[self.others], self.recv_sem.at[self.place.column + 1])
        for plane in (3, 1, 2):
            self.plane_out[plane] = self.line(plane).astype(self.kind)
            self.post(
                1,
                self.place.column,
                self.plane_out.at[plane],
                self.plane_in.at[plane],
                plane * 2,
            )

    def total(self):
        value = self.line(0)
        arrived(self.plane_in.at[pl.ds(1, 3)], self.recv_sem.at[self.place.column])
        for plane in (1, 2, 3):
            value = value + self.plane_in[plane].astype(jnp.float32)
        return value

    def sent(self):
        return [
            (self.core_out, self.send_sem.at[0]),
            (self.plane_out.at[pl.ds(1, 3)], self.send_sem.at[1]),
            (self.column_out.at[self.others], self.send_sem.at[2]),
        ]


def collect(place, values, size, local_rows, boxes, sems, fill, filler):
    pieces = pieces_of(size // local_rows)
    made = [
        (ColumnFirst if piece[2] else PlaneFirst)(
            place,
            values,
            size,
            local_rows,
            piece,
            boxes[6 * i : 6 * i + 6],
            sems[2 * i : 2 * i + 2],
        )
        for i, piece in enumerate(pieces)
    ]
    across, wide, rest = made
    far = list(reversed(range(1, place.column)))
    fill(0)
    across.core()
    fill(2)
    rest.core()
    across.columns()
    fill(1)
    for k in far[:2]:
        rest.plane(k)
    wide.core()
    for k in far[2:]:
        rest.plane(k)
    for k in far:
        wide.plane(k)
    rest.plane(0)
    wide.plane(0)
    filler()
    rest.column(far[0])
    rest.column(far[1])
    across.planes()
    for k in far[2:]:
        rest.column(k)
    for k in far:
        wide.column(k)
    total = jnp.concatenate([piece.total() for piece in made], axis=0)
    return total, [copy for piece in made for copy in piece.sent()]


def layer_kernel(
    shards,
    per_block,
    *refs,
):
    given, (mixed_out, expert_out), refs = refs[:16], refs[16:18], refs[18:]
    held, load_sem = refs[:16], refs[16]
    (
        prefix_ref,
        length_ref,
        keys_ref,
        values_ref,
        own_key_ref,
        own_value_ref,
        queries_ref,
        ids_ref,
        route_ref,
        w_out_ref,
        gate_ref,
        gate_scale_ref,
        down_ref,
        down_scale_ref,
        hidden_ref,
        gain_ref,
    ) = held
    (
        stage,
        q_send,
        q_column,
        q_plane,
        q_core,
        q_wide,
        kv_send,
        kv_all,
        own_wide,
        attended,
        partial,
        mixed_ref,
        normed_ref,
        normed_all,
        rows_wide,
        rows_ref,
    ) = refs[17 : 17 + 16]
    boxes_and_sems = refs[17 + 16 :]
    first_boxes, second_boxes = boxes_and_sems[0:18], boxes_and_sems[18:36]
    sems = boxes_and_sems[36:]
    q_sems, kv_sems, row_sems = [sems[2 * i : 2 * i + 2] for i in range(3)]
    first_sems, second_sems = sems[6:12], sems[12:18]
    place = Place(shards)
    me = place.me
    local_rows, width = queries_ref.shape
    lanes = width // 128
    size = local_rows * lanes
    prefixes, positions, _ = keys_ref.shape
    blocks = shards // per_block
    span = blocks * positions
    key_groups = own_key_ref.shape[1] // HD
    per_group = shards // key_groups
    score_scale = 1.0 / math.sqrt(HD)
    f32 = jnp.float32
    pieces = pieces_of(lanes)

    place.greet()
    loads = []
    for i, (source, target) in enumerate(zip(given, held)):
        load = pltpu.make_async_copy(source, target, load_sem.at[i])
        load.start()
        loads.append(load)
    for load in loads[:9]:
        load.wait()

    lengths = []
    for b in range(blocks):
        prefix = prefix_ref[b * per_block * local_rows]
        length = length_ref[0]
        for p in range(1, prefixes):
            length = jnp.where(prefix == p, length_ref[p], length)
        lengths.append(length)
        prefix_of = jnp.full((positions, keys_ref.shape[2]), prefix, jnp.int32)
        for which, ref in enumerate((keys_ref, values_ref)):
            chosen = ref[0].astype(f32)
            for p in range(1, prefixes):
                chosen = jnp.where(prefix_of == p, ref[p].astype(f32), chosen)
            at = which * span + b * positions
            for g in range(key_groups):
                kv_send[g, at : at + positions, :] = chosen[:, g * HD : (g + 1) * HD].astype(
                    jnp.bfloat16
                )
    stage[...] = jnp.zeros((16, HD), f32)
    lane = lax.broadcasted_iota(jnp.int32, (local_rows, 128), 1)
    dense = jnp.zeros((local_rows, 128), f32)
    for choice in range(ids_ref.shape[1]):
        dense = dense + jnp.where(
            lane % 64 == ids_ref[:, choice : choice + 1], route_ref[:, choice : choice + 1], 0.0
        )
    coarse = dense.astype(jnp.bfloat16).astype(f32)
    stage[local_rows : 2 * local_rows, :] = jnp.where(lane < 64, coarse, dense - coarse)
    for g in range(key_groups):
        cut = slice(g * HD, (g + 1) * HD)
        stage[0:local_rows, :] = own_key_ref[:, cut].astype(f32)
        stage[8 : 8 + local_rows, :] = own_value_ref[:, cut].astype(f32)
        kv_send[g, 2 * span : 2 * span + 16, :] = stage[...].astype(jnp.bfloat16)
    for d in range(shards):
        q_send[d] = queries_ref[:, d * HD : (d + 1) * HD]
    place.met()

    column = place.column

    def q_post(kind, source, target, slot, towards):
        remote(source, target, q_sems[0].at[kind], q_sems[1].at[slot], place.peer(towards))

    def q_start(k):
        first = place.peer(k * 8) // 8 * 8
        q_post(0, q_send.at[pl.ds(first, 8)], q_column.at[k], k, k * 8)

    def q_on_column(k):
        if k:
            arrived(q_column.at[k], q_sems[1].at[k])
        for plane in (3, 1, 2):
            first = place.peer(plane * 2) % 8 // 2 * 2
            source = (q_column.at[k] if k else q_send).at[
                pl.ds(first + (0 if k else me // 8 * 8), 2)
            ]
            q_post(1, source, q_plane.at[k, plane], column + k, plane * 2)
        mine = me // 2 * 2
        q_plane[k, 0] = q_column[k, pl.ds(mine % 8, 2)] if k else q_send[pl.ds(mine, 2)]

    def q_on_plane(k):
        arrived(q_plane.at[k, pl.ds(1, 3)], q_sems[1].at[column + k])
        q_post(2, q_plane.at[k, :, place.peer(1) % 2], q_core.at[k], 2 * column, 1)

    my_group = me // per_group

    def dequantize_gate():
        loads[10].wait()
        loads[11].wait()

        def block_row(i, carry):
            at = pl.ds(pl.multiple_of(i * 128, 128), 128)
            for j in range(gate_ref.shape[1] // 128):
                cut = slice(j * 128, (j + 1) * 128)
                wide = gate_ref[at, cut].astype(f32) * gate_scale_ref[j, 0, i]
                gate_ref[at, cut] = wide.astype(jnp.bfloat16)
            return carry

        lax.fori_loop(0, gate_ref.shape[0] // 128, block_row, 0)

    def dequantize_down():
        loads[12].wait()
        loads[13].wait()

        def block_column(j, carry):
            at = pl.ds(pl.multiple_of(j * 128, 128), 128)
            for i in range(down_ref.shape[0] // 128):
                cut = slice(i * 128, (i + 1) * 128)
                wide = down_ref[cut, at].astype(f32) * down_scale_ref[i, 0, j]
                down_ref[cut, at] = wide.astype(jnp.bfloat16)
            return carry

        lax.fori_loop(0, down_ref.shape[1] // 128, block_column, 0)

    kv_all[0, 0, 0] = kv_send[my_group]
    waits = spread(
        place,
        lambda k: kv_send.at[place.peer(k * 8) // per_group],
        kv_all,
        kv_sems,
        q_start,
        q_on_column,
        q_on_plane,
        lambda k: None,
        dequantize_gate,
    )

    waits = waits + [
        (q_column.at[pl.ds(1, column - 1)], q_sems[0].at[0]),
        (q_plane.at[:, pl.ds(1, 3)], q_sems[0].at[1]),
        (q_core, q_sems[0].at[2]),
    ]
    arrived(q_core, q_sems[1].at[2 * column])
    for k in range(column):
        for plane in range(4):
            for core, block in ((0, q_plane[k, plane, me % 2]), (1, q_core[k, plane])):
                device = place.peer(k * 8 + plane * 2 + core)
                q_wide[pl.ds(pl.multiple_of(device * 8, 8), local_rows), :] = block.astype(f32)
                own_wide[pl.ds(pl.multiple_of(device * 16, 16), 16), :] = kv_all[
                    k, plane, core, 2 * span : 2 * span + 16
                ].astype(f32)
    total_positions = shards * positions
    counted = lax.broadcasted_iota(jnp.int32, (1, total_positions), 1)
    position = (counted // positions ^ me) * positions + counted % positions

    def picked(ref, start, count, stride):
        return jnp.concatenate(
            [ref[pl.ds(start + r, count, stride=stride), :] for r in range(local_rows)], axis=0
        )

    for b in range(blocks):
        first = b * per_block
        key_at, value_at = b * positions, span + b * positions
        key = kv_all[:, :, :, key_at : key_at + positions, :].reshape(total_positions, HD)
        value = kv_all[:, :, :, value_at : value_at + positions, :].reshape(total_positions, HD)
        query = picked(q_wide, first * 8, per_block, 8)
        own_k = picked(own_wide, first * 16, per_block, 16)
        own_v = picked(own_wide, first * 16 + 8, per_block, 16)
        scores = lax.dot_general(
            query.astype(jnp.bfloat16), key, (((1,), (1,)), ((), ())), preferred_element_type=f32
        )
        is_valid = position < lengths[b]
        scores = jnp.where(is_valid, scores * score_scale, NEG)
        own_score = jnp.sum(query * own_k, axis=1, keepdims=True) * score_scale
        top = jnp.maximum(jnp.max(scores, axis=1, keepdims=True), own_score)
        weights = jnp.where(is_valid, jnp.exp(scores - top), 0.0)
        own_weight = jnp.exp(own_score - top)
        denominator = jnp.sum(weights, axis=1, keepdims=True) + own_weight
        numerator = jnp.dot(weights.astype(jnp.bfloat16), value, preferred_element_type=f32)
        result = (numerator + own_weight * own_v) / denominator
        for r in range(local_rows):
            attended[r * shards + first : r * shards + first + per_block, :] = result[
                r * per_block : (r + 1) * per_block, :
            ]

    def multiply_out(rows, matrix_ref, piece):
        first, count, _ = pieces[piece]
        for at in range(first, first + count, 4):
            result = jnp.dot(
                rows, matrix_ref[:, at * 128 : (at + 4) * 128], preferred_element_type=f32
            )
            for i in range(4):
                for r in range(local_rows):
                    partial[pl.ds((at + i) * local_rows + r, shards, stride=size), :] = result[
                        r * shards : (r + 1) * shards, i * 128 : (i + 1) * 128
                    ]

    loads[9].wait()
    head_rows = attended[...].astype(jnp.bfloat16)
    projected, more = collect(
        place,
        partial,
        size,
        local_rows,
        first_boxes,
        first_sems,
        lambda piece: multiply_out(head_rows, w_out_ref, piece),
        dequantize_down,
    )
    waits = waits + more

    loads[14].wait()
    loads[15].wait()
    for i in range(lanes):
        mixed_ref[i * local_rows : (i + 1) * local_rows, :] = hidden_ref[
            :, i * 128 : (i + 1) * 128
        ].astype(f32)
    mixed = mixed_ref[...] + projected
    mixed_ref[...] = mixed
    for r in range(local_rows):
        row = mixed_ref[pl.ds(r, lanes, stride=local_rows), :]
        squares = jnp.sum(jnp.sum(row * row, axis=0, keepdims=True), axis=1, keepdims=True)
        normed_ref[pl.ds(r, lanes, stride=local_rows), :] = (
            row * lax.rsqrt(squares / width + EPSILON) * gain_ref[...]
        )
    normed_all[0, 0, 0] = normed_ref[...].astype(jnp.bfloat16)

    def widen(k, core):
        for plane in range(4):
            device = place.peer(k * 8 + plane * 2 + core)
            at = pl.ds(pl.multiple_of(device * size, size), size)
            rows_wide[at, :] = normed_all[k, plane, core].astype(f32)

    def write_attention():
        for i in range(lanes):
            mixed_out[:, i * 128 : (i + 1) * 128] = mixed_ref[
                i * local_rows : (i + 1) * local_rows, :
            ]

    more = spread(
        place,
        lambda k: normed_all.at[0, 0, 0],
        normed_all,
        row_sems,
        lambda k: None,
        lambda k: None,
        lambda k: widen(k, 0),
        lambda k: widen(k, 1),
        write_attention,
    )
    waits = waits + more
    for i in range(lanes):
        for r in range(local_rows):
            rows_ref[r * shards : (r + 1) * shards, i * 128 : (i + 1) * 128] = rows_wide[
                pl.ds(i * local_rows + r, shards, stride=size), :
            ].astype(jnp.bfloat16)
    half = down_ref.shape[0]
    projected_in = jnp.dot(rows_ref[...], gate_ref[...], preferred_element_type=f32)
    split = picked(own_wide, local_rows, shards, 16)
    lane = lax.broadcasted_iota(jnp.int32, split.shape, 1)
    weight = jnp.sum(jnp.where(lane % 64 == me // 2, split, 0.0), axis=1, keepdims=True)
    gate = projected_in[:, :half]
    activated = gate / (1.0 + jnp.exp(-gate)) * projected_in[:, half:]
    activated = jnp.where(weight != 0.0, activated * weight, 0.0).astype(jnp.bfloat16)
    expert_sum, more = collect(
        place,
        partial,
        size,
        local_rows,
        second_boxes,
        second_sems,
        lambda piece: multiply_out(activated, down_ref, piece),
        lambda: None,
    )
    waits = waits + more
    mixed_ref[...] = expert_sum
    for i in range(lanes):
        expert_out[:, i * 128 : (i + 1) * 128] = mixed_ref[i * local_rows : (i + 1) * local_rows, :]
    for ref, sem in waits:
        arrived(ref, sem)


def fused_layer(
    queries,
    own_key,
    own_value,
    cache_keys,
    cache_values,
    prefix_of_row,
    context_len,
    hidden_in,
    w_out,
    norm_gain,
    expert_ids,
    route_weights,
    gate_up_codes,
    gate_up_scales,
    down_codes,
    down_scales,
):
    shards = lax.axis_size("ctx")
    local_rows, width = queries.shape
    lanes = width // 128
    size = local_rows * lanes
    span = shards * local_rows // CAND * cache_keys.shape[1]
    column = shards // 8
    bf16, f32 = jnp.bfloat16, jnp.float32
    kv_rows = 2 * span + 16
    boxes = []
    for _, count, column_first in pieces_of(lanes):
        rows = count * local_rows
        chips, line, plane = (column, 4, rows, 128), (column, rows, 128), (4, rows, 128)
        last = (plane, plane, chips, chips) if column_first else (chips, chips, line, line)
        boxes = boxes + [pltpu.VMEM(shape, bf16) for shape in (chips, chips) + last]
    operands = (
        prefix_of_row,
        context_len,
        cache_keys,
        cache_values,
        own_key,
        own_value,
        queries,
        expert_ids,
        route_weights,
        w_out,
        gate_up_codes[0],
        gate_up_scales.transpose(2, 0, 1),
        down_codes[0],
        down_scales.transpose(1, 0, 2),
        hidden_in,
        norm_gain.reshape(lanes, 128),
    )
    scalars = (0, 1, 11, 13)
    out = jax.ShapeDtypeStruct((local_rows, width), f32)
    vmem = pl.BlockSpec(memory_space=pltpu.VMEM)
    mixed, expert_sum = pl.pallas_call(
        lambda *refs: layer_kernel(shards, CAND // local_rows, *refs),
        out_shape=(out, out),
        in_specs=[pl.BlockSpec(memory_space=pltpu.HBM)] * len(operands),
        out_specs=(vmem, vmem),
        scratch_shapes=[
            (pltpu.SMEM if i in scalars else pltpu.VMEM)(x.shape, x.dtype)
            for i, x in enumerate(operands)
        ]
        + [
            pltpu.SemaphoreType.DMA((len(operands),)),
            pltpu.VMEM((16, 128), f32),
            pltpu.VMEM((shards, local_rows, 128), bf16),
            pltpu.VMEM((column, 8, local_rows, 128), bf16),
            pltpu.VMEM((column, 4, 2, local_rows, 128), bf16),
            pltpu.VMEM((column, 4, local_rows, 128), bf16),
            pltpu.VMEM((shards * 8, 128), f32),
            pltpu.VMEM((own_key.shape[1] // HD, kv_rows, 128), bf16),
            pltpu.VMEM((column, 4, 2, kv_rows, 128), bf16),
            pltpu.VMEM((shards * 16, 128), f32),
            pltpu.VMEM((shards * local_rows, 128), f32),
            pltpu.VMEM((shards * size, 128), f32),
            pltpu.VMEM((size, 128), f32),
            pltpu.VMEM((size, 128), f32),
            pltpu.VMEM((column, 4, 2, size, 128), bf16),
            pltpu.VMEM((shards * size, 128), f32),
            pltpu.VMEM((shards * local_rows, width), bf16),
        ]
        + boxes
        + boxes
        + [
            pltpu.SemaphoreType.DMA((count,))
            for count in (3, 2 * column + 1, 3, 3 * column, 3, 3 * column)
            + (3, column + 2, 3, 2 * column + 1, 3, 2 * column + 1) * 2
        ],
        compiler_params=pltpu.CompilerParams(
            collective_id=1, has_side_effects=True, vmem_limit_bytes=VMEM_BYTES
        ),
        name="fused_layer",
    )(*operands)
    return mixed.astype(bf16), (mixed + expert_sum).astype(bf16)


def fits_fused(queries, own_key, cache_keys, w_out, expert_ids):
    shards = lax.axis_size("ctx")
    local_rows, width = queries.shape
    return (
        shards % 8 == 0
        and shards & (shards - 1) == 0
        and w_out.shape[0] == HD
        and width == shards * HD
        and w_out.shape[1] == width
        and local_rows == 4
        and width % (128 * 32) == 0
        and shards // 2 <= 64
        and shards % (own_key.shape[1] // HD * 8) == 0
        and shards * local_rows % CAND == 0
        and cache_keys.shape[1] % 16 == 0
    )


def local(*arrays):
    queries, own_key, cache_keys = arrays[0], arrays[1], arrays[3]
    if fits_fused(queries, own_key, cache_keys, arrays[8], arrays[10]):
        return fused_layer(*arrays)
    return staged_layer(*arrays)


def solution(mesh):
    return jax.shard_map(
        local,
        mesh=mesh,
        in_specs=(
            P(("replica", "ctx"), None),
            P(("replica", "ctx"), None),
            P(("replica", "ctx"), None),
            P("replica", "ctx", None),
            P("replica", "ctx", None),
            P("replica"),
            P("replica"),
            P(("replica", "ctx"), None),
            P("ctx", None),
            P(),
            P(("replica", "ctx"), None),
            P(("replica", "ctx"), None),
            P("ctx", None, None),
            P("ctx", None, None),
            P("ctx", None, None),
            P("ctx", None, None),
        ),
        out_specs=(P(("replica", "ctx"), None), P(("replica", "ctx"), None)),
        check_vma=False,
    )
```
